128 devices in a mesh: seqs: 1, rows: 2 (over core), states: 64 (over z, y, x).
Axes of the slice: x: 4, y: 4, z: 4, core: 2. Of those that a mesh axis runs over, the one named last changes fastest.
Arguments:
- trans_mat: bfloat16 [16384, 2, 8192], P('rows', None, 'states')
- emit_mat: bfloat16 [16384, 10000], P(('rows', 'states'))
- init_dist: float32 [16384], P(('rows', 'states'))
- tokens: int32 [16, 128], P('seqs')
- lengths: int32 [16], P('seqs')
Outputs:
- output 1: float32 [16], P('seqs')
- output 2: float32 [16, 16384], P('seqs', ('rows', 'states'))
All inputs are finite; a program needn't handle non-finite values.
Results may differ from the reference program's by a relative error of at most 0.001.
Values are sent between devices in bfloat16 or wider.
A program may use at most 1 GiB of HBM per device.

```python
import jax
import jax.numpy as jnp
from jax import lax
import functools

STATES = 16384
VOCAB = 10000
BATCH = 16
STEPS = 128
ROW_SPLIT = 2
DRAW_ROWS = 256


def draw_rows(key, n_cols, sharpness):
    logits = sharpness * jax.random.normal(key, (DRAW_ROWS, n_cols), jnp.float32)
    return jax.nn.softmax(logits, axis=1).astype(jnp.bfloat16)


def draw_sequences(key):
    key_tok, key_len, key_long, key_short = jax.random.split(key, 4)
    tokens = jax.random.randint(key_tok, (BATCH, STEPS), 0, VOCAB, dtype=jnp.int32)
    lengths = jax.random.randint(key_len, (BATCH,), 1, STEPS + 1, dtype=jnp.int32)
    long_row = jax.random.randint(key_long, (), 0, BATCH, dtype=jnp.int32)
    short_row = (long_row + 1 + jax.random.randint(key_short, (), 0, BATCH - 1, dtype=jnp.int32)) % BATCH
    lengths = lengths.at[long_row].set(STEPS).at[short_row].set(1)
    return tokens, lengths


def setup_inputs(seed: int = 0, part: int = 0) -> dict:
    base_key = jax.random.key(seed)
    key_trans, key_emit, key_init, key_seq = jax.random.split(base_key, 4)
    n_blocks = STATES // DRAW_ROWS
    trans_rows = lax.map(functools.partial(draw_rows, n_cols=STATES, sharpness=2.5), jax.random.split(key_trans, n_blocks))
    emit_rows = lax.map(functools.partial(draw_rows, n_cols=VOCAB, sharpness=2.0), jax.random.split(key_emit, n_blocks))
    init_dist = jax.nn.softmax(1.5 * jax.random.normal(key_init, (STATES,), jnp.float32))
    tokens, lengths = draw_sequences(jax.random.fold_in(key_seq, part))
    return {'trans_mat': trans_rows.reshape(STATES, ROW_SPLIT, STATES // ROW_SPLIT), 'emit_mat': emit_rows.reshape(STATES, VOCAB), 'init_dist': init_dist, 'tokens': tokens, 'lengths': lengths}


def emission(emit_mat, step_tok):
    return jnp.take(emit_mat, step_tok, axis=1).T.astype(jnp.float32)


def reference(trans_mat, emit_mat, init_dist, tokens, lengths):
    trans_full = trans_mat.reshape(STATES, STATES)
    first_raw = init_dist[None, :] * emission(emit_mat, tokens[:, 0])
    norm_c = jnp.sum(first_raw, axis=1)
    alpha_init = first_raw / norm_c[:, None]
    loglik_init = jnp.log(norm_c)

    def one_step(state_in, inputs):
        alpha_cur, loglik = state_in
        step_tok, t_index = inputs
        mix_sum = jnp.dot(alpha_cur.astype(jnp.bfloat16), trans_full, preferred_element_type=jnp.float32)
        raw_next = mix_sum * emission(emit_mat, step_tok)
        norm_step = jnp.sum(raw_next, axis=1)
        active = t_index < lengths
        alpha_cur = jnp.where(active[:, None], raw_next / norm_step[:, None], alpha_cur)
        loglik = loglik + jnp.where(active, jnp.log(norm_step), 0.0)
        return (alpha_cur, loglik), None

    scan_out = lax.scan(one_step, (alpha_init, loglik_init), (tokens[:, 1:].T, jnp.arange(1, STEPS)))
    alpha_last, loglik = scan_out[0]
    return loglik, alpha_last
```

```python
import functools

import jax
import jax.numpy as jnp
from jax import lax
from jax.experimental import pallas as pl
from jax.experimental.pallas import tpu as pltpu
from jax.sharding import PartitionSpec as P

CHIPS = (4, 4, 4)
SB = 128
F32 = jnp.float32
BF16 = jnp.bfloat16


def ring_distance(offset, n):
    return min(offset, n - offset)


def forward_kernel(dims, n_steps, a_ref, e_ref, r0_ref, lencol_ref, lenrow_ref, alpha_ref, ll_ref,
                   a_loc, e_loc, r_in, c_in, p_in, u_in, u_out, a_bf, alpha_acc, ll_acc, fin_alpha, fin_ll,
                   a_sem, a_send, e_sem, e_send, r0_sem, r0_send, own_sem,
                   g_recv, g_send, c_recv, c_send, u_recv, u_send, p_recv, p_send, f_recv, f_send):
    nz, ny, nx = dims
    plane = ny * nx
    batch = r0_ref.shape[0]
    half = plane * SB
    core = lax.axis_index('rows')
    me = lax.axis_index('states')
    z = me // plane
    yx = me % plane
    y = yx // nx
    x = yx % nx
    far_z = sorted(range(1, nz), key=lambda d: -ring_distance(d, nz))
    far_yx = sorted(((j, i) for j in range(ny) for i in range(nx) if j or i),
                    key=lambda o: -(ring_distance(o[0], ny) + ring_distance(o[1], nx)))

    def line_peer(dz):
        return ((z + dz) % nz) * plane + yx

    def plane_peer(dy, dx):
        return z * plane + ((y + dy) % ny) * nx + (x + dx) % nx

    def remote(src, dst, send, recv, state):
        return pltpu.make_async_remote_copy(src_ref=src, dst_ref=dst, send_sem=send, recv_sem=recv,
                                            device_id={'rows': 1, 'states': state},
                                            device_id_type=pl.DeviceIdType.MESH)

    def wait_bytes(ref, sem):
        pltpu.make_async_copy(ref, ref, sem).wait()

    def hand_over(h):
        copies = []
        for k in range(nz):
            if h == 1 and k == 0:
                continue
            dz = (nz - k) % nz
            rows = pl.ds(((z + k) % nz) * half, half)
            copies.append(remote(a_ref.at[rows], a_loc.at[dz, pl.ds(h * half, half)],
                                 a_send.at[k], a_sem.at[dz, h], line_peer(k)))
        for k in range(nz):
            if h == 1 and k == 0:
                continue
            dz = (nz - k) % nz
            copies.append(remote(e_ref, e_loc.at[dz, h], e_send.at[k], e_sem.at[dz, h], line_peer(k)))
        return copies

    @pl.when(core == 0)
    def helper():
        first = remote(r0_ref, r_in.at[0, yx, 0], r0_send, r0_sem, me)
        first.start()
        copies = hand_over(0)
        for copy in copies:
            copy.start()
        first.wait_send()
        for copy in copies:
            copy.wait_send()
        wait_bytes(fin_alpha, f_recv.at[0])
        wait_bytes(fin_ll, f_recv.at[1])
        alpha_ref[...] = fin_alpha[...]
        ll_ref[...] = fin_ll[...]

    @pl.when(core == 1)
    def owner():
        eye = (lax.broadcasted_iota(jnp.int32, (batch, SB), 0)
               == lax.broadcasted_iota(jnp.int32, (batch, SB), 1))

        def as_row(tile):
            col = jnp.sum(tile, axis=1, keepdims=True)
            return jnp.sum(jnp.where(eye, col, 0.0), axis=0, keepdims=True)

        def as_col(row):
            return jnp.sum(jnp.where(eye, row, 0.0), axis=1, keepdims=True)

        def start_gather(slot):
            for dy, dx in far_yx:
                remote(r_in.at[slot, yx], r_in.at[slot, yx], g_send, g_recv.at[slot], plane_peer(dy, dx)).start()

        def start_norms(slot):
            for dy, dx in far_yx:
                remote(c_in.at[slot, yx], c_in.at[slot, yx], c_send, c_recv.at[slot], plane_peer(dy, dx)).start()

        def start_line_sums(slot):
            for dz in far_z:
                remote(p_in.at[slot, z], p_in.at[slot, z], p_send, p_recv.at[slot], line_peer(dz)).start()

        def finish_norm(slot):
            wait_bytes(p_in.at[slot, pl.ds(0, nz - 1)], p_recv.at[slot])
            c_in[slot, yx] = jnp.sum(p_in[slot], axis=0)
            start_norms(slot)

        others = pl.ds(0, plane - 1)

        def norm(slot):
            wait_bytes(c_in.at[slot, others], c_recv.at[slot])
            c_row = jnp.sum(c_in[slot], axis=0)
            return c_row, 1.0 / as_col(c_row)

        def keep(t, slot, c_row, inv):
            active = t < lencol_ref[...]
            for h in range(2):
                alpha_acc[h] = jnp.where(active, r_in[slot, yx, h] * inv, alpha_acc[h])
            ll_acc[...] = ll_acc[...] + jnp.where(t < lenrow_ref[...], jnp.log(c_row), 0.0)

        copies = hand_over(1)
        for copy in copies:
            copy.start()
        own = [pltpu.make_async_copy(a_ref.at[pl.ds(z * half, half)], a_loc.at[0, pl.ds(half, half)], own_sem.at[0]),
               pltpu.make_async_copy(e_ref, e_loc.at[0, 1], own_sem.at[1])]
        for copy in own:
            copy.start()
        alpha_acc[...] = jnp.zeros_like(alpha_acc)
        ll_acc[...] = jnp.zeros_like(ll_acc)
        r_in[0, yx, 1] = r0_ref[...]
        wait_bytes(r0_ref, r0_sem)
        p_in[0, z] = as_row(r_in[0, yx, 0] + r_in[0, yx, 1])
        start_line_sums(0)
        start_gather(0)
        finish_norm(0)
        wait_bytes(p_in.at[0, pl.ds(0, nz - 1)], p_send)
        for copy in own:
            copy.wait()
        for h in range(2):
            for dz in range(nz):
                if h == 1 and dz == 0:
                    continue
                wait_bytes(e_loc.at[dz, h], e_sem.at[dz, h])
                wait_bytes(a_loc.at[dz, pl.ds(h * half, half)], a_sem.at[dz, h])
        for copy in copies:
            copy.wait_send()

        def one_step(t, carry):
            cur = t % 2
            nxt = (t + 1) % 2
            c_row, inv = norm(cur)
            wait_bytes(r_in.at[cur, others], g_recv.at[cur])
            for src in range(plane):
                for h in range(2):
                    a_bf[:, pl.ds(h * half + src * SB, SB)] = (r_in[cur, src, h] * inv).astype(BF16)
            total = jnp.zeros((batch, SB), F32)
            for dz in far_z + [0]:
                part = jnp.dot(a_bf[...], a_loc[dz], preferred_element_type=F32)
                parts = (part[:, :SB], part[:, SB:])
                if dz:
                    for h in range(2):
                        u_out[dz - 1, h] = parts[h]
                    remote(u_out.at[dz - 1], u_in.at[nxt, nz - dz - 1], u_send, u_recv.at[nxt], line_peer(dz)).start()
                for h in range(2):
                    total = total + parts[h] * e_loc[dz, h, t + 1].astype(F32)
            p_in[nxt, z] = as_row(total)
            start_line_sums(nxt)
            wait_bytes(r_in.at[cur, others], g_send)
            wait_bytes(c_in.at[cur, others], c_send)
            keep(t, cur, c_row, inv)
            wait_bytes(u_in.at[nxt], u_recv.at[nxt])
            for h in range(2):
                u = parts[h]
                for k in range(nz - 1):
                    u = u + u_in[nxt, k, h]
                r_in[nxt, yx, h] = u * e_loc[0, h, t + 1].astype(F32)
            start_gather(nxt)
            finish_norm(nxt)
            wait_bytes(u_out, u_send)
            wait_bytes(p_in.at[nxt, pl.ds(0, nz - 1)], p_send)
            return carry

        lax.fori_loop(0, n_steps - 1, one_step, 0)
        last = (n_steps - 1) % 2
        c_row, inv = norm(last)
        wait_bytes(r_in.at[last, others], g_recv.at[last])
        keep(n_steps - 1, last, c_row, inv)
        wait_bytes(r_in.at[last, others], g_send)
        wait_bytes(c_in.at[last, others], c_send)

        def to_helper(src, dst, i):
            return pltpu.make_async_remote_copy(src_ref=src, dst_ref=dst, send_sem=f_send.at[i], recv_sem=f_recv.at[i],
                                                device_id={'rows': 0, 'states': me},
                                                device_id_type=pl.DeviceIdType.MESH)

        result = [to_helper(alpha_acc.at[0], fin_alpha, 0), to_helper(ll_acc, fin_ll, 1)]
        for copy in result:
            copy.start()
        alpha_ref[...] = alpha_acc[1]
        ll_ref[...] = ll_acc[...]
        for copy in result:
            copy.wait_send()


def solution(mesh):
    vec_axes = ('rows', 'states')
    nz, ny, nx = CHIPS
    plane = ny * nx

    def local_forward(trans_blk, emit_blk, init_blk, tokens, lengths):
        batch, n_steps = tokens.shape
        cols = 2 * SB
        a_blk = trans_blk.reshape(trans_blk.shape[0], cols)
        emis = jnp.transpose(jnp.take(emit_blk, tokens, axis=1), (2, 1, 0))
        first_raw = init_blk[None, :] * emis[0].astype(F32)
        len_col = jnp.broadcast_to(lengths[:, None], (batch, SB))
        len_row = jnp.pad(lengths, (0, SB - batch))[None, :]
        vmem = pl.BlockSpec(memory_space=pltpu.VMEM)
        hbm = pl.BlockSpec(memory_space=pl.ANY)
        dma = pltpu.SemaphoreType.DMA
        k_rows = 2 * plane * SB
        alpha, ll = pl.pallas_call(
            functools.partial(forward_kernel, CHIPS, n_steps),
            out_shape=(jax.ShapeDtypeStruct((batch, SB), F32), jax.ShapeDtypeStruct((1, SB), F32)),
            in_specs=[hbm, hbm, vmem, vmem, vmem],
            out_specs=(vmem, vmem),
            scratch_shapes=[
                pltpu.VMEM((nz, k_rows, cols), BF16),
                pltpu.VMEM((nz, 2, n_steps, batch, SB), BF16),
                pltpu.VMEM((2, plane, 2, batch, SB), F32),
                pltpu.VMEM((2, plane, 1, SB), F32),
                pltpu.VMEM((2, nz, 1, SB), F32),
                pltpu.VMEM((2, nz - 1, 2, batch, SB), F32),
                pltpu.VMEM((nz - 1, 2, batch, SB), F32),
                pltpu.VMEM((batch, k_rows), BF16),
                pltpu.VMEM((2, batch, SB), F32),
                pltpu.VMEM((1, SB), F32),
                pltpu.VMEM((batch, SB), F32),
                pltpu.VMEM((1, SB), F32),
                dma((nz, 2)), dma((nz,)), dma((nz, 2)), dma((nz,)), dma, dma, dma((2,)),
                dma((2,)), dma, dma((2,)), dma, dma((2,)), dma, dma((2,)), dma, dma((2,)), dma((2,)),
            ],
            compiler_params=pltpu.CompilerParams(has_side_effects=True, vmem_limit_bytes=48 * 1024 * 1024),
            cost_estimate=pl.CostEstimate(flops=2 * batch * (n_steps - 1) * nz * k_rows * cols,
                                          bytes_accessed=nz * k_rows * cols * 2, transcendentals=0),
        )(a_blk, emis, first_raw, len_col, len_row)
        return ll[0, :batch], alpha

    return jax.shard_map(local_forward, mesh=mesh, in_specs=(P('rows', None, 'states'), P(vec_axes, None), P(vec_axes), P('seqs', None), P('seqs')), out_specs=(P('seqs'), P('seqs', vec_axes)), check_vma=False)
```

```python
import functools

import jax
import jax.numpy as jnp
from jax import lax
from jax.experimental import pallas as pl
from jax.experimental.pallas import tpu as pltpu
from jax.sharding import PartitionSpec as P

CHIPS = (4, 4, 4)
SB = 128
LIFT = 2.0 ** 64
F32 = jnp.float32
BF16 = jnp.bfloat16


def ring_distance(offset, n):
    return min(offset, n - offset)


def forward_kernel(dims, n_steps, a_ref, e_ref, r0_ref, lencol_ref, lenrow_ref, alpha_ref, ll_ref,
                   a_loc, e_both, e_loc, w_loc, r_in, c_in, p_in, u_in, u_out, a_bf, alpha_acc, ll_acc, fin_alpha,
                   fin_ll, a_sem, a_send, e_pair, e_send, e_sem, r0_sem, r0_send, own_sem,
                   g_recv, g_send, c_recv, c_send, u_recv, u_send, p_recv, p_send, f_recv, f_send):
    nz, ny, nx = dims
    plane = nz * ny
    batch = r0_ref.shape[0]
    half = nx * SB
    block = plane
    rows = block * batch
    n_blocks = n_steps // block
    core = lax.axis_index('rows')
    me = lax.axis_index('states')
    zy = me // nx
    x = me % nx
    z = zy // ny
    y = zy % ny
    offsets = [(j, i) for j in range(nz) for i in range(ny)]
    rel = {o: k for k, o in enumerate(offsets)}
    mirror = [rel[(-j) % nz, (-i) % ny] for j, i in offsets]
    far = sorted(range(1, plane), key=lambda k: -(ring_distance(offsets[k][0], nz) + ring_distance(offsets[k][1], ny)))
    far_x = sorted(range(1, nx), key=lambda d: -ring_distance(d, nx))

    def plane_zy(k):
        return ((z + offsets[k][0]) % nz) * ny + (y + offsets[k][1]) % ny

    def plane_peer(k):
        return plane_zy(k) * nx + x

    def line_peer(d):
        return zy * nx + (x + d) % nx

    def remote(src, dst, send, recv, state, to=1):
        return pltpu.make_async_remote_copy(src_ref=src, dst_ref=dst, send_sem=send, recv_sem=recv,
                                            device_id={'rows': to, 'states': state},
                                            device_id_type=pl.DeviceIdType.MESH)

    def wait_bytes(ref, sem):
        pltpu.make_async_copy(ref, ref, sem).wait()

    def hand_over(h):
        return [remote(a_ref.at[pl.ds(plane_zy(k) * half, half)], a_loc.at[mirror[k], pl.ds(h * half, half)],
                       a_send.at[k], a_sem.at[mirror[k], h], plane_peer(k))
                for k in far + ([0] if h == 0 else [])]

    @pl.when(core == 0)
    def helper():
        first = remote(r0_ref, r_in.at[0, x, 0], r0_send, r0_sem, me)
        first.start()
        mine = pltpu.make_async_copy(e_ref, e_both.at[:, pl.ds(0, SB)], own_sem.at[0])
        mine.start()
        copies = hand_over(0)
        for copy in copies:
            copy.start()
        mine.wait()
        wait_bytes(e_both.at[:, pl.ds(SB, SB)], e_pair)

        def send_block(b, carry):
            src = e_both.at[pl.ds(b * rows, rows)]
            for k in [0] + far:
                remote(src, e_loc.at[b, mirror[k]], e_send, e_sem.at[b], plane_peer(k)).start()
            wait_bytes(e_loc.at[b], e_send)
            return carry

        lax.fori_loop(0, n_blocks, send_block, 0)
        first.wait_send()
        for copy in copies:
            copy.wait_send()
        wait_bytes(fin_alpha, f_recv.at[0])
        wait_bytes(fin_ll, f_recv.at[1])
        alpha_ref[...] = fin_alpha[...]
        ll_ref[...] = fin_ll[...]

    @pl.when(core == 1)
    def owner():
        eye = (lax.broadcasted_iota(jnp.int32, (batch, SB), 0)
               == lax.broadcasted_iota(jnp.int32, (batch, SB), 1))

        def as_row(tile):
            col = jnp.sum(tile, axis=1, keepdims=True)
            return jnp.sum(jnp.where(eye, col, 0.0), axis=0, keepdims=True)

        def as_col(row):
            return jnp.sum(jnp.where(eye, row, 0.0), axis=1, keepdims=True)

        def start_gather(slot):
            for d in far_x:
                remote(r_in.at[slot, x], r_in.at[slot, x], g_send, g_recv.at[slot], line_peer(d)).start()

        def start_plane_sums(slot):
            for k in far:
                remote(p_in.at[slot, zy], p_in.at[slot, zy], p_send, p_recv.at[slot], plane_peer(k)).start()

        others = pl.ds(0, nx - 1)
        peers = pl.ds(0, plane - 1)

        def finish_norm(slot):
            wait_bytes(p_in.at[slot, peers], p_recv.at[slot])
            c_in[slot, x] = jnp.sum(p_in[slot], axis=0)
            for d in far_x:
                remote(c_in.at[slot, x], c_in.at[slot, x], c_send, c_recv.at[slot], line_peer(d)).start()

        def norm(slot):
            wait_bytes(c_in.at[slot, others], c_recv.at[slot])
            c_row = jnp.sum(c_in[slot], axis=0)
            return c_row, 1.0 / as_col(c_row)

        def keep(t, slot, c_row, inv):
            active = t < lencol_ref[...]
            for h in range(2):
                alpha_acc[h] = jnp.where(active, r_in[slot, x, h] * inv, alpha_acc[h])
            ll_acc[...] = ll_acc[...] + jnp.where(t < lenrow_ref[...], jnp.log(c_row * (1.0 / LIFT)), 0.0)

        def add_w(b, k, fresh):
            part = lax.dot_general(e_loc[b, k], a_loc[k], (((1,), (1,)), ((), ())), preferred_element_type=F32)
            slot = b % 2
            w_loc[slot] = jnp.where(fresh, 0.0, w_loc[slot]) + part

        copies = hand_over(1)
        pair = remote(e_ref, e_both.at[:, pl.ds(SB, SB)], own_sem.at[0], e_pair, me, to=0)
        pair.start()
        for copy in copies:
            copy.start()
        own = pltpu.make_async_copy(a_ref.at[pl.ds(zy * half, half)], a_loc.at[0, pl.ds(half, half)], own_sem.at[1])
        own.start()
        alpha_acc[...] = jnp.zeros_like(alpha_acc)
        ll_acc[...] = jnp.zeros_like(ll_acc)
        r_in[0, x, 1] = r0_ref[...]
        wait_bytes(r0_ref, r0_sem)
        p_in[0, zy] = as_row(r_in[0, x, 0] + r_in[0, x, 1])
        start_plane_sums(0)
        start_gather(0)
        finish_norm(0)
        wait_bytes(p_in.at[0, peers], p_send)
        own.wait()
        for k in range(plane):
            for h in range(2):
                if h == 0 or k:
                    wait_bytes(a_loc.at[k, pl.ds(h * half, half)], a_sem.at[k, h])
        pair.wait_send()
        for copy in copies:
            copy.wait_send()
        wait_bytes(e_loc.at[0], e_sem.at[0])
        w_loc[...] = jnp.zeros_like(w_loc)

        def first_w(k, carry):
            add_w(0, k, False)
            return carry

        lax.fori_loop(0, plane, first_w, 0)

        def one_step(t, carry):
            cur = t % 2
            nxt = (t + 1) % 2
            b = t // block
            row = pl.ds((t % block) * batch, batch)
            c_row, inv = norm(cur)
            wait_bytes(r_in.at[cur, others], g_recv.at[cur])
            total = jnp.zeros((batch, SB), F32)
            for h in range(2):
                for src in range(nx):
                    cols = pl.ds(h * half + src * SB, SB)
                    tile = (r_in[cur, src, h] * inv).astype(BF16)
                    a_bf[:, cols] = tile
                    total = total + tile.astype(F32) * w_loc[b % 2, row, cols]
            for i, k in enumerate(far + [0]):
                part = jnp.dot(a_bf[...], a_loc[k], preferred_element_type=F32)
                parts = (part[:, :SB], part[:, SB:])
                if k:
                    for h in range(2):
                        u_out[k - 1, h] = parts[h]
                    remote(u_out.at[k - 1], u_in.at[nxt, mirror[k] - 1], u_send, u_recv.at[nxt], plane_peer(k)).start()
                if i == 0:
                    p_in[nxt, zy] = as_row(total)
                    start_plane_sums(nxt)
            wait_bytes(r_in.at[cur, others], g_send)
            wait_bytes(c_in.at[cur, others], c_send)
            keep(t, cur, c_row, inv)
            wait_bytes(u_in.at[nxt], u_recv.at[nxt])
            for h in range(2):
                u = parts[h]
                for k in range(plane - 1):
                    u = u + u_in[nxt, k, h]
                r_in[nxt, x, h] = u * e_loc[b, 0, row, pl.ds(h * SB, SB)].astype(F32)
            start_gather(nxt)
            finish_norm(nxt)

            @pl.when(b + 1 < n_blocks)
            def next_w():
                k = t % block
                later = b + 1

                @pl.when(k == 0)
                def arrived():
                    wait_bytes(e_loc.at[later], e_sem.at[later])

                add_w(later, k, k == 0)

            wait_bytes(u_out, u_send)
            wait_bytes(p_in.at[nxt, peers], p_send)
            return carry

        lax.fori_loop(0, n_steps - 1, one_step, 0)
        last = (n_steps - 1) % 2
        c_row, inv = norm(last)
        wait_bytes(r_in.at[last, others], g_recv.at[last])
        keep(n_steps - 1, last, c_row, inv)
        wait_bytes(r_in.at[last, others], g_send)
        wait_bytes(c_in.at[last, others], c_send)
        result = [remote(alpha_acc.at[0], fin_alpha, f_send.at[0], f_recv.at[0], me, to=0),
                  remote(ll_acc, fin_ll, f_send.at[1], f_recv.at[1], me, to=0)]
        for copy in result:
            copy.start()
        alpha_ref[...] = alpha_acc[1]
        ll_ref[...] = ll_acc[...]
        for copy in result:
            copy.wait_send()


def solution(mesh):
    vec_axes = ('rows', 'states')
    nz, ny, nx = CHIPS
    plane = nz * ny

    def local_forward(trans_blk, emit_blk, init_blk, tokens, lengths):
        batch, n_steps = tokens.shape
        cols = 2 * SB
        a_blk = trans_blk.reshape(trans_blk.shape[0], cols)
        emis = jnp.transpose(jnp.take(emit_blk, jnp.roll(tokens, -1, axis=1), axis=1), (2, 1, 0))
        emis = emis * jnp.asarray(LIFT, emis.dtype)
        first_raw = init_blk[None, :] * emis[-1].astype(F32)
        len_col = jnp.broadcast_to(lengths[:, None], (batch, SB))
        len_row = jnp.pad(lengths, (0, SB - batch))[None, :]
        vmem = pl.BlockSpec(memory_space=pltpu.VMEM)
        hbm = pl.BlockSpec(memory_space=pl.ANY)
        dma = pltpu.SemaphoreType.DMA
        k_rows = 2 * nx * SB
        block_rows = plane * batch
        n_blocks = n_steps // plane
        alpha, ll = pl.pallas_call(
            functools.partial(forward_kernel, CHIPS, n_steps),
            out_shape=(jax.ShapeDtypeStruct((batch, SB), F32), jax.ShapeDtypeStruct((1, SB), F32)),
            in_specs=[hbm, hbm, vmem, vmem, vmem],
            out_specs=(vmem, vmem),
            scratch_shapes=[
                pltpu.VMEM((plane, k_rows, cols), BF16),
                pltpu.VMEM((n_steps * batch, cols), BF16),
                pltpu.VMEM((n_blocks, plane, block_rows, cols), BF16),
                pltpu.VMEM((2, block_rows, k_rows), F32),
                pltpu.VMEM((2, nx, 2, batch, SB), F32),
                pltpu.VMEM((2, nx, 1, SB), F32),
                pltpu.VMEM((2, plane, 1, SB), F32),
                pltpu.VMEM((2, plane - 1, 2, batch, SB), F32),
                pltpu.VMEM((plane - 1, 2, batch, SB), F32),
                pltpu.VMEM((batch, k_rows), BF16),
                pltpu.VMEM((2, batch, SB), F32),
                pltpu.VMEM((1, SB), F32),
                pltpu.VMEM((batch, SB), F32),
                pltpu.VMEM((1, SB), F32),
                dma((plane, 2)), dma((plane,)), dma, dma, dma((n_blocks,)), dma, dma, dma((2,)),
                dma((2,)), dma, dma((2,)), dma, dma((2,)), dma, dma((2,)), dma, dma((2,)), dma((2,)),
            ],
            compiler_params=pltpu.CompilerParams(has_side_effects=True, vmem_limit_bytes=48 * 1024 * 1024),
            cost_estimate=pl.CostEstimate(flops=2 * batch * (n_steps - 1) * plane * k_rows * cols,
                                          bytes_accessed=plane * k_rows * cols * 2, transcendentals=0),
        )(a_blk, emis.reshape(n_steps * batch, SB), first_raw, len_col, len_row)
        return ll[0, :batch], alpha

    return jax.shard_map(local_forward, mesh=mesh, in_specs=(P('rows', None, 'states'), P(vec_axes, None), P(vec_axes), P('seqs', None), P('seqs')), out_specs=(P('seqs'), P('seqs', vec_axes)), check_vma=False)
```

```python
import functools

import jax
import jax.numpy as jnp
from jax import lax
from jax.experimental import pallas as pl
from jax.experimental.pallas import tpu as pltpu
from jax.sharding import PartitionSpec as P

CHIPS = (4, 4, 4)
SB = 128
LIFT = 2.0 ** 64
LAG = 3
F32 = jnp.float32
BF16 = jnp.bfloat16


def ring_distance(offset, n):
    return min(offset, n - offset)


def forward_kernel(dims, n_steps, a_ref, e_ref, r0_ref, lencol_ref, lenrow_ref, alpha_ref, ll_ref,
                   a_loc, e_both, e_loc, w_loc, r_in, c_in, p_in, u_in, u_out, a_bf, alpha_acc, ll_acc, fin_alpha,
                   fin_ll, a_sem, a_send, e_pair, e_send, e_sem, r0_sem, r0_send, own_sem,
                   g_recv, g_send, c_recv, c_send, u_recv, u_send, p_recv, p_send, f_recv, f_send):
    nz, ny, nx = dims
    plane = nz * ny
    batch = r0_ref.shape[0]
    half = nx * SB
    block = plane
    rows = block * batch
    n_blocks = n_steps // block
    core = lax.axis_index('rows')
    me = lax.axis_index('states')
    zy = me // nx
    x = me % nx
    z = zy // ny
    y = zy % ny
    offsets = [(j, i) for j in range(nz) for i in range(ny)]
    rel = {o: k for k, o in enumerate(offsets)}
    mirror = [rel[(-j) % nz, (-i) % ny] for j, i in offsets]
    far = sorted(range(1, plane), key=lambda k: -(ring_distance(offsets[k][0], nz) + ring_distance(offsets[k][1], ny)))
    far_x = sorted(range(1, nx), key=lambda d: -ring_distance(d, nx))

    def plane_zy(k):
        return ((z + offsets[k][0]) % nz) * ny + (y + offsets[k][1]) % ny

    def plane_peer(k):
        return plane_zy(k) * nx + x

    def line_peer(d):
        return zy * nx + (x + d) % nx

    def remote(src, dst, send, recv, state, to=1):
        return pltpu.make_async_remote_copy(src_ref=src, dst_ref=dst, send_sem=send, recv_sem=recv,
                                            device_id={'rows': to, 'states': state},
                                            device_id_type=pl.DeviceIdType.MESH)

    def wait_bytes(ref, sem):
        pltpu.make_async_copy(ref, ref, sem).wait()

    def hand_over(h):
        return [remote(a_ref.at[pl.ds(plane_zy(k) * half, half)], a_loc.at[mirror[k], pl.ds(h * half, half)],
                       a_send.at[k], a_sem.at[mirror[k], h], plane_peer(k))
                for k in far + ([0] if h == 0 else [])]

    @pl.when(core == 0)
    def helper():
        first = remote(r0_ref, r_in.at[0, x, 0], r0_send, r0_sem, me)
        first.start()
        mine = pltpu.make_async_copy(e_ref, e_both.at[:, pl.ds(0, SB)], own_sem.at[0])
        mine.start()
        copies = hand_over(0)
        for copy in copies:
            copy.start()
        mine.wait()
        wait_bytes(e_both.at[:, pl.ds(SB, SB)], e_pair)

        def send_block(b, carry):
            src = e_both.at[pl.ds(b * rows, rows)]
            for k in [0] + far:
                remote(src, e_loc.at[b, mirror[k]], e_send, e_sem.at[b], plane_peer(k)).start()
            wait_bytes(e_loc.at[b], e_send)
            return carry

        lax.fori_loop(0, n_blocks, send_block, 0)
        first.wait_send()
        for copy in copies:
            copy.wait_send()
        wait_bytes(fin_alpha, f_recv.at[0])
        wait_bytes(fin_ll, f_recv.at[1])
        alpha_ref[...] = fin_alpha[...]
        ll_ref[...] = fin_ll[...]

    @pl.when(core == 1)
    def owner():
        eye = (lax.broadcasted_iota(jnp.int32, (batch, SB), 0)
               == lax.broadcasted_iota(jnp.int32, (batch, SB), 1))

        def as_row(tile):
            col = jnp.sum(tile, axis=1, keepdims=True)
            return jnp.sum(jnp.where(eye, col, 0.0), axis=0, keepdims=True)

        def as_col(row):
            return jnp.sum(jnp.where(eye, row, 0.0), axis=1, keepdims=True)

        def start_gather(slot):
            for d in far_x:
                remote(r_in.at[slot, x], r_in.at[slot, x], g_send, g_recv.at[slot], line_peer(d)).start()

        def start_plane_sums(slot):
            for k in far:
                remote(p_in.at[slot, zy], p_in.at[slot, zy], p_send, p_recv.at[slot], plane_peer(k)).start()

        others = pl.ds(0, nx - 1)
        peers = pl.ds(0, plane - 1)

        def finish_norm(slot):
            wait_bytes(p_in.at[slot, peers], p_recv.at[slot])
            c_in[slot, x] = jnp.sum(p_in[slot], axis=0)
            for d in far_x:
                remote(c_in.at[slot, x], c_in.at[slot, x], c_send, c_recv.at[slot], line_peer(d)).start()

        def norm(slot):
            wait_bytes(c_in.at[slot, others], c_recv.at[slot])
            c_row = jnp.sum(c_in[slot], axis=0)
            return c_row, 1.0 / as_col(c_row)

        def keep(t, slot, c_row, inv):
            active = t < lencol_ref[...]
            for h in range(2):
                alpha_acc[h] = jnp.where(active, r_in[slot, x, h] * inv, alpha_acc[h])
            ll_acc[...] = ll_acc[...] + jnp.where(t < lenrow_ref[...], jnp.log(c_row * (1.0 / LIFT)), 0.0)

        def add_w(b, k, fresh):
            part = lax.dot_general(e_loc[b, k], a_loc[k], (((1,), (1,)), ((), ())), preferred_element_type=F32)
            slot = b % 2
            w_loc[slot] = jnp.where(fresh, 0.0, w_loc[slot]) + part

        copies = hand_over(1)
        pair = remote(e_ref, e_both.at[:, pl.ds(SB, SB)], own_sem.at[0], e_pair, me, to=0)
        pair.start()
        for copy in copies:
            copy.start()
        own = pltpu.make_async_copy(a_ref.at[pl.ds(zy * half, half)], a_loc.at[0, pl.ds(half, half)], own_sem.at[1])
        own.start()
        alpha_acc[...] = jnp.zeros_like(alpha_acc)
        ll_acc[...] = jnp.zeros_like(ll_acc)
        r_in[0, x, 1] = r0_ref[...]
        wait_bytes(r0_ref, r0_sem)
        p_in[0, zy] = as_row(r_in[0, x, 0] + r_in[0, x, 1])
        start_plane_sums(0)
        start_gather(0)
        finish_norm(0)
        wait_bytes(p_in.at[0, peers], p_send)
        own.wait()
        for k in range(plane):
            for h in range(2):
                if h == 0 or k:
                    wait_bytes(a_loc.at[k, pl.ds(h * half, half)], a_sem.at[k, h])
        pair.wait_send()
        for copy in copies:
            copy.wait_send()
        wait_bytes(e_loc.at[0], e_sem.at[0])
        w_loc[...] = jnp.zeros_like(w_loc)

        def first_w(k, carry):
            add_w(0, k, False)
            return carry

        lax.fori_loop(0, plane, first_w, 0)

        def one_step(t, carry):
            cur = t % 2
            nxt = (t + 1) % 2
            b = t // block
            row = pl.ds((t % block) * batch, batch)
            c_row, inv = norm(cur)
            wait_bytes(r_in.at[cur, others], g_recv.at[cur])
            total = jnp.zeros((batch, SB), F32)
            for h in range(2):
                for src in range(nx):
                    cols = pl.ds(h * half + src * SB, SB)
                    tile = (r_in[cur, src, h] * inv).astype(BF16)
                    a_bf[:, cols] = tile
                    total = total + tile.astype(F32) * w_loc[b % 2, row, cols]
            ready = []

            def send_sum():
                k, part = ready.pop(0)
                for h in range(2):
                    u_out[k - 1, h] = part[:, h * SB:(h + 1) * SB]
                remote(u_out.at[k - 1], u_in.at[nxt, mirror[k] - 1], u_send, u_recv.at[nxt], plane_peer(k)).start()

            for i, k in enumerate(far + [0]):
                ready.append((k, jnp.dot(a_bf[...], a_loc[k], preferred_element_type=F32)))
                if len(ready) > LAG:
                    send_sum()
                if i == 4:
                    p_in[nxt, zy] = as_row(total)
                    start_plane_sums(nxt)
            while len(ready) > 1:
                send_sum()
            own_part = ready[0][1]
            wait_bytes(r_in.at[cur, others], g_send)
            wait_bytes(c_in.at[cur, others], c_send)
            keep(t, cur, c_row, inv)
            wait_bytes(u_in.at[nxt], u_recv.at[nxt])
            for h in range(2):
                u = own_part[:, h * SB:(h + 1) * SB]
                for k in range(plane - 1):
                    u = u + u_in[nxt, k, h]
                r_in[nxt, x, h] = u * e_loc[b, 0, row, pl.ds(h * SB, SB)].astype(F32)
            start_gather(nxt)
            finish_norm(nxt)

            @pl.when(b + 1 < n_blocks)
            def next_w():
                k = t % block
                later = b + 1

                @pl.when(k == 0)
                def arrived():
                    wait_bytes(e_loc.at[later], e_sem.at[later])

                add_w(later, k, k == 0)

            wait_bytes(u_out, u_send)
            wait_bytes(p_in.at[nxt, peers], p_send)
            return carry

        lax.fori_loop(0, n_steps - 1, one_step, 0)
        last = (n_steps - 1) % 2
        c_row, inv = norm(last)
        wait_bytes(r_in.at[last, others], g_recv.at[last])
        keep(n_steps - 1, last, c_row, inv)
        wait_bytes(r_in.at[last, others], g_send)
        wait_bytes(c_in.at[last, others], c_send)
        result = [remote(alpha_acc.at[0], fin_alpha, f_send.at[0], f_recv.at[0], me, to=0),
                  remote(ll_acc, fin_ll, f_send.at[1], f_recv.at[1], me, to=0)]
        for copy in result:
            copy.start()
        alpha_ref[...] = alpha_acc[1]
        ll_ref[...] = ll_acc[...]
        for copy in result:
            copy.wait_send()


def solution(mesh):
    vec_axes = ('rows', 'states')
    nz, ny, nx = CHIPS
    plane = nz * ny

    def local_forward(trans_blk, emit_blk, init_blk, tokens, lengths):
        batch, n_steps = tokens.shape
        cols = 2 * SB
        a_blk = trans_blk.reshape(trans_blk.shape[0], cols)
        emis = jnp.transpose(jnp.take(emit_blk, jnp.roll(tokens, -1, axis=1), axis=1), (2, 1, 0))
        emis = emis * jnp.asarray(LIFT, emis.dtype)
        first_raw = init_blk[None, :] * emis[-1].astype(F32)
        len_col = jnp.broadcast_to(lengths[:, None], (batch, SB))
        len_row = jnp.pad(lengths, (0, SB - batch))[None, :]
        vmem = pl.BlockSpec(memory_space=pltpu.VMEM)
        hbm = pl.BlockSpec(memory_space=pl.ANY)
        dma = pltpu.SemaphoreType.DMA
        k_rows = 2 * nx * SB
        block_rows = plane * batch
        n_blocks = n_steps // plane
        alpha, ll = pl.pallas_call(
            functools.partial(forward_kernel, CHIPS, n_steps),
            out_shape=(jax.ShapeDtypeStruct((batch, SB), F32), jax.ShapeDtypeStruct((1, SB), F32)),
            in_specs=[hbm, hbm, vmem, vmem, vmem],
            out_specs=(vmem, vmem),
            scratch_shapes=[
                pltpu.VMEM((plane, k_rows, cols), BF16),
                pltpu.VMEM((n_steps * batch, cols), BF16),
                pltpu.VMEM((n_blocks, plane, block_rows, cols), BF16),
                pltpu.VMEM((2, block_rows, k_rows), F32),
                pltpu.VMEM((2, nx, 2, batch, SB), F32),
                pltpu.VMEM((2, nx, 1, SB), F32),
                pltpu.VMEM((2, plane, 1, SB), F32),
                pltpu.VMEM((2, plane - 1, 2, batch, SB), F32),
                pltpu.VMEM((plane - 1, 2, batch, SB), F32),
                pltpu.VMEM((batch, k_rows), BF16),
                pltpu.VMEM((2, batch, SB), F32),
                pltpu.VMEM((1, SB), F32),
                pltpu.VMEM((batch, SB), F32),
                pltpu.VMEM((1, SB), F32),
                dma((plane, 2)), dma((plane,)), dma, dma, dma((n_blocks,)), dma, dma, dma((2,)),
                dma((2,)), dma, dma((2,)), dma, dma((2,)), dma, dma((2,)), dma, dma((2,)), dma((2,)),
            ],
            compiler_params=pltpu.CompilerParams(has_side_effects=True, vmem_limit_bytes=48 * 1024 * 1024),
            cost_estimate=pl.CostEstimate(flops=2 * batch * (n_steps - 1) * plane * k_rows * cols,
                                          bytes_accessed=plane * k_rows * cols * 2, transcendentals=0),
        )(a_blk, emis.reshape(n_steps * batch, SB), first_raw, len_col, len_row)
        return ll[0, :batch], alpha

    return jax.shard_map(local_forward, mesh=mesh, in_specs=(P('rows', None, 'states'), P(vec_axes, None), P(vec_axes), P('seqs', None), P('seqs')), out_specs=(P('seqs'), P('seqs', vec_axes)), check_vma=False)
```

```python
import functools

import jax
import jax.numpy as jnp
from jax import lax
from jax.experimental import pallas as pl
from jax.experimental.pallas import tpu as pltpu
from jax.sharding import PartitionSpec as P

CHIPS = (4, 4, 4)
SB = 128
LIFT = 2.0 ** 64
LAG = 3
P_AFTER = 2
F32 = jnp.float32
BF16 = jnp.bfloat16


def ring_distance(offset, n):
    return min(offset, n - offset)


def forward_kernel(dims, n_steps, a_ref, e_ref, r0_ref, lencol_ref, lenrow_ref, alpha_ref, ll_ref,
                   a_loc, e_both, e_loc, w_loc, r_in, c_in, p_in, u_in, u_out, a_bf, alpha_acc, ll_acc, fin_alpha,
                   fin_ll, a_sem, a_send, e_pair, e_send, e_sem, r0_sem, r0_send, own_sem,
                   g_recv, g_send, c_recv, c_send, u_recv, u_send, p_recv, p_send, f_recv, f_send):
    nz, ny, nx = dims
    plane = nz * ny
    batch = r0_ref.shape[0]
    half = nx * SB
    block = plane
    rows = block * batch
    n_blocks = n_steps // block
    core = lax.axis_index('rows')
    me = lax.axis_index('states')
    zy = me // nx
    x = me % nx
    z = zy // ny
    y = zy % ny
    offsets = [(j, i) for j in range(nz) for i in range(ny)]
    rel = {o: k for k, o in enumerate(offsets)}
    mirror = [rel[(-j) % nz, (-i) % ny] for j, i in offsets]
    far = sorted(range(1, plane), key=lambda k: -(ring_distance(offsets[k][0], nz) + ring_distance(offsets[k][1], ny)))
    far_x = sorted(range(1, nx), key=lambda d: -ring_distance(d, nx))

    def plane_zy(k):
        return ((z + offsets[k][0]) % nz) * ny + (y + offsets[k][1]) % ny

    def plane_peer(k):
        return plane_zy(k) * nx + x

    def line_peer(d):
        return zy * nx + (x + d) % nx

    def remote(src, dst, send, recv, state, to=1):
        return pltpu.make_async_remote_copy(src_ref=src, dst_ref=dst, send_sem=send, recv_sem=recv,
                                            device_id={'rows': to, 'states': state},
                                            device_id_type=pl.DeviceIdType.MESH)

    def wait_bytes(ref, sem):
        pltpu.make_async_copy(ref, ref, sem).wait()

    def hand_over(h):
        return [remote(a_ref.at[pl.ds(plane_zy(k) * half, half)], a_loc.at[mirror[k], pl.ds(h * half, half)],
                       a_send.at[k], a_sem.at[mirror[k], h], plane_peer(k))
                for k in far + ([0] if h == 0 else [])]

    @pl.when(core == 0)
    def helper():
        first = remote(r0_ref, r_in.at[0, x, 0], r0_send, r0_sem, me)
        first.start()
        mine = pltpu.make_async_copy(e_ref, e_both.at[:, pl.ds(0, SB)], own_sem.at[0])
        mine.start()
        copies = hand_over(0)
        for copy in copies:
            copy.start()
        mine.wait()
        wait_bytes(e_both.at[:, pl.ds(SB, SB)], e_pair)

        def send_block(b, carry):
            src = e_both.at[pl.ds(b * rows, rows)]
            for k in [0] + far:
                remote(src, e_loc.at[b, mirror[k]], e_send, e_sem.at[b], plane_peer(k)).start()
            wait_bytes(e_loc.at[b], e_send)
            return carry

        lax.fori_loop(0, n_blocks, send_block, 0)
        first.wait_send()
        for copy in copies:
            copy.wait_send()
        wait_bytes(fin_alpha, f_recv.at[0])
        wait_bytes(fin_ll, f_recv.at[1])
        alpha_ref[...] = fin_alpha[...]
        ll_ref[...] = fin_ll[...]

    @pl.when(core == 1)
    def owner():
        eye = (lax.broadcasted_iota(jnp.int32, (batch, SB), 0)
               == lax.broadcasted_iota(jnp.int32, (batch, SB), 1))

        def as_row(tile):
            col = jnp.sum(tile, axis=1, keepdims=True)
            return jnp.sum(jnp.where(eye, col, 0.0), axis=0, keepdims=True)

        def as_col(row):
            return jnp.sum(jnp.where(eye, row, 0.0), axis=1, keepdims=True)

        def start_gather(slot):
            for d in far_x:
                remote(r_in.at[slot, x], r_in.at[slot, x], g_send, g_recv.at[slot], line_peer(d)).start()

        def start_plane_sums(slot):
            for k in far:
                remote(p_in.at[slot, zy], p_in.at[slot, zy], p_send, p_recv.at[slot], plane_peer(k)).start()

        others = pl.ds(0, nx - 1)
        peers = pl.ds(0, plane - 1)

        def finish_norm(slot):
            wait_bytes(p_in.at[slot, peers], p_recv.at[slot])
            c_in[slot, x] = jnp.sum(p_in[slot], axis=0)
            for d in far_x:
                remote(c_in.at[slot, x], c_in.at[slot, x], c_send, c_recv.at[slot], line_peer(d)).start()

        def norm(slot):
            wait_bytes(c_in.at[slot, others], c_recv.at[slot])
            c_row = jnp.sum(c_in[slot], axis=0)
            return c_row, 1.0 / as_col(c_row)

        def keep(t, slot, c_row, inv):
            active = t < lencol_ref[...]
            for h in range(2):
                alpha_acc[h] = jnp.where(active, r_in[slot, x, h] * inv, alpha_acc[h])
            ll_acc[...] = ll_acc[...] + jnp.where(t < lenrow_ref[...], jnp.log(c_row * (1.0 / LIFT)), 0.0)

        def add_w(b, k, fresh):
            part = lax.dot_general(e_loc[b, k], a_loc[k], (((1,), (1,)), ((), ())), preferred_element_type=F32)
            slot = b % 2
            w_loc[slot] = jnp.where(fresh, 0.0, w_loc[slot]) + part

        copies = hand_over(1)
        pair = remote(e_ref, e_both.at[:, pl.ds(SB, SB)], own_sem.at[0], e_pair, me, to=0)
        pair.start()
        for copy in copies:
            copy.start()
        own = pltpu.make_async_copy(a_ref.at[pl.ds(zy * half, half)], a_loc.at[0, pl.ds(half, half)], own_sem.at[1])
        own.start()
        alpha_acc[...] = jnp.zeros_like(alpha_acc)
        ll_acc[...] = jnp.zeros_like(ll_acc)
        r_in[0, x, 1] = r0_ref[...]
        wait_bytes(r0_ref, r0_sem)
        p_in[0, zy] = as_row(r_in[0, x, 0] + r_in[0, x, 1])
        start_plane_sums(0)
        start_gather(0)
        finish_norm(0)
        wait_bytes(p_in.at[0, peers], p_send)
        own.wait()
        for k in range(plane):
            for h in range(2):
                if h == 0 or k:
                    wait_bytes(a_loc.at[k, pl.ds(h * half, half)], a_sem.at[k, h])
        pair.wait_send()
        for copy in copies:
            copy.wait_send()
        wait_bytes(e_loc.at[0], e_sem.at[0])
        w_loc[...] = jnp.zeros_like(w_loc)

        def first_w(k, carry):
            add_w(0, k, False)
            return carry

        lax.fori_loop(0, plane, first_w, 0)

        def one_step(t, carry):
            cur = t % 2
            nxt = (t + 1) % 2
            b = t // block
            row = pl.ds((t % block) * batch, batch)
            c_row, inv = norm(cur)
            wait_bytes(r_in.at[cur, others], g_recv.at[cur])
            total = jnp.zeros((batch, SB), F32)
            for h in range(2):
                for src in range(nx):
                    cols = pl.ds(h * half + src * SB, SB)
                    tile = (r_in[cur, src, h] * inv).astype(BF16)
                    a_bf[:, cols] = tile
                    total = total + tile.astype(F32) * w_loc[b % 2, row, cols]
            ready = []

            def send_sum():
                k, part = ready.pop(0)
                for h in range(2):
                    u_out[k - 1, h] = part[:, h * SB:(h + 1) * SB]
                remote(u_out.at[k - 1], u_in.at[nxt, mirror[k] - 1], u_send, u_recv.at[nxt], plane_peer(k)).start()

            for i, k in enumerate(far + [0]):
                ready.append((k, jnp.dot(a_bf[...], a_loc[k], preferred_element_type=F32)))
                if i == P_AFTER:
                    p_in[nxt, zy] = as_row(total)
                    start_plane_sums(nxt)
                if len(ready) > LAG:
                    send_sum()
            while len(ready) > 1:
                send_sum()
            own_part = ready[0][1]
            wait_bytes(r_in.at[cur, others], g_send)
            wait_bytes(c_in.at[cur, others], c_send)
            keep(t, cur, c_row, inv)
            finish_norm(nxt)
            wait_bytes(u_in.at[nxt], u_recv.at[nxt])
            for h in range(2):
                u = own_part[:, h * SB:(h + 1) * SB]
                for k in range(plane - 1):
                    u = u + u_in[nxt, k, h]
                r_in[nxt, x, h] = u * e_loc[b, 0, row, pl.ds(h * SB, SB)].astype(F32)
            start_gather(nxt)

            @pl.when(b + 1 < n_blocks)
            def next_w():
                k = t % block
                later = b + 1

                @pl.when(k == 0)
                def arrived():
                    wait_bytes(e_loc.at[later], e_sem.at[later])

                add_w(later, k, k == 0)

            wait_bytes(u_out, u_send)
            wait_bytes(p_in.at[nxt, peers], p_send)
            return carry

        lax.fori_loop(0, n_steps - 1, one_step, 0)
        last = (n_steps - 1) % 2
        c_row, inv = norm(last)
        wait_bytes(r_in.at[last, others], g_recv.at[last])
        keep(n_steps - 1, last, c_row, inv)
        wait_bytes(r_in.at[last, others], g_send)
        wait_bytes(c_in.at[last, others], c_send)
        result = [remote(alpha_acc.at[0], fin_alpha, f_send.at[0], f_recv.at[0], me, to=0),
                  remote(ll_acc, fin_ll, f_send.at[1], f_recv.at[1], me, to=0)]
        for copy in result:
            copy.start()
        alpha_ref[...] = alpha_acc[1]
        ll_ref[...] = ll_acc[...]
        for copy in result:
            copy.wait_send()


def solution(mesh):
    vec_axes = ('rows', 'states')
    nz, ny, nx = CHIPS
    plane = nz * ny

    def local_forward(trans_blk, emit_blk, init_blk, tokens, lengths):
        batch, n_steps = tokens.shape
        cols = 2 * SB
        a_blk = trans_blk.reshape(trans_blk.shape[0], cols)
        emis = jnp.transpose(jnp.take(emit_blk, jnp.roll(tokens, -1, axis=1), axis=1), (2, 1, 0))
        emis = emis * jnp.asarray(LIFT, emis.dtype)
        first_raw = init_blk[None, :] * emis[-1].astype(F32)
        len_col = jnp.broadcast_to(lengths[:, None], (batch, SB))
        len_row = jnp.pad(lengths, (0, SB - batch))[None, :]
        vmem = pl.BlockSpec(memory_space=pltpu.VMEM)
        hbm = pl.BlockSpec(memory_space=pl.ANY)
        dma = pltpu.SemaphoreType.DMA
        k_rows = 2 * nx * SB
        block_rows = plane * batch
        n_blocks = n_steps // plane
        alpha, ll = pl.pallas_call(
            functools.partial(forward_kernel, CHIPS, n_steps),
            out_shape=(jax.ShapeDtypeStruct((batch, SB), F32), jax.ShapeDtypeStruct((1, SB), F32)),
            in_specs=[hbm, hbm, vmem, vmem, vmem],
            out_specs=(vmem, vmem),
            scratch_shapes=[
                pltpu.VMEM((plane, k_rows, cols), BF16),
                pltpu.VMEM((n_steps * batch, cols), BF16),
                pltpu.VMEM((n_blocks, plane, block_rows, cols), BF16),
                pltpu.VMEM((2, block_rows, k_rows), F32),
                pltpu.VMEM((2, nx, 2, batch, SB), F32),
                pltpu.VMEM((2, nx, 1, SB), F32),
                pltpu.VMEM((2, plane, 1, SB), F32),
                pltpu.VMEM((2, plane - 1, 2, batch, SB), F32),
                pltpu.VMEM((plane - 1, 2, batch, SB), F32),
                pltpu.VMEM((batch, k_rows), BF16),
                pltpu.VMEM((2, batch, SB), F32),
                pltpu.VMEM((1, SB), F32),
                pltpu.VMEM((batch, SB), F32),
                pltpu.VMEM((1, SB), F32),
                dma((plane, 2)), dma((plane,)), dma, dma, dma((n_blocks,)), dma, dma, dma((2,)),
                dma((2,)), dma, dma((2,)), dma, dma((2,)), dma, dma((2,)), dma, dma((2,)), dma((2,)),
            ],
            compiler_params=pltpu.CompilerParams(has_side_effects=True, vmem_limit_bytes=48 * 1024 * 1024),
            cost_estimate=pl.CostEstimate(flops=2 * batch * (n_steps - 1) * plane * k_rows * cols,
                                          bytes_accessed=plane * k_rows * cols * 2, transcendentals=0),
        )(a_blk, emis.reshape(n_steps * batch, SB), first_raw, len_col, len_row)
        return ll[0, :batch], alpha

    return jax.shard_map(local_forward, mesh=mesh, in_specs=(P('rows', None, 'states'), P(vec_axes, None), P(vec_axes), P('seqs', None), P('seqs')), out_specs=(P('seqs'), P('seqs', vec_axes)), check_vma=False)
```

```python
import functools

import jax
import jax.numpy as jnp
from jax import lax
from jax.experimental import pallas as pl
from jax.experimental.pallas import tpu as pltpu
from jax.sharding import PartitionSpec as P

CHIPS = (4, 4, 4)
SB = 128
LIFT = 2.0 ** 64
LAG = 3
P_AFTER = 2
BLOCK = 8
AHEAD = 6
F32 = jnp.float32
BF16 = jnp.bfloat16


def ring_distance(offset, n):
    return min(offset, n - offset)


def forward_kernel(dims, n_steps, block, a_ref, e_ref, r0_ref, len_ref, alpha_ref, ll_ref,
                   a_loc, e_both, e_loc, w_loc, r_in, c_in, p_in, u_in, u_out, a_bf, len_col, alpha_acc, ll_acc, fin_alpha,
                   fin_ll, tick, a_sem, a_send, e_pair, e_send, e_sem, r0_sem, r0_send, own_sem,
                   g_recv, g_send, c_recv, c_send, u_recv, u_send, p_recv, p_send, f_recv, f_send):
    nz, ny, nx = dims
    plane = nz * ny
    batch = r0_ref.shape[0]
    half = nx * SB
    rows = block * batch
    per_step = plane // block
    n_blocks = n_steps // block
    core = lax.axis_index('rows')
    me = lax.axis_index('states')
    zy = me // nx
    x = me % nx
    z = zy // ny
    y = zy % ny
    offsets = [(j, i) for j in range(nz) for i in range(ny)]
    rel = {o: k for k, o in enumerate(offsets)}
    mirror = [rel[(-j) % nz, (-i) % ny] for j, i in offsets]
    far = sorted(range(1, plane), key=lambda k: -(ring_distance(offsets[k][0], nz) + ring_distance(offsets[k][1], ny)))
    far_x = sorted(range(1, nx), key=lambda d: -ring_distance(d, nx))

    def plane_zy(k):
        return ((z + offsets[k][0]) % nz) * ny + (y + offsets[k][1]) % ny

    def plane_peer(k):
        return plane_zy(k) * nx + x

    def line_peer(d):
        return zy * nx + (x + d) % nx

    def remote(src, dst, send, recv, state, to=1):
        return pltpu.make_async_remote_copy(src_ref=src, dst_ref=dst, send_sem=send, recv_sem=recv,
                                            device_id={'rows': to, 'states': state},
                                            device_id_type=pl.DeviceIdType.MESH)

    def wait_bytes(ref, sem):
        pltpu.make_async_copy(ref, ref, sem).wait()

    def slot_peer(j):
        return (((z - j // ny + nz) % nz) * ny + (y - j % ny + ny) % ny) * nx + x

    def a_copy(h, j):
        peer = slot_peer(j)
        return remote(a_ref.at[pl.ds((peer // nx) * half, half)], a_loc.at[j, pl.ds(h * half, half)],
                      a_send.at[j], a_sem.at[j, h], peer)

    def e_copy(b, j):
        return remote(e_both.at[pl.ds(b * rows, rows)], e_loc.at[b, j], e_send, e_sem.at[b % 2, j], slot_peer(j))

    barrier = pltpu.get_barrier_semaphore()

    def announce(state, to):
        pl.semaphore_signal(barrier, inc=1, device_id={'rows': to, 'states': state}, device_id_type=pl.DeviceIdType.MESH)

    @pl.when(core == 0)
    def helper():
        announce(me, 1)
        pl.semaphore_wait(barrier, plane)
        first = remote(r0_ref, r_in.at[0, x, 0], r0_send, r0_sem, me)
        first.start()
        mine = pltpu.make_async_copy(e_ref, e_both.at[:, pl.ds(0, SB)], own_sem.at[0])
        mine.start()
        copies = [a_copy(0, j) for j in range(plane)]
        copies[0].start()
        copies[1].start()
        mine.wait()
        wait_bytes(e_both.at[:, pl.ds(SB, SB)], e_pair)
        e_copy(0, 0).start()
        e_copy(0, 1).start()
        for j in range(2, plane):
            copies[j].start()
            e_copy(0, j).start()
        wait_bytes(e_loc.at[0], e_send)

        def send_part(i, carry):
            @pl.when(i >= AHEAD)
            def paced():
                pl.semaphore_wait(tick, 1)

            for n in range(per_step):
                e_copy(1 + i // block, (i % block) * per_step + n).start()
            wait_bytes(e_loc.at[0, pl.ds(0, per_step)], e_send)
            return carry

        lax.fori_loop(0, n_steps - block, send_part, 0)
        first.wait_send()
        for copy in copies:
            copy.wait_send()
        wait_bytes(fin_alpha, f_recv.at[0])
        wait_bytes(fin_ll, f_recv.at[1])
        alpha_ref[...] = fin_alpha[...]
        ll_ref[...] = fin_ll[...]

    @pl.when(core == 1)
    def owner():
        eye = (lax.broadcasted_iota(jnp.int32, (batch, SB), 0)
               == lax.broadcasted_iota(jnp.int32, (batch, SB), 1))

        def as_row(tile):
            col = jnp.sum(tile, axis=1, keepdims=True)
            return jnp.sum(jnp.where(eye, col, 0.0), axis=0, keepdims=True)

        def as_col(row):
            return jnp.sum(jnp.where(eye, row, 0.0), axis=1, keepdims=True)

        def start_gather(slot):
            for d in far_x:
                remote(r_in.at[slot, x], r_in.at[slot, x], g_send, g_recv.at[slot], line_peer(d)).start()

        def start_plane_sums(slot):
            for k in far:
                remote(p_in.at[slot, zy], p_in.at[slot, zy], p_send, p_recv.at[slot], plane_peer(k)).start()

        others = pl.ds(0, nx - 1)
        peers = pl.ds(0, plane - 1)

        def finish_norm(slot):
            wait_bytes(p_in.at[slot, peers], p_recv.at[slot])
            c_in[slot, x] = jnp.sum(p_in[slot], axis=0)
            for d in far_x:
                remote(c_in.at[slot, x], c_in.at[slot, x], c_send, c_recv.at[slot], line_peer(d)).start()

        def norm(slot):
            wait_bytes(c_in.at[slot, others], c_recv.at[slot])
            c_row = jnp.sum(c_in[slot], axis=0)
            return c_row, 1.0 / as_col(c_row)

        def keep(t, slot, c_row, inv):
            now = lax.convert_element_type(t, F32)
            active = now < len_col[...]
            for h in range(2):
                alpha_acc[h] = jnp.where(active, r_in[slot, x, h] * inv, alpha_acc[h])
            ll_acc[...] = ll_acc[...] + jnp.where(now < len_ref[...], jnp.log(c_row * (1.0 / LIFT)), 0.0)

        def add_w(b, k, fresh):
            part = lax.dot_general(e_loc[b, k], a_loc[k], (((1,), (1,)), ((), ())), preferred_element_type=F32)
            slot = b % 2
            w_loc[slot] = jnp.where(fresh, 0.0, w_loc[slot]) + part

        for k in far:
            announce(plane_peer(k), 1)
        for d in far_x:
            announce(line_peer(d), 1)
        for k in range(plane):
            announce(plane_peer(k), 0)
        pl.semaphore_wait(barrier, plane + nx - 1)
        pair = remote(e_ref, e_both.at[:, pl.ds(SB, SB)], own_sem.at[0], e_pair, me, to=0)
        pair.start()
        copies = [a_copy(1, j) for j in range(1, plane)]
        for copy in copies:
            copy.start()
        own = pltpu.make_async_copy(a_ref.at[pl.ds(zy * half, half)], a_loc.at[0, pl.ds(half, half)], own_sem.at[1])
        own.start()
        alpha_acc[...] = jnp.zeros_like(alpha_acc)
        ll_acc[...] = jnp.zeros_like(ll_acc)
        w_loc[...] = jnp.zeros_like(w_loc)
        len_col[...] = jnp.broadcast_to(as_col(len_ref[...]), (batch, SB))
        r_in[0, x, 1] = r0_ref[...]
        wait_bytes(r0_ref, r0_sem)
        p_in[0, zy] = as_row(r_in[0, x, 0] + r_in[0, x, 1])
        start_plane_sums(0)
        start_gather(0)
        finish_norm(0)
        wait_bytes(p_in.at[0, peers], p_send)
        own.wait()

        def first_w(k, carry):
            wait_bytes(a_loc.at[k, pl.ds(0, half)], a_sem.at[k, 0])

            @pl.when(k > 0)
            def from_owner():
                wait_bytes(a_loc.at[k, pl.ds(half, half)], a_sem.at[k, 1])

            wait_bytes(e_loc.at[0, k], e_sem.at[0, k])
            add_w(0, k, False)
            return carry

        lax.fori_loop(0, plane, first_w, 0)
        pair.wait_send()
        for copy in copies:
            copy.wait_send()

        def one_step(t, carry):
            cur = t % 2
            nxt = (t + 1) % 2
            b = t // block
            row = pl.ds((t % block) * batch, batch)
            c_row, inv = norm(cur)
            wait_bytes(r_in.at[cur, others], g_recv.at[cur])
            total = jnp.zeros((batch, SB), F32)
            for h in range(2):
                for src in range(nx):
                    cols = pl.ds(h * half + src * SB, SB)
                    tile = (r_in[cur, src, h] * inv).astype(BF16)
                    a_bf[:, cols] = tile
                    total = total + tile.astype(F32) * w_loc[b % 2, row, cols]
            ready = []

            def send_sum():
                k, part = ready.pop(0)
                for h in range(2):
                    u_out[k - 1, h] = part[:, h * SB:(h + 1) * SB]
                remote(u_out.at[k - 1], u_in.at[nxt, mirror[k] - 1], u_send, u_recv.at[nxt], plane_peer(k)).start()

            for i, k in enumerate(far + [0]):
                ready.append((k, jnp.dot(a_bf[...], a_loc[k], preferred_element_type=F32)))
                if i == P_AFTER:
                    p_in[nxt, zy] = as_row(total)
                    start_plane_sums(nxt)
                if len(ready) > LAG:
                    send_sum()
            while len(ready) > 1:
                send_sum()
            own_part = ready[0][1]
            wait_bytes(r_in.at[cur, others], g_send)
            wait_bytes(c_in.at[cur, others], c_send)
            keep(t, cur, c_row, inv)
            finish_norm(nxt)
            wait_bytes(u_in.at[nxt], u_recv.at[nxt])
            for h in range(2):
                u = own_part[:, h * SB:(h + 1) * SB]
                for k in range(plane - 1):
                    u = u + u_in[nxt, k, h]
                r_in[nxt, x, h] = u * e_loc[b, 0, row, pl.ds(h * SB, SB)].astype(F32)
            start_gather(nxt)

            @pl.when(t < n_steps - block - AHEAD)
            def go_on():
                pl.semaphore_signal(tick, inc=1, device_id={'rows': 0, 'states': me},
                                    device_id_type=pl.DeviceIdType.MESH)

            @pl.when(b + 1 < n_blocks)
            def next_w():
                later = b + 1
                for n in range(per_step):
                    k = (t % block) * per_step + n
                    wait_bytes(e_loc.at[later, k], e_sem.at[later % 2, k])
                    add_w(later, k, k == 0)

            wait_bytes(u_out, u_send)
            wait_bytes(p_in.at[nxt, peers], p_send)
            return carry

        lax.fori_loop(0, n_steps - 1, one_step, 0)
        last = (n_steps - 1) % 2
        c_row, inv = norm(last)
        wait_bytes(r_in.at[last, others], g_recv.at[last])
        keep(n_steps - 1, last, c_row, inv)
        wait_bytes(r_in.at[last, others], g_send)
        wait_bytes(c_in.at[last, others], c_send)
        result = [remote(alpha_acc.at[0], fin_alpha, f_send.at[0], f_recv.at[0], me, to=0),
                  remote(ll_acc, fin_ll, f_send.at[1], f_recv.at[1], me, to=0)]
        for copy in result:
            copy.start()
        alpha_ref[...] = alpha_acc[1]
        ll_ref[...] = ll_acc[...]
        for copy in result:
            copy.wait_send()


def solution(mesh):
    vec_axes = ('rows', 'states')
    nz, ny, nx = CHIPS
    plane = nz * ny

    def local_forward(trans_blk, emit_blk, init_blk, tokens, lengths):
        batch, n_steps = tokens.shape
        cols = 2 * SB
        a_blk = trans_blk.reshape(trans_blk.shape[0], cols)
        emis = jnp.transpose(emit_blk.at[:, jnp.roll(tokens, -1, axis=1)].get(mode='promise_in_bounds'), (2, 1, 0))
        emis = emis * jnp.asarray(LIFT, emis.dtype)
        first_raw = init_blk[None, :] * emis[-1].astype(F32)
        len_row = jnp.pad(lengths.astype(F32), (0, SB - batch))[None, :]
        vmem = pl.BlockSpec(memory_space=pltpu.VMEM)
        hbm = pl.BlockSpec(memory_space=pl.ANY)
        dma = pltpu.SemaphoreType.DMA
        k_rows = 2 * nx * SB
        block = min(BLOCK, plane)
        block_rows = block * batch
        n_blocks = n_steps // block
        alpha, ll = pl.pallas_call(
            functools.partial(forward_kernel, CHIPS, n_steps, block),
            out_shape=(jax.ShapeDtypeStruct((batch, SB), F32), jax.ShapeDtypeStruct((1, SB), F32)),
            in_specs=[hbm, hbm, vmem, vmem],
            out_specs=(vmem, vmem),
            scratch_shapes=[
                pltpu.VMEM((plane, k_rows, cols), BF16),
                pltpu.VMEM((n_steps * batch, cols), BF16),
                pltpu.VMEM((n_blocks, plane, block_rows, cols), BF16),
                pltpu.VMEM((2, block_rows, k_rows), F32),
                pltpu.VMEM((2, nx, 2, batch, SB), F32),
                pltpu.VMEM((2, nx, 1, SB), F32),
                pltpu.VMEM((2, plane, 1, SB), F32),
                pltpu.VMEM((2, plane - 1, 2, batch, SB), F32),
                pltpu.VMEM((plane - 1, 2, batch, SB), F32),
                pltpu.VMEM((batch, k_rows), BF16),
                pltpu.VMEM((batch, SB), F32),
                pltpu.VMEM((2, batch, SB), F32),
                pltpu.VMEM((1, SB), F32),
                pltpu.VMEM((batch, SB), F32),
                pltpu.VMEM((1, SB), F32),
                pltpu.SemaphoreType.REGULAR,
                dma((plane, 2)), dma((plane,)), dma, dma, dma((2, plane)), dma, dma, dma((2,)),
                dma((2,)), dma, dma((2,)), dma, dma((2,)), dma, dma((2,)), dma, dma((2,)), dma((2,)),
            ],
            compiler_params=pltpu.CompilerParams(collective_id=0, has_side_effects=True, vmem_limit_bytes=48 * 1024 * 1024),
            cost_estimate=pl.CostEstimate(flops=2 * batch * (n_steps - 1) * plane * k_rows * cols,
                                          bytes_accessed=plane * k_rows * cols * 2, transcendentals=0),
        )(a_blk, emis.reshape(n_steps * batch, SB), first_raw, len_row)
        return ll[0, :batch], alpha

    return jax.shard_map(local_forward, mesh=mesh, in_specs=(P('rows', None, 'states'), P(vec_axes, None), P(vec_axes), P('seqs', None), P('seqs')), out_specs=(P('seqs'), P('seqs', vec_axes)), check_vma=False)
```

```python
import functools

import jax
import jax.numpy as jnp
from jax import lax
from jax.experimental import pallas as pl
from jax.experimental.pallas import tpu as pltpu
from jax.sharding import PartitionSpec as P

CHIPS = (4, 4, 4)
SB = 128
LIFT = 2.0 ** 64
LAG = 1
P_AFTER = 1
BLOCK = 8
AHEAD = 6
F32 = jnp.float32
BF16 = jnp.bfloat16


def ring_distance(offset, n):
    return min(offset, n - offset)


def forward_kernel(dims, n_steps, block, a_ref, e_ref, r0_ref, len_ref, alpha_ref, ll_ref,
                   a_loc, e_both, e_loc, w_loc, r_in, c_in, p_in, u_in, u_out, a_bf, len_col, alpha_acc, ll_acc,
                   fin_alpha, fin_ll, tick, a_sem, a_send, e_pair, e_send, e_sem, r0_sem, r0_send, own_sem,
                   g_recv, g_send, c_recv, c_send, u_recv, u_send, p_recv, p_send, f_recv, f_send):
    nz, ny, nx = dims
    n_sum, n_gather = 2 * nz, 2 * nx
    batch = r0_ref.shape[0]
    half = n_gather * SB
    rows = block * batch
    n_blocks = n_steps // block
    per_step = n_sum // block
    core = lax.axis_index('rows')
    me = lax.axis_index('states')
    z = me // (ny * nx)
    y = (me // nx) % ny
    x = me % nx
    group = me // n_gather
    place = me % n_gather
    c_place = (((y + 1) // 2) % 2) * nx + x
    far = sorted(range(1, n_sum), key=lambda k: -(ring_distance(k // 2, nz) + k % 2))
    far_gather = sorted(((f, d) for f in range(2) for d in range(nx) if f or d),
                        key=lambda o: -(o[0] + ring_distance(o[1], nx)))

    def sum_peer(k, sign=1):
        flip = k % 2
        return ((z + sign * (k // 2) + nz) % nz) * ny * nx + (y + flip * (ny - 1 - 2 * y)) * nx + x

    def mirror(k):
        return ((nz - k // 2) % nz) * 2 + k % 2

    def gather_peer(flip, d):
        return (me // (ny * nx)) * ny * nx + (y + flip * (1 - 2 * (y % 2))) * nx + (x + d) % nx

    def remote(src, dst, send, recv, state, to=1):
        return pltpu.make_async_remote_copy(src_ref=src, dst_ref=dst, send_sem=send, recv_sem=recv,
                                            device_id={'rows': to, 'states': state},
                                            device_id_type=pl.DeviceIdType.MESH)

    def wait_bytes(ref, sem):
        pltpu.make_async_copy(ref, ref, sem).wait()

    def a_copy(h, k):
        peer = sum_peer(k, -1)
        return remote(a_ref.at[pl.ds((peer // n_gather) * half, half)], a_loc.at[k, pl.ds(h * half, half)],
                      a_send.at[k], a_sem.at[k, h], peer)

    def e_copy(b, k):
        return remote(e_both.at[pl.ds(b * rows, rows)], e_loc.at[b, k], e_send, e_sem.at[b % 2, k], sum_peer(k, -1))

    barrier = pltpu.get_barrier_semaphore()

    def announce(state, to):
        pl.semaphore_signal(barrier, inc=1, device_id={'rows': to, 'states': state}, device_id_type=pl.DeviceIdType.MESH)

    @pl.when(core == 0)
    def helper():
        announce(me, 1)
        pl.semaphore_wait(barrier, n_sum)
        first = remote(r0_ref, r_in.at[0, place, 0], r0_send, r0_sem, me)
        first.start()
        mine = pltpu.make_async_copy(e_ref, e_both.at[:, pl.ds(0, SB)], own_sem.at[0])
        mine.start()
        copies = [a_copy(0, k) for k in range(n_sum)]
        copies[0].start()
        copies[1].start()
        mine.wait()
        wait_bytes(e_both.at[:, pl.ds(SB, SB)], e_pair)
        e_copy(0, 0).start()
        e_copy(0, 1).start()
        for k in range(2, n_sum):
            copies[k].start()
            e_copy(0, k).start()
        wait_bytes(e_loc.at[0], e_send)

        def send_part(i, carry):
            @pl.when(i >= AHEAD)
            def paced():
                pl.semaphore_wait(tick, 1)

            for n in range(per_step):
                e_copy(1 + i // block, (i % block) * per_step + n).start()
            wait_bytes(e_loc.at[0, pl.ds(0, per_step)], e_send)
            return carry

        lax.fori_loop(0, n_steps - block, send_part, 0)
        first.wait_send()
        for copy in copies:
            copy.wait_send()
        wait_bytes(fin_alpha, f_recv.at[0])
        wait_bytes(fin_ll, f_recv.at[1])
        alpha_ref[...] = fin_alpha[...]
        ll_ref[...] = fin_ll[...]

    @pl.when(core == 1)
    def owner():
        eye = (lax.broadcasted_iota(jnp.int32, (batch, SB), 0)
               == lax.broadcasted_iota(jnp.int32, (batch, SB), 1))

        def as_row(tile):
            col = jnp.sum(tile, axis=1, keepdims=True)
            return jnp.sum(jnp.where(eye, col, 0.0), axis=0, keepdims=True)

        def as_col(row):
            return jnp.sum(jnp.where(eye, row, 0.0), axis=1, keepdims=True)

        def start_gather(slot):
            for o in far_gather:
                remote(r_in.at[slot, place], r_in.at[slot, place], g_send, g_recv.at[slot], gather_peer(*o)).start()

        def start_parts(slot):
            for k in far:
                remote(p_in.at[slot, group], p_in.at[slot, group], p_send, p_recv.at[slot], sum_peer(k)).start()

        others = pl.ds(0, n_gather - 1)
        peers = pl.ds(0, n_sum - 1)

        def finish_norm(slot):
            wait_bytes(p_in.at[slot, peers], p_recv.at[slot])
            c_in[slot, c_place] = jnp.sum(p_in[slot], axis=0)
            for o in far_gather:
                remote(c_in.at[slot, c_place], c_in.at[slot, c_place], c_send, c_recv.at[slot], gather_peer(*o)).start()

        def norm(slot):
            wait_bytes(c_in.at[slot, others], c_recv.at[slot])
            c_row = jnp.sum(c_in[slot], axis=0)
            c_col = as_col(c_row)
            inv = 1.0 / c_col
            return c_row, inv * (2.0 - c_col * inv)

        def keep(t, slot, c_row, inv):
            now = lax.convert_element_type(t, F32)
            active = now < len_col[...]
            for h in range(2):
                alpha_acc[h] = jnp.where(active, r_in[slot, place, h] * inv, alpha_acc[h])
            ll_acc[...] = ll_acc[...] + jnp.where(now < len_ref[...], jnp.log(c_row * (1.0 / LIFT)), 0.0)

        def add_w(b, k, fresh):
            part = lax.dot_general(e_loc[b, k], a_loc[k], (((1,), (1,)), ((), ())), preferred_element_type=F32)
            slot = b % 2
            w_loc[slot] = jnp.where(fresh, 0.0, w_loc[slot]) + part

        for k in far:
            announce(sum_peer(k), 1)
        for o in far_gather:
            announce(gather_peer(*o), 1)
        for k in range(n_sum):
            announce(sum_peer(k), 0)
        pl.semaphore_wait(barrier, n_sum + n_gather - 1)
        pair = remote(e_ref, e_both.at[:, pl.ds(SB, SB)], own_sem.at[0], e_pair, me, to=0)
        pair.start()
        copies = [a_copy(1, k) for k in range(1, n_sum)]
        for copy in copies:
            copy.start()
        own = pltpu.make_async_copy(a_ref.at[pl.ds(group * half, half)], a_loc.at[0, pl.ds(half, half)], own_sem.at[1])
        own.start()
        alpha_acc[...] = jnp.zeros_like(alpha_acc)
        ll_acc[...] = jnp.zeros_like(ll_acc)
        w_loc[...] = jnp.zeros_like(w_loc)
        len_col[...] = jnp.broadcast_to(as_col(len_ref[...]), (batch, SB))
        r_in[0, place, 1] = r0_ref[...]
        wait_bytes(r0_ref, r0_sem)
        p_in[0, group] = as_row(r_in[0, place, 0] + r_in[0, place, 1])
        start_parts(0)
        start_gather(0)
        finish_norm(0)
        wait_bytes(p_in.at[0, peers], p_send)
        own.wait()

        def first_w(k, carry):
            wait_bytes(a_loc.at[k, pl.ds(0, half)], a_sem.at[k, 0])

            @pl.when(k > 0)
            def from_owner():
                wait_bytes(a_loc.at[k, pl.ds(half, half)], a_sem.at[k, 1])

            wait_bytes(e_loc.at[0, k], e_sem.at[0, k])
            add_w(0, k, False)
            return carry

        lax.fori_loop(0, n_sum, first_w, 0)
        pair.wait_send()
        for copy in copies:
            copy.wait_send()

        def one_step(t, carry):
            cur = t % 2
            nxt = (t + 1) % 2
            b = t // block
            row = pl.ds((t % block) * batch, batch)
            c_row, inv = norm(cur)
            wait_bytes(r_in.at[cur, others], g_recv.at[cur])
            total = jnp.zeros((batch, SB), F32)
            for h in range(2):
                for src in range(n_gather):
                    cols = pl.ds(h * half + src * SB, SB)
                    tile = (r_in[cur, src, h] * inv).astype(BF16)
                    a_bf[:, cols] = tile
                    total = total + tile.astype(F32) * w_loc[b % 2, row, cols]
            unit = jnp.where(t >= 0, jnp.float32(1.0), jnp.float32(0.0))
            ready = []

            def send_sum():
                k, part = ready.pop(0)
                for h in range(2):
                    u_out[k - 1, h] = part[:, h * SB:(h + 1) * SB]
                remote(u_out.at[k - 1], u_in.at[nxt, mirror(k) - 1], u_send, u_recv.at[nxt], sum_peer(k)).start()

            for i, k in enumerate(far + [0]):
                low = jnp.dot(a_bf[:, :half], a_loc[k, :half], preferred_element_type=F32)
                high = jnp.dot(a_bf[:, half:], a_loc[k, half:], preferred_element_type=F32)
                ready.append((k, low * unit + high))
                if i == P_AFTER:
                    p_in[nxt, group] = as_row(total)
                    start_parts(nxt)
                if len(ready) > LAG:
                    send_sum()
            while len(ready) > 1:
                send_sum()
            own_part = ready[0][1]
            wait_bytes(r_in.at[cur, others], g_send)
            wait_bytes(c_in.at[cur, others], c_send)
            keep(t, cur, c_row, inv)
            finish_norm(nxt)
            wait_bytes(u_in.at[nxt], u_recv.at[nxt])
            for h in range(2):
                parts = [own_part[:, h * SB:(h + 1) * SB]] + [u_in[nxt, k, h] for k in range(n_sum - 1)]
                while len(parts) > 1:
                    parts = [parts[i] + parts[i + 1] for i in range(0, len(parts), 2)]
                r_in[nxt, place, h] = parts[0] * e_loc[b, 0, row, pl.ds(h * SB, SB)].astype(F32)
            start_gather(nxt)

            @pl.when(t < n_steps - block - AHEAD)
            def go_on():
                pl.semaphore_signal(tick, inc=1, device_id={'rows': 0, 'states': me},
                                    device_id_type=pl.DeviceIdType.MESH)

            @pl.when(b + 1 < n_blocks)
            def next_w():
                later = b + 1
                for n in range(per_step):
                    k = (t % block) * per_step + n
                    wait_bytes(e_loc.at[later, k], e_sem.at[later % 2, k])
                    add_w(later, k, k == 0)

            wait_bytes(u_out, u_send)
            wait_bytes(p_in.at[nxt, peers], p_send)
            return carry

        lax.fori_loop(0, n_steps - 1, one_step, 0)
        last = (n_steps - 1) % 2
        c_row, inv = norm(last)
        wait_bytes(r_in.at[last, others], g_recv.at[last])
        keep(n_steps - 1, last, c_row, inv)
        wait_bytes(r_in.at[last, others], g_send)
        wait_bytes(c_in.at[last, others], c_send)
        result = [remote(alpha_acc.at[0], fin_alpha, f_send.at[0], f_recv.at[0], me, to=0),
                  remote(ll_acc, fin_ll, f_send.at[1], f_recv.at[1], me, to=0)]
        for copy in result:
            copy.start()
        alpha_ref[...] = alpha_acc[1]
        ll_ref[...] = ll_acc[...]
        for copy in result:
            copy.wait_send()


def solution(mesh):
    vec_axes = ('rows', 'states')
    nz, ny, nx = CHIPS
    n_sum, n_gather = 2 * nz, 2 * nx

    def local_forward(trans_blk, emit_blk, init_blk, tokens, lengths):
        batch, n_steps = tokens.shape
        cols = 2 * SB
        a_blk = trans_blk.reshape(trans_blk.shape[0], cols)
        emis = jnp.transpose(emit_blk.at[:, jnp.roll(tokens, -1, axis=1)].get(mode='promise_in_bounds'), (2, 1, 0))
        emis = emis * jnp.asarray(LIFT, emis.dtype)
        first_raw = init_blk[None, :] * emis[-1].astype(F32)
        len_row = jnp.pad(lengths.astype(F32), (0, SB - batch))[None, :]
        vmem = pl.BlockSpec(memory_space=pltpu.VMEM)
        hbm = pl.BlockSpec(memory_space=pl.ANY)
        dma = pltpu.SemaphoreType.DMA
        k_rows = 2 * n_gather * SB
        block = min(BLOCK, n_sum)
        block_rows = block * batch
        n_blocks = n_steps // block
        alpha, ll = pl.pallas_call(
            functools.partial(forward_kernel, CHIPS, n_steps, block),
            out_shape=(jax.ShapeDtypeStruct((batch, SB), F32), jax.ShapeDtypeStruct((1, SB), F32)),
            in_specs=[hbm, hbm, vmem, vmem],
            out_specs=(vmem, vmem),
            scratch_shapes=[
                pltpu.VMEM((n_sum, k_rows, cols), BF16),
                pltpu.VMEM((n_steps * batch, cols), BF16),
                pltpu.VMEM((n_blocks, n_sum, block_rows, cols), BF16),
                pltpu.VMEM((2, block_rows, k_rows), F32),
                pltpu.VMEM((2, n_gather, 2, batch, SB), F32),
                pltpu.VMEM((2, n_gather, 1, SB), F32),
                pltpu.VMEM((2, n_sum, 1, SB), F32),
                pltpu.VMEM((2, n_sum - 1, 2, batch, SB), F32),
                pltpu.VMEM((n_sum - 1, 2, batch, SB), F32),
                pltpu.VMEM((batch, k_rows), BF16),
                pltpu.VMEM((batch, SB), F32),
                pltpu.VMEM((2, batch, SB), F32),
                pltpu.VMEM((1, SB), F32),
                pltpu.VMEM((batch, SB), F32),
                pltpu.VMEM((1, SB), F32),
                pltpu.SemaphoreType.REGULAR,
                dma((n_sum, 2)), dma((n_sum,)), dma, dma, dma((2, n_sum)), dma, dma, dma((2,)),
                dma((2,)), dma, dma((2,)), dma, dma((2,)), dma, dma((2,)), dma, dma((2,)), dma((2,)),
            ],
            compiler_params=pltpu.CompilerParams(collective_id=0, has_side_effects=True,
                                                 vmem_limit_bytes=48 * 1024 * 1024),
            cost_estimate=pl.CostEstimate(flops=2 * batch * (n_steps - 1) * n_sum * k_rows * cols,
                                          bytes_accessed=n_sum * k_rows * cols * 2, transcendentals=0),
        )(a_blk, emis.reshape(n_steps * batch, SB), first_raw, len_row)
        return ll[0, :batch], alpha

    return jax.shard_map(local_forward, mesh=mesh, in_specs=(P('rows', None, 'states'), P(vec_axes, None), P(vec_axes), P('seqs', None), P('seqs')), out_specs=(P('seqs'), P('seqs', vec_axes)), check_vma=False)
```

```python
import functools

import jax
import jax.numpy as jnp
from jax import lax
from jax.experimental import pallas as pl
from jax.experimental.pallas import tpu as pltpu
from jax.sharding import PartitionSpec as P

CHIPS = (4, 4, 4)
SB = 128
LIFT = 2.0 ** 64
LAG = 2
P_AFTER = 2
NEAR = 4
BLOCK = 8
AHEAD = 6
F32 = jnp.float32
BF16 = jnp.bfloat16


def ring_distance(offset, n):
    return min(offset, n - offset)


def forward_kernel(dims, n_steps, block, a_ref, e_ref, r0_ref, len_ref, alpha_ref, ll_ref,
                   a_loc, e_both, e_loc, w_loc, r_in, c_in, p_in, u_in, u_out, a_bf, len_row, len_col, alpha_acc, ll_acc,
                   fin_alpha, fin_ll, tick, a_sem, a_send, e_pair, e_send, e_sem, r0_sem, r0_send, own_sem,
                   g_recv, g_send, c_recv, c_send, u_recv, u_send, p_recv, p_send, f_recv, f_send):
    nz, ny, nx = dims
    n_sum, n_gather = 2 * nz, 2 * nx
    batch = r0_ref.shape[0]
    half = n_gather * SB
    rows = block * batch
    n_blocks = n_steps // block
    per_step = n_sum // block
    core = lax.axis_index('rows')
    me = lax.axis_index('states')
    z = me // (ny * nx)
    y = (me // nx) % ny
    x = me % nx
    group = me // n_gather
    c_place = (((y + 1) // 2) % 2) * nx + x
    far = sorted(range(1, n_sum), key=lambda k: -(ring_distance(k // 2, nz) + k % 2))
    sources = sorted(((f, d) for f in range(2) for d in range(nx)), key=lambda o: o[0] + ring_distance(o[1], nx))
    slot_of = {o: i for i, o in enumerate(sources)}
    far_gather = sources[:0:-1]
    n_near = n_gather // 2
    n_far = n_gather - n_near

    def sum_peer(k, sign=1):
        flip = k % 2
        return ((z + sign * (k // 2) + nz) % nz) * ny * nx + (y + flip * (ny - 1 - 2 * y)) * nx + x

    def mirror(k):
        return ((nz - k // 2) % nz) * 2 + k % 2

    def gather_peer(flip, d):
        return (me // (ny * nx)) * ny * nx + (y + flip * (1 - 2 * (y % 2))) * nx + (x + d) % nx

    def remote(src, dst, send, recv, state, to=1):
        return pltpu.make_async_remote_copy(src_ref=src, dst_ref=dst, send_sem=send, recv_sem=recv,
                                            device_id={'rows': to, 'states': state},
                                            device_id_type=pl.DeviceIdType.MESH)

    def wait_bytes(ref, sem):
        pltpu.make_async_copy(ref, ref, sem).wait()

    def a_rows(state, h):
        for i, (f, d) in enumerate(sources):
            there = ((state // nx + f) % 2) * nx + (x + d) % nx
            yield (a_ref.at[pl.ds((state // n_gather) * half + there * SB, SB)], pl.ds((2 * i + h) * SB, SB))

    def start_a(h, k):
        peer = sum_peer(k, -1)
        for src, to in a_rows(peer, h):
            remote(src, a_loc.at[k, to], a_send.at[k], a_sem.at[k, h], peer).start()

    def e_copy(b, k):
        return remote(e_both.at[pl.ds(b * rows + batch, rows)], e_loc.at[b, k], e_send, e_sem.at[b % 2, k], sum_peer(k, -1))

    barrier = pltpu.get_barrier_semaphore()

    def announce(state, to):
        pl.semaphore_signal(barrier, inc=1, device_id={'rows': to, 'states': state}, device_id_type=pl.DeviceIdType.MESH)

    @pl.when(core == 0)
    def helper():
        announce(me, 1)
        pl.semaphore_wait(barrier, n_sum)
        first = remote(r0_ref, r_in.at[0, 0, 0], r0_send, r0_sem, me)
        first.start()
        every = pl.ds(0, n_steps * batch)
        mine = pltpu.make_async_copy(e_ref, e_both.at[every, pl.ds(0, SB)], own_sem.at[0])
        mine.start()
        e_both[pl.ds(n_steps * batch, batch), :] = jnp.zeros((batch, 2 * SB), BF16)
        start_a(0, 0)
        start_a(0, 1)
        mine.wait()
        wait_bytes(e_both.at[every, pl.ds(SB, SB)], e_pair)
        e_copy(0, 0).start()
        e_copy(0, 1).start()
        for k in range(2, n_sum):
            start_a(0, k)
            e_copy(0, k).start()
        wait_bytes(e_loc.at[0], e_send)

        def send_part(i, carry):
            @pl.when(i >= AHEAD)
            def paced():
                pl.semaphore_wait(tick, 1)

            for n in range(per_step):
                e_copy(1 + i // block, (i % block) * per_step + n).start()
            wait_bytes(e_loc.at[0, pl.ds(0, per_step)], e_send)
            return carry

        lax.fori_loop(0, n_steps - block, send_part, 0)
        first.wait_send()
        for k in range(n_sum):
            wait_bytes(a_loc.at[k, pl.ds(0, half)], a_send.at[k])
        wait_bytes(fin_alpha, f_recv.at[0])
        wait_bytes(fin_ll, f_recv.at[1])
        alpha_ref[...] = fin_alpha[...]
        ll_ref[...] = fin_ll[...]

    @pl.when(core == 1)
    def owner():
        eye = (lax.broadcasted_iota(jnp.int32, (batch, SB), 0)
               == lax.broadcasted_iota(jnp.int32, (batch, SB), 1))

        def as_row(tile):
            col = jnp.sum(tile, axis=1, keepdims=True)
            return jnp.sum(jnp.where(eye, col, 0.0), axis=0, keepdims=True)

        def as_col(row):
            return jnp.sum(jnp.where(eye, row, 0.0), axis=1, keepdims=True)

        def start_gather(slot):
            for f, d in far_gather:
                there = slot_of[f, (nx - d) % nx]
                remote(r_in.at[slot, 0], r_in.at[slot, there], g_send, g_recv.at[slot, there // n_near],
                       gather_peer(f, d)).start()

        def start_parts(slot):
            for k in far:
                remote(p_in.at[slot, group], p_in.at[slot, group], p_send, p_recv.at[slot], sum_peer(k)).start()

        others = pl.ds(0, n_gather - 1)
        peers = pl.ds(0, n_sum - 1)

        def finish_norm(slot):
            wait_bytes(p_in.at[slot, peers], p_recv.at[slot])
            c_in[slot, c_place] = jnp.sum(p_in[slot], axis=0)
            for o in far_gather:
                remote(c_in.at[slot, c_place], c_in.at[slot, c_place], c_send, c_recv.at[slot], gather_peer(*o)).start()

        def wait_near(slot):
            if n_near > 1:
                wait_bytes(r_in.at[slot, pl.ds(0, n_near - 1)], g_recv.at[slot, 0])

        def wait_far(slot):
            wait_bytes(r_in.at[slot, pl.ds(0, n_far)], g_recv.at[slot, 1])

        def norm(slot):
            wait_bytes(c_in.at[slot, others], c_recv.at[slot])
            c_row = jnp.sum(c_in[slot], axis=0)
            c_col = as_col(c_row)
            inv = 1.0 / c_col
            return c_row, inv * (2.0 - c_col * inv)

        def keep(t, slot, c_row, inv):
            now = lax.convert_element_type(t, F32)
            active = now < len_col[...]
            for h in range(2):
                alpha_acc[h] = jnp.where(active, r_in[slot, 0, h] * inv, alpha_acc[h])
            ll_acc[...] = ll_acc[...] + jnp.where(now < len_row[...], jnp.log(c_row * (1.0 / LIFT)), 0.0)

        def add_w(b, k, fresh):
            part = lax.dot_general(e_loc[b, k], a_loc[k], (((1,), (1,)), ((), ())), preferred_element_type=F32)
            slot = b % 2
            w_loc[slot] = jnp.where(fresh, 0.0, w_loc[slot]) + part

        for k in far:
            announce(sum_peer(k), 1)
        for o in far_gather:
            announce(gather_peer(*o), 1)
        for k in range(n_sum):
            announce(sum_peer(k), 0)
        pl.semaphore_wait(barrier, n_sum + n_gather - 1)
        pair = remote(e_ref, e_both.at[pl.ds(0, n_steps * batch), pl.ds(SB, SB)], own_sem.at[0], e_pair, me, to=0)
        pair.start()
        for k in range(1, n_sum):
            start_a(1, k)
        for src, to in a_rows(me, 1):
            pltpu.make_async_copy(src, a_loc.at[0, to], own_sem.at[1]).start()
        alpha_acc[...] = jnp.zeros_like(alpha_acc)
        ll_acc[...] = jnp.zeros_like(ll_acc)
        w_loc[...] = jnp.zeros_like(w_loc)
        len_row[...] = jnp.zeros_like(len_row)
        len_row[:, :batch] = len_ref[...].astype(F32)
        len_col[...] = jnp.broadcast_to(as_col(len_row[...]), (batch, SB))
        r_in[0, 0, 1] = r0_ref[...]
        wait_bytes(r0_ref, r0_sem)
        p_in[0, group] = as_row(r_in[0, 0, 0] + r_in[0, 0, 1])
        start_parts(0)
        start_gather(0)
        finish_norm(0)
        wait_bytes(p_in.at[0, peers], p_send)
        wait_bytes(a_loc.at[0, pl.ds(0, half)], own_sem.at[1])

        def first_w(k, carry):
            wait_bytes(a_loc.at[k, pl.ds(0, half)], a_sem.at[k, 0])

            @pl.when(k > 0)
            def from_owner():
                wait_bytes(a_loc.at[k, pl.ds(0, half)], a_sem.at[k, 1])

            wait_bytes(e_loc.at[0, k], e_sem.at[0, k])
            add_w(0, k, False)
            return carry

        lax.fori_loop(0, n_sum, first_w, 0)
        pair.wait_send()
        for k in range(1, n_sum):
            wait_bytes(a_loc.at[k, pl.ds(0, half)], a_send.at[k])

        def one_step(t, carry):
            cur = t % 2
            nxt = (t + 1) % 2
            b = t // block
            row = pl.ds((t % block) * batch, batch)
            c_row, inv = norm(cur)
            total = jnp.zeros((batch, SB), F32)

            def take(first, last, total):
                for i in range(first, last):
                    for h in range(2):
                        cols = pl.ds((2 * i + h) * SB, SB)
                        tile = (r_in[cur, i, h] * inv).astype(BF16)
                        a_bf[:, cols] = tile
                        total = total + tile.astype(F32) * w_loc[b % 2, row, cols]
                return total

            def times(k, first, last):
                return jnp.dot(a_bf[:, first:last], a_loc[k, first:last], preferred_element_type=F32)

            order = far + [0]
            near_rows, all_rows = 2 * n_near * SB, 2 * half
            wait_near(cur)
            total = take(0, n_near, total)
            near = [times(k, 0, near_rows) for k in order[:NEAR]]
            wait_far(cur)
            total = take(n_near, n_gather, total)
            unit = jnp.where(t >= 0, jnp.float32(1.0), jnp.float32(0.0))
            ready = []

            def send_sum():
                k, part = ready.pop(0)
                for h in range(2):
                    u_out[k - 1, h] = part[:, h * SB:(h + 1) * SB]
                remote(u_out.at[k - 1], u_in.at[nxt, mirror(k) - 1], u_send, u_recv.at[nxt], sum_peer(k)).start()

            for i, k in enumerate(order):
                begin = near_rows if i < NEAR else 0
                middle = (begin + all_rows) // 2
                part = times(k, begin, middle) * unit + times(k, middle, all_rows)
                ready.append((k, part + near[i] if i < NEAR else part))
                if i == P_AFTER:
                    p_in[nxt, group] = as_row(total)
                    start_parts(nxt)
                if len(ready) > LAG:
                    send_sum()
            while len(ready) > 1:
                send_sum()
            own_part = ready[0][1]
            wait_bytes(r_in.at[cur, others], g_send)
            wait_bytes(c_in.at[cur, others], c_send)
            keep(t, cur, c_row, inv)
            finish_norm(nxt)
            wait_bytes(u_in.at[nxt], u_recv.at[nxt])
            for h in range(2):
                parts = [own_part[:, h * SB:(h + 1) * SB]] + [u_in[nxt, k, h] for k in range(n_sum - 1)]
                while len(parts) > 1:
                    parts = [parts[i] + parts[i + 1] for i in range(0, len(parts), 2)]
                r_in[nxt, 0, h] = parts[0] * e_loc[b, 0, row, pl.ds(h * SB, SB)].astype(F32)
            start_gather(nxt)

            @pl.when(t < n_steps - block - AHEAD)
            def go_on():
                pl.semaphore_signal(tick, inc=1, device_id={'rows': 0, 'states': me},
                                    device_id_type=pl.DeviceIdType.MESH)

            @pl.when(b + 1 < n_blocks)
            def next_w():
                later = b + 1
                for n in range(per_step):
                    k = (t % block) * per_step + n
                    wait_bytes(e_loc.at[later, k], e_sem.at[later % 2, k])
                    add_w(later, k, k == 0)

            wait_bytes(u_out, u_send)
            wait_bytes(p_in.at[nxt, peers], p_send)
            return carry

        lax.fori_loop(0, n_steps - 1, one_step, 0)
        last = (n_steps - 1) % 2
        c_row, inv = norm(last)
        wait_near(last)
        wait_far(last)
        keep(n_steps - 1, last, c_row, inv)
        wait_bytes(r_in.at[last, others], g_send)
        wait_bytes(c_in.at[last, others], c_send)
        result = [remote(alpha_acc.at[0], fin_alpha, f_send.at[0], f_recv.at[0], me, to=0),
                  remote(ll_acc, fin_ll, f_send.at[1], f_recv.at[1], me, to=0)]
        for copy in result:
            copy.start()
        alpha_ref[...] = alpha_acc[1]
        ll_ref[...] = ll_acc[...]
        for copy in result:
            copy.wait_send()


def solution(mesh):
    vec_axes = ('rows', 'states')
    nz, ny, nx = CHIPS
    n_sum, n_gather = 2 * nz, 2 * nx

    def local_forward(trans_blk, emit_blk, init_blk, tokens, lengths):
        batch, n_steps = tokens.shape
        cols = 2 * SB
        a_blk = trans_blk.reshape(trans_blk.shape[0], cols)
        emis = jnp.transpose(emit_blk.at[:, tokens].get(mode='promise_in_bounds'), (2, 1, 0))
        emis = emis * jnp.asarray(LIFT, emis.dtype)
        first_raw = init_blk[None, :] * emis[0].astype(F32)
        vmem = pl.BlockSpec(memory_space=pltpu.VMEM)
        hbm = pl.BlockSpec(memory_space=pl.ANY)
        dma = pltpu.SemaphoreType.DMA
        k_rows = 2 * n_gather * SB
        block = min(BLOCK, n_sum)
        block_rows = block * batch
        n_blocks = n_steps // block
        alpha, ll = pl.pallas_call(
            functools.partial(forward_kernel, CHIPS, n_steps, block),
            out_shape=(jax.ShapeDtypeStruct((batch, SB), F32), jax.ShapeDtypeStruct((1, SB), F32)),
            in_specs=[hbm, hbm, vmem, vmem],
            out_specs=(vmem, vmem),
            scratch_shapes=[
                pltpu.VMEM((n_sum, k_rows, cols), BF16),
                pltpu.VMEM(((n_steps + 1) * batch, cols), BF16),
                pltpu.VMEM((n_blocks, n_sum, block_rows, cols), BF16),
                pltpu.VMEM((2, block_rows, k_rows), F32),
                pltpu.VMEM((2, n_gather, 2, batch, SB), F32),
                pltpu.VMEM((2, n_gather, 1, SB), F32),
                pltpu.VMEM((2, n_sum, 1, SB), F32),
                pltpu.VMEM((2, n_sum - 1, 2, batch, SB), F32),
                pltpu.VMEM((n_sum - 1, 2, batch, SB), F32),
                pltpu.VMEM((batch, k_rows), BF16),
                pltpu.VMEM((1, SB), F32),
                pltpu.VMEM((batch, SB), F32),
                pltpu.VMEM((2, batch, SB), F32),
                pltpu.VMEM((1, SB), F32),
                pltpu.VMEM((batch, SB), F32),
                pltpu.VMEM((1, SB), F32),
                pltpu.SemaphoreType.REGULAR,
                dma((n_sum, 2)), dma((n_sum,)), dma, dma, dma((2, n_sum)), dma, dma, dma((2,)),
                dma((2, 2)), dma, dma((2,)), dma, dma((2,)), dma, dma((2,)), dma, dma((2,)), dma((2,)),
            ],
            compiler_params=pltpu.CompilerParams(collective_id=0, has_side_effects=True,
                                                 vmem_limit_bytes=48 * 1024 * 1024),
            cost_estimate=pl.CostEstimate(flops=2 * batch * (n_steps - 1) * n_sum * k_rows * cols,
                                          bytes_accessed=n_sum * k_rows * cols * 2, transcendentals=0),
        )(a_blk, emis.reshape(n_steps * batch, SB), first_raw, lengths[None, :])
        return ll[0, :batch], alpha

    return jax.shard_map(local_forward, mesh=mesh, in_specs=(P('rows', None, 'states'), P(vec_axes, None), P(vec_axes), P('seqs', None), P('seqs')), out_specs=(P('seqs'), P('seqs', vec_axes)), check_vma=False)
```

```python
import functools

import jax
import jax.numpy as jnp
from jax import lax
from jax.experimental import pallas as pl
from jax.experimental.pallas import tpu as pltpu
from jax.sharding import PartitionSpec as P

CHIPS = (4, 4, 4)
SB = 128
LIFT = 2.0 ** 64
LAG = 1
P_AFTER = 1
NEAR = 2
BLOCK = 8
AHEAD = 6
F32 = jnp.float32
BF16 = jnp.bfloat16


def ring_distance(offset, n):
    return min(offset, n - offset)


def forward_kernel(dims, n_steps, block, a_ref, e_ref, r0_ref, len_ref, alpha_ref, ll_ref,
                   a_loc, e_both, e_loc, w_loc, r_in, c_in, p_in, u_in, u_out, a_bf, len_row, len_col, alpha_acc, ll_acc,
                   fin_alpha, fin_ll, tick, a_sem, a_send, e_pair, e_send, e_sem, r0_sem, r0_send, own_sem,
                   g_recv, g_send, c_recv, c_send, u_recv, u_send, p_recv, p_send, f_recv, f_send):
    nz, ny, nx = dims
    n_sum, n_gather = 2 * nz, 2 * nx
    batch = r0_ref.shape[0]
    half = n_gather * SB
    rows = block * batch
    n_blocks = n_steps // block
    per_step = n_sum // block
    core = lax.axis_index('rows')
    me = lax.axis_index('states')
    z = me // (ny * nx)
    y = (me // nx) % ny
    x = me % nx
    group = me // n_gather
    c_place = (((y + 1) // 2) % 2) * nx + x
    far = sorted(range(1, n_sum), key=lambda k: -(ring_distance(k // 2, nz) + k % 2))
    sources = sorted(((f, d) for f in range(2) for d in range(nx)), key=lambda o: o[0] + ring_distance(o[1], nx))
    slot_of = {o: i for i, o in enumerate(sources)}
    far_gather = sources[:0:-1]
    n_near = n_gather // 2
    n_far = n_gather - n_near

    def sum_peer(k, sign=1):
        flip = k % 2
        return ((z + sign * (k // 2) + nz) % nz) * ny * nx + (y + flip * (ny - 1 - 2 * y)) * nx + x

    def mirror(k):
        return ((nz - k // 2) % nz) * 2 + k % 2

    def gather_peer(flip, d):
        return (me // (ny * nx)) * ny * nx + (y + flip * (1 - 2 * (y % 2))) * nx + (x + d) % nx

    def remote(src, dst, send, recv, state, to=1):
        return pltpu.make_async_remote_copy(src_ref=src, dst_ref=dst, send_sem=send, recv_sem=recv,
                                            device_id={'rows': to, 'states': state},
                                            device_id_type=pl.DeviceIdType.MESH)

    def wait_bytes(ref, sem):
        pltpu.make_async_copy(ref, ref, sem).wait()

    def a_rows(state, h):
        for i, (f, d) in enumerate(sources):
            there = ((state // nx + f) % 2) * nx + (x + d) % nx
            yield (a_ref.at[pl.ds((state // n_gather) * half + there * SB, SB)], pl.ds((2 * i + h) * SB, SB))

    def start_a(h, k):
        peer = sum_peer(k, -1)
        for src, to in a_rows(peer, h):
            remote(src, a_loc.at[k, to], a_send.at[k], a_sem.at[k, h], peer).start()

    def e_copy(b, k):
        return remote(e_both.at[pl.ds(b * rows + batch, rows)], e_loc.at[b, k], e_send, e_sem.at[b % 2, k], sum_peer(k, -1))

    barrier = pltpu.get_barrier_semaphore()

    def announce(state, to):
        pl.semaphore_signal(barrier, inc=1, device_id={'rows': to, 'states': state}, device_id_type=pl.DeviceIdType.MESH)

    @pl.when(core == 0)
    def helper():
        announce(me, 1)
        pl.semaphore_wait(barrier, n_sum)
        first = remote(r0_ref, r_in.at[0, 0, 0], r0_send, r0_sem, me)
        first.start()
        every = pl.ds(0, n_steps * batch)
        mine = pltpu.make_async_copy(e_ref, e_both.at[every, pl.ds(0, SB)], own_sem.at[0])
        mine.start()
        e_both[pl.ds(n_steps * batch, batch), :] = jnp.zeros((batch, 2 * SB), BF16)
        start_a(0, 0)
        start_a(0, 1)
        mine.wait()
        wait_bytes(e_both.at[every, pl.ds(SB, SB)], e_pair)
        e_copy(0, 0).start()
        e_copy(0, 1).start()
        for k in range(2, n_sum):
            start_a(0, k)
            e_copy(0, k).start()
        wait_bytes(e_loc.at[0], e_send)

        def send_part(i, carry):
            @pl.when(i >= AHEAD)
            def paced():
                pl.semaphore_wait(tick, 1)

            for n in range(per_step):
                e_copy(1 + i // block, (i % block) * per_step + n).start()
            wait_bytes(e_loc.at[0, pl.ds(0, per_step)], e_send)
            return carry

        lax.fori_loop(0, n_steps - block, send_part, 0)
        first.wait_send()
        for k in range(n_sum):
            wait_bytes(a_loc.at[k, pl.ds(0, half)], a_send.at[k])
        wait_bytes(fin_alpha, f_recv.at[0])
        wait_bytes(fin_ll, f_recv.at[1])
        alpha_ref[...] = fin_alpha[...]
        ll_ref[...] = fin_ll[...]

    @pl.when(core == 1)
    def owner():
        eye = (lax.broadcasted_iota(jnp.int32, (batch, SB), 0)
               == lax.broadcasted_iota(jnp.int32, (batch, SB), 1))

        def as_row(tile):
            col = jnp.sum(tile, axis=1, keepdims=True)
            return jnp.sum(jnp.where(eye, col, 0.0), axis=0, keepdims=True)

        def as_col(row):
            return jnp.sum(jnp.where(eye, row, 0.0), axis=1, keepdims=True)

        def start_gather(slot):
            for f, d in far_gather:
                there = slot_of[f, (nx - d) % nx]
                remote(r_in.at[slot, 0], r_in.at[slot, there], g_send, g_recv.at[slot, there // n_near],
                       gather_peer(f, d)).start()

        def start_parts(slot):
            for k in far:
                remote(p_in.at[slot, group], p_in.at[slot, group], p_send, p_recv.at[slot], sum_peer(k)).start()

        others = pl.ds(0, n_gather - 1)
        peers = pl.ds(0, n_sum - 1)

        def finish_norm(slot):
            wait_bytes(p_in.at[slot, peers], p_recv.at[slot])
            c_in[slot, c_place] = jnp.sum(p_in[slot], axis=0)
            for o in far_gather:
                remote(c_in.at[slot, c_place], c_in.at[slot, c_place], c_send, c_recv.at[slot], gather_peer(*o)).start()

        def wait_near(slot):
            if n_near > 1:
                wait_bytes(r_in.at[slot, pl.ds(0, n_near - 1)], g_recv.at[slot, 0])

        def wait_far(slot):
            wait_bytes(r_in.at[slot, pl.ds(0, n_far)], g_recv.at[slot, 1])

        def norm(slot):
            wait_bytes(c_in.at[slot, others], c_recv.at[slot])
            c_row = jnp.sum(c_in[slot], axis=0)
            c_col = as_col(c_row)
            inv = 1.0 / c_col
            return c_row, inv * (2.0 - c_col * inv)

        def keep(t, slot, c_row, inv):
            now = lax.convert_element_type(t, F32)
            active = now < len_col[...]
            for h in range(2):
                alpha_acc[h] = jnp.where(active, r_in[slot, 0, h] * inv, alpha_acc[h])
            ll_acc[...] = ll_acc[...] + jnp.where(now < len_row[...], jnp.log(c_row * (1.0 / LIFT)), 0.0)

        def add_w(b, k, fresh):
            part = lax.dot_general(e_loc[b, k], a_loc[k], (((1,), (1,)), ((), ())), preferred_element_type=F32)
            slot = b % 2
            w_loc[slot] = jnp.where(fresh, 0.0, w_loc[slot]) + part

        for k in far:
            announce(sum_peer(k), 1)
        for o in far_gather:
            announce(gather_peer(*o), 1)
        for k in range(n_sum):
            announce(sum_peer(k), 0)
        pl.semaphore_wait(barrier, n_sum + n_gather - 1)
        pair = remote(e_ref, e_both.at[pl.ds(0, n_steps * batch), pl.ds(SB, SB)], own_sem.at[0], e_pair, me, to=0)
        pair.start()
        for k in range(1, n_sum):
            start_a(1, k)
        for src, to in a_rows(me, 1):
            pltpu.make_async_copy(src, a_loc.at[0, to], own_sem.at[1]).start()
        alpha_acc[...] = jnp.zeros_like(alpha_acc)
        ll_acc[...] = jnp.zeros_like(ll_acc)
        w_loc[...] = jnp.zeros_like(w_loc)
        len_row[...] = jnp.zeros_like(len_row)
        len_row[:, :batch] = len_ref[...].astype(F32)
        len_col[...] = jnp.broadcast_to(as_col(len_row[...]), (batch, SB))
        r_in[0, 0, 1] = r0_ref[...]
        wait_bytes(r0_ref, r0_sem)
        p_in[0, group] = as_row(r_in[0, 0, 0] + r_in[0, 0, 1])
        start_parts(0)
        start_gather(0)
        finish_norm(0)
        wait_bytes(p_in.at[0, peers], p_send)
        wait_bytes(a_loc.at[0, pl.ds(0, half)], own_sem.at[1])

        def first_w(k, carry):
            wait_bytes(a_loc.at[k, pl.ds(0, half)], a_sem.at[k, 0])

            @pl.when(k > 0)
            def from_owner():
                wait_bytes(a_loc.at[k, pl.ds(0, half)], a_sem.at[k, 1])

            wait_bytes(e_loc.at[0, k], e_sem.at[0, k])
            add_w(0, k, False)
            return carry

        lax.fori_loop(0, n_sum, first_w, 0)
        pair.wait_send()
        for k in range(1, n_sum):
            wait_bytes(a_loc.at[k, pl.ds(0, half)], a_send.at[k])

        def one_step(t, carry):
            cur = t % 2
            nxt = (t + 1) % 2
            b = t // block
            row = pl.ds((t % block) * batch, batch)
            c_row, inv = norm(cur)
            total = jnp.zeros((batch, SB), F32)

            def take(first, last, total):
                for i in range(first, last):
                    for h in range(2):
                        cols = pl.ds((2 * i + h) * SB, SB)
                        tile = (r_in[cur, i, h] * inv).astype(BF16)
                        a_bf[:, cols] = tile
                        total = total + tile.astype(F32) * w_loc[b % 2, row, cols]
                return total

            def times(k, first, last):
                return jnp.dot(a_bf[:, first:last], a_loc[k, first:last], preferred_element_type=F32)

            order = far + [0]
            near_rows, all_rows = 2 * n_near * SB, 2 * half
            wait_near(cur)
            total = take(0, n_near, total)
            near = [times(k, 0, near_rows) for k in order[:NEAR]]
            wait_far(cur)
            total = take(n_near, n_gather, total)
            unit = jnp.where(t >= 0, jnp.float32(1.0), jnp.float32(0.0))
            ready = []

            def send_sum():
                k, part = ready.pop(0)
                for h in range(2):
                    u_out[k - 1, h] = part[:, h * SB:(h + 1) * SB]
                remote(u_out.at[k - 1], u_in.at[nxt, mirror(k) - 1], u_send, u_recv.at[nxt], sum_peer(k)).start()

            for i, k in enumerate(order):
                begin = near_rows if i < NEAR else 0
                middle = (begin + all_rows) // 2
                part = times(k, begin, middle) * unit + times(k, middle, all_rows)
                ready.append((k, part + near[i] if i < NEAR else part))
                if i == P_AFTER:
                    p_in[nxt, group] = as_row(total)
                    start_parts(nxt)
                if len(ready) > LAG:
                    send_sum()
            while len(ready) > 1:
                send_sum()
            own_part = ready[0][1]
            wait_bytes(r_in.at[cur, others], g_send)
            wait_bytes(c_in.at[cur, others], c_send)
            keep(t, cur, c_row, inv)
            finish_norm(nxt)
            wait_bytes(u_in.at[nxt], u_recv.at[nxt])
            for h in range(2):
                parts = [own_part[:, h * SB:(h + 1) * SB]] + [u_in[nxt, k, h] for k in range(n_sum - 1)]
                while len(parts) > 1:
                    parts = [parts[i] + parts[i + 1] for i in range(0, len(parts), 2)]
                r_in[nxt, 0, h] = parts[0] * e_loc[b, 0, row, pl.ds(h * SB, SB)].astype(F32)
            start_gather(nxt)

            @pl.when(t < n_steps - block - AHEAD)
            def go_on():
                pl.semaphore_signal(tick, inc=1, device_id={'rows': 0, 'states': me},
                                    device_id_type=pl.DeviceIdType.MESH)

            @pl.when(b + 1 < n_blocks)
            def next_w():
                later = b + 1
                for n in range(per_step):
                    k = (t % block) * per_step + n
                    wait_bytes(e_loc.at[later, k], e_sem.at[later % 2, k])
                    add_w(later, k, k == 0)

            wait_bytes(u_out, u_send)
            wait_bytes(p_in.at[nxt, peers], p_send)
            return carry

        lax.fori_loop(0, n_steps - 1, one_step, 0)
        last = (n_steps - 1) % 2
        c_row, inv = norm(last)
        wait_near(last)
        wait_far(last)
        keep(n_steps - 1, last, c_row, inv)
        wait_bytes(r_in.at[last, others], g_send)
        wait_bytes(c_in.at[last, others], c_send)
        result = [remote(alpha_acc.at[0], fin_alpha, f_send.at[0], f_recv.at[0], me, to=0),
                  remote(ll_acc, fin_ll, f_send.at[1], f_recv.at[1], me, to=0)]
        for copy in result:
            copy.start()
        alpha_ref[...] = alpha_acc[1]
        ll_ref[...] = ll_acc[...]
        for copy in result:
            copy.wait_send()


def solution(mesh):
    vec_axes = ('rows', 'states')
    nz, ny, nx = CHIPS
    n_sum, n_gather = 2 * nz, 2 * nx

    def local_forward(trans_blk, emit_blk, init_blk, tokens, lengths):
        batch, n_steps = tokens.shape
        cols = 2 * SB
        a_blk = trans_blk.reshape(trans_blk.shape[0], cols)
        emis = jnp.transpose(emit_blk.at[:, tokens].get(mode='promise_in_bounds'), (2, 1, 0))
        emis = emis * jnp.asarray(LIFT, emis.dtype)
        first_raw = init_blk[None, :] * emis[0].astype(F32)
        vmem = pl.BlockSpec(memory_space=pltpu.VMEM)
        hbm = pl.BlockSpec(memory_space=pl.ANY)
        dma = pltpu.SemaphoreType.DMA
        k_rows = 2 * n_gather * SB
        block = min(BLOCK, n_sum)
        block_rows = block * batch
        n_blocks = n_steps // block
        alpha, ll = pl.pallas_call(
            functools.partial(forward_kernel, CHIPS, n_steps, block),
            out_shape=(jax.ShapeDtypeStruct((batch, SB), F32), jax.ShapeDtypeStruct((1, SB), F32)),
            in_specs=[hbm, hbm, vmem, vmem],
            out_specs=(vmem, vmem),
            scratch_shapes=[
                pltpu.VMEM((n_sum, k_rows, cols), BF16),
                pltpu.VMEM(((n_steps + 1) * batch, cols), BF16),
                pltpu.VMEM((n_blocks, n_sum, block_rows, cols), BF16),
                pltpu.VMEM((2, block_rows, k_rows), F32),
                pltpu.VMEM((2, n_gather, 2, batch, SB), F32),
                pltpu.VMEM((2, n_gather, 1, SB), F32),
                pltpu.VMEM((2, n_sum, 1, SB), F32),
                pltpu.VMEM((2, n_sum - 1, 2, batch, SB), F32),
                pltpu.VMEM((n_sum - 1, 2, batch, SB), F32),
                pltpu.VMEM((batch, k_rows), BF16),
                pltpu.VMEM((1, SB), F32),
                pltpu.VMEM((batch, SB), F32),
                pltpu.VMEM((2, batch, SB), F32),
                pltpu.VMEM((1, SB), F32),
                pltpu.VMEM((batch, SB), F32),
                pltpu.VMEM((1, SB), F32),
                pltpu.SemaphoreType.REGULAR,
                dma((n_sum, 2)), dma((n_sum,)), dma, dma, dma((2, n_sum)), dma, dma, dma((2,)),
                dma((2, 2)), dma, dma((2,)), dma, dma((2,)), dma, dma((2,)), dma, dma((2,)), dma((2,)),
            ],
            compiler_params=pltpu.CompilerParams(collective_id=0, has_side_effects=True,
                                                 vmem_limit_bytes=48 * 1024 * 1024),
            cost_estimate=pl.CostEstimate(flops=2 * batch * (n_steps - 1) * n_sum * k_rows * cols,
                                          bytes_accessed=n_sum * k_rows * cols * 2, transcendentals=0),
        )(a_blk, emis.reshape(n_steps * batch, SB), first_raw, lengths[None, :])
        return ll[0, :batch], alpha

    return jax.shard_map(local_forward, mesh=mesh, in_specs=(P('rows', None, 'states'), P(vec_axes, None), P(vec_axes), P('seqs', None), P('seqs')), out_specs=(P('seqs'), P('seqs', vec_axes)), check_vma=False)
```

```python
import functools

import jax
import jax.numpy as jnp
from jax import lax
from jax.experimental import pallas as pl
from jax.experimental.pallas import tpu as pltpu
from jax.sharding import PartitionSpec as P

CHIPS = (4, 4, 4)
SB = 128
LIFT = 2.0 ** 64
LAG = 1
P_AFTER = 1
NEAR = 0
BLOCK = 8
AHEAD = 6
F32 = jnp.float32
BF16 = jnp.bfloat16


def ring_distance(offset, n):
    return min(offset, n - offset)


def forward_kernel(dims, n_steps, block, a_ref, e_ref, r0_ref, len_ref, alpha_ref, ll_ref,
                   a_loc, e_both, e_loc, w_loc, r_in, c_in, p_in, u_in, u_out, a_bf, len_row, len_col, alpha_acc, ll_acc,
                   fin_alpha, fin_ll, tick, a_sem, a_send, e_pair, e_send, e_sem, r0_sem, r0_send, own_sem,
                   g_recv, g_send, c_recv, c_send, u_recv, u_send, p_recv, p_send, f_recv, f_send):
    nz, ny, nx = dims
    n_sum, n_gather = 2 * nz, 2 * nx
    batch = r0_ref.shape[0]
    half = n_gather * SB
    rows = block * batch
    n_blocks = n_steps // block
    per_step = n_sum // block
    core = lax.axis_index('rows')
    me = lax.axis_index('states')
    z = me // (ny * nx)
    y = (me // nx) % ny
    x = me % nx
    group = me // n_gather
    c_place = (((y + 1) // 2) % 2) * nx + x
    far = sorted(range(1, n_sum), key=lambda k: -(ring_distance(k // 2, nz) + k % 2))
    sources = sorted(((f, d) for f in range(2) for d in range(nx)), key=lambda o: o[0] + ring_distance(o[1], nx))
    slot_of = {o: i for i, o in enumerate(sources)}
    far_gather = sources[:0:-1]
    n_near = n_gather // 2
    n_far = n_gather - n_near

    def sum_peer(k, sign=1):
        flip = k % 2
        return ((z + sign * (k // 2) + nz) % nz) * ny * nx + (y + flip * (ny - 1 - 2 * y)) * nx + x

    def mirror(k):
        return ((nz - k // 2) % nz) * 2 + k % 2

    def gather_peer(flip, d):
        return (me // (ny * nx)) * ny * nx + (y + flip * (1 - 2 * (y % 2))) * nx + (x + d) % nx

    def remote(src, dst, send, recv, state, to=1):
        return pltpu.make_async_remote_copy(src_ref=src, dst_ref=dst, send_sem=send, recv_sem=recv,
                                            device_id={'rows': to, 'states': state},
                                            device_id_type=pl.DeviceIdType.MESH)

    def wait_bytes(ref, sem):
        pltpu.make_async_copy(ref, ref, sem).wait()

    def a_rows(state, h):
        for i, (f, d) in enumerate(sources):
            there = ((state // nx + f) % 2) * nx + (x + d) % nx
            yield (a_ref.at[pl.ds((state // n_gather) * half + there * SB, SB)], pl.ds((2 * i + h) * SB, SB))

    def start_a(h, k):
        peer = sum_peer(k, -1)
        for src, to in a_rows(peer, h):
            remote(src, a_loc.at[k, to], a_send.at[k], a_sem.at[k, h], peer).start()

    def e_copy(b, k):
        return remote(e_both.at[pl.ds(b * rows + batch, rows)], e_loc.at[b, k], e_send, e_sem.at[b % 2, k], sum_peer(k, -1))

    barrier = pltpu.get_barrier_semaphore()

    def announce(state, to):
        pl.semaphore_signal(barrier, inc=1, device_id={'rows': to, 'states': state}, device_id_type=pl.DeviceIdType.MESH)

    @pl.when(core == 0)
    def helper():
        announce(me, 1)
        pl.semaphore_wait(barrier, n_sum)
        first = remote(r0_ref, r_in.at[0, 0, 0], r0_send, r0_sem, me)
        first.start()
        every = pl.ds(0, n_steps * batch)
        mine = pltpu.make_async_copy(e_ref, e_both.at[every, pl.ds(0, SB)], own_sem.at[0])
        mine.start()
        e_both[pl.ds(n_steps * batch, batch), :] = jnp.zeros((batch, 2 * SB), BF16)
        start_a(0, 0)
        start_a(0, 1)
        mine.wait()
        wait_bytes(e_both.at[every, pl.ds(SB, SB)], e_pair)
        e_copy(0, 0).start()
        e_copy(0, 1).start()
        for k in range(2, n_sum):
            start_a(0, k)
            e_copy(0, k).start()
        wait_bytes(e_loc.at[0], e_send)

        def send_part(i, carry):
            @pl.when(i >= AHEAD)
            def paced():
                pl.semaphore_wait(tick, 1)

            for n in range(per_step):
                e_copy(1 + i // block, (i % block) * per_step + n).start()
            wait_bytes(e_loc.at[0, pl.ds(0, per_step)], e_send)
            return carry

        lax.fori_loop(0, n_steps - block, send_part, 0)
        first.wait_send()
        for k in range(n_sum):
            wait_bytes(a_loc.at[k, pl.ds(0, half)], a_send.at[k])
        wait_bytes(fin_alpha, f_recv.at[0])
        wait_bytes(fin_ll, f_recv.at[1])
        alpha_ref[...] = fin_alpha[...]
        ll_ref[...] = fin_ll[...]

    @pl.when(core == 1)
    def owner():
        eye = (lax.broadcasted_iota(jnp.int32, (batch, SB), 0)
               == lax.broadcasted_iota(jnp.int32, (batch, SB), 1))

        def as_row(tile):
            col = jnp.sum(tile, axis=1, keepdims=True)
            return jnp.sum(jnp.where(eye, col, 0.0), axis=0, keepdims=True)

        def as_col(row):
            return jnp.sum(jnp.where(eye, row, 0.0), axis=1, keepdims=True)

        def start_gather(slot):
            for f, d in far_gather:
                there = slot_of[f, (nx - d) % nx]
                remote(r_in.at[slot, 0], r_in.at[slot, there], g_send, g_recv.at[slot, there // n_near],
                       gather_peer(f, d)).start()

        def start_parts(slot):
            for k in far:
                remote(p_in.at[slot, group], p_in.at[slot, group], p_send, p_recv.at[slot], sum_peer(k)).start()

        others = pl.ds(0, n_gather - 1)
        peers = pl.ds(0, n_sum - 1)

        def finish_norm(slot):
            wait_bytes(p_in.at[slot, peers], p_recv.at[slot])
            c_in[slot, c_place] = jnp.sum(p_in[slot], axis=0)
            for o in far_gather:
                remote(c_in.at[slot, c_place], c_in.at[slot, c_place], c_send, c_recv.at[slot], gather_peer(*o)).start()

        def wait_near(slot):
            if n_near > 1:
                wait_bytes(r_in.at[slot, pl.ds(0, n_near - 1)], g_recv.at[slot, 0])

        def wait_far(slot):
            wait_bytes(r_in.at[slot, pl.ds(0, n_far)], g_recv.at[slot, 1])

        def norm(slot):
            wait_bytes(c_in.at[slot, others], c_recv.at[slot])
            c_row = jnp.sum(c_in[slot], axis=0)
            c_col = as_col(c_row)
            inv = 1.0 / c_col
            return c_row, inv * (2.0 - c_col * inv)

        def keep(t, slot, c_row, inv):
            now = lax.convert_element_type(t, F32)
            active = now < len_col[...]
            for h in range(2):
                alpha_acc[h] = jnp.where(active, r_in[slot, 0, h] * inv, alpha_acc[h])
            ll_acc[...] = ll_acc[...] + jnp.where(now < len_row[...], jnp.log(c_row * (1.0 / LIFT)), 0.0)

        def add_w(b, k, fresh):
            part = lax.dot_general(e_loc[b, k], a_loc[k], (((1,), (1,)), ((), ())), preferred_element_type=F32)
            slot = b % 2
            w_loc[slot] = jnp.where(fresh, 0.0, w_loc[slot]) + part

        for k in far:
            announce(sum_peer(k), 1)
        for o in far_gather:
            announce(gather_peer(*o), 1)
        for k in range(n_sum):
            announce(sum_peer(k), 0)
        pl.semaphore_wait(barrier, n_sum + n_gather - 1)
        pair = remote(e_ref, e_both.at[pl.ds(0, n_steps * batch), pl.ds(SB, SB)], own_sem.at[0], e_pair, me, to=0)
        pair.start()
        for k in range(1, n_sum):
            start_a(1, k)
        for src, to in a_rows(me, 1):
            pltpu.make_async_copy(src, a_loc.at[0, to], own_sem.at[1]).start()
        alpha_acc[...] = jnp.zeros_like(alpha_acc)
        ll_acc[...] = jnp.zeros_like(ll_acc)
        w_loc[...] = jnp.zeros_like(w_loc)
        len_row[...] = jnp.zeros_like(len_row)
        len_row[:, :batch] = len_ref[...].astype(F32)
        len_col[...] = jnp.broadcast_to(as_col(len_row[...]), (batch, SB))
        r_in[0, 0, 1] = r0_ref[...]
        wait_bytes(r0_ref, r0_sem)
        p_in[0, group] = as_row(r_in[0, 0, 0] + r_in[0, 0, 1])
        start_parts(0)
        start_gather(0)
        finish_norm(0)
        wait_bytes(p_in.at[0, peers], p_send)
        wait_bytes(a_loc.at[0, pl.ds(0, half)], own_sem.at[1])

        def first_w(k, carry):
            wait_bytes(a_loc.at[k, pl.ds(0, half)], a_sem.at[k, 0])

            @pl.when(k > 0)
            def from_owner():
                wait_bytes(a_loc.at[k, pl.ds(0, half)], a_sem.at[k, 1])

            wait_bytes(e_loc.at[0, k], e_sem.at[0, k])
            add_w(0, k, False)
            return carry

        lax.fori_loop(0, n_sum, first_w, 0)
        pair.wait_send()
        for k in range(1, n_sum):
            wait_bytes(a_loc.at[k, pl.ds(0, half)], a_send.at[k])

        def one_step(t, carry):
            cur = t % 2
            nxt = (t + 1) % 2
            b = t // block
            row = pl.ds((t % block) * batch, batch)
            c_row, inv = norm(cur)
            total = jnp.zeros((batch, SB), F32)

            def take(first, last, total):
                for i in range(first, last):
                    for h in range(2):
                        cols = pl.ds((2 * i + h) * SB, SB)
                        tile = (r_in[cur, i, h] * inv).astype(BF16)
                        a_bf[:, cols] = tile
                        total = total + tile.astype(F32) * w_loc[b % 2, row, cols]
                return total

            def times(k, first, last):
                return jnp.dot(a_bf[:, first:last], a_loc[k, first:last], preferred_element_type=F32)

            order = far + [0]
            near_rows, all_rows = 2 * n_near * SB, 2 * half
            wait_near(cur)
            total = take(0, n_near, total)
            near = [times(k, 0, near_rows) for k in order[:NEAR]]
            wait_far(cur)
            total = take(n_near, n_gather, total)
            unit = jnp.where(t >= 0, jnp.float32(1.0), jnp.float32(0.0))
            ready = []

            def send_sum():
                k, part = ready.pop(0)
                for h in range(2):
                    u_out[k - 1, h] = part[:, h * SB:(h + 1) * SB]
                remote(u_out.at[k - 1], u_in.at[nxt, mirror(k) - 1], u_send, u_recv.at[nxt], sum_peer(k)).start()

            for i, k in enumerate(order):
                begin = near_rows if i < NEAR else 0
                middle = (begin + all_rows) // 2
                part = times(k, begin, middle) * unit + times(k, middle, all_rows)
                ready.append((k, part + near[i] if i < NEAR else part))
                if i == P_AFTER:
                    p_in[nxt, group] = as_row(total)
                    start_parts(nxt)
                if len(ready) > LAG:
                    send_sum()
            while len(ready) > 1:
                send_sum()
            own_part = ready[0][1]
            wait_bytes(r_in.at[cur, others], g_send)
            wait_bytes(c_in.at[cur, others], c_send)
            keep(t, cur, c_row, inv)
            finish_norm(nxt)
            wait_bytes(u_in.at[nxt], u_recv.at[nxt])
            for h in range(2):
                parts = [own_part[:, h * SB:(h + 1) * SB]] + [u_in[nxt, k, h] for k in range(n_sum - 1)]
                while len(parts) > 1:
                    parts = [parts[i] + parts[i + 1] for i in range(0, len(parts), 2)]
                r_in[nxt, 0, h] = parts[0] * e_loc[b, 0, row, pl.ds(h * SB, SB)].astype(F32)
            start_gather(nxt)

            @pl.when(t < n_steps - block - AHEAD)
            def go_on():
                pl.semaphore_signal(tick, inc=1, device_id={'rows': 0, 'states': me},
                                    device_id_type=pl.DeviceIdType.MESH)

            @pl.when(b + 1 < n_blocks)
            def next_w():
                later = b + 1
                for n in range(per_step):
                    k = (t % block) * per_step + n
                    wait_bytes(e_loc.at[later, k], e_sem.at[later % 2, k])
                    add_w(later, k, k == 0)

            wait_bytes(u_out, u_send)
            wait_bytes(p_in.at[nxt, peers], p_send)
            return carry

        lax.fori_loop(0, n_steps - 1, one_step, 0)
        last = (n_steps - 1) % 2
        c_row, inv = norm(last)
        wait_near(last)
        wait_far(last)
        keep(n_steps - 1, last, c_row, inv)
        wait_bytes(r_in.at[last, others], g_send)
        wait_bytes(c_in.at[last, others], c_send)
        result = [remote(alpha_acc.at[0], fin_alpha, f_send.at[0], f_recv.at[0], me, to=0),
                  remote(ll_acc, fin_ll, f_send.at[1], f_recv.at[1], me, to=0)]
        for copy in result:
            copy.start()
        alpha_ref[...] = alpha_acc[1]
        ll_ref[...] = ll_acc[...]
        for copy in result:
            copy.wait_send()


def solution(mesh):
    vec_axes = ('rows', 'states')
    nz, ny, nx = CHIPS
    n_sum, n_gather = 2 * nz, 2 * nx

    def local_forward(trans_blk, emit_blk, init_blk, tokens, lengths):
        batch, n_steps = tokens.shape
        cols = 2 * SB
        a_blk = trans_blk.reshape(trans_blk.shape[0], cols)
        emis = jnp.transpose(emit_blk.at[:, tokens].get(mode='promise_in_bounds'), (2, 1, 0))
        emis = emis * jnp.asarray(LIFT, emis.dtype)
        first_raw = init_blk[None, :] * emis[0].astype(F32)
        vmem = pl.BlockSpec(memory_space=pltpu.VMEM)
        hbm = pl.BlockSpec(memory_space=pl.ANY)
        dma = pltpu.SemaphoreType.DMA
        k_rows = 2 * n_gather * SB
        block = min(BLOCK, n_sum)
        block_rows = block * batch
        n_blocks = n_steps // block
        alpha, ll = pl.pallas_call(
            functools.partial(forward_kernel, CHIPS, n_steps, block),
            out_shape=(jax.ShapeDtypeStruct((batch, SB), F32), jax.ShapeDtypeStruct((1, SB), F32)),
            in_specs=[hbm, hbm, vmem, vmem],
            out_specs=(vmem, vmem),
            scratch_shapes=[
                pltpu.VMEM((n_sum, k_rows, cols), BF16),
                pltpu.VMEM(((n_steps + 1) * batch, cols), BF16),
                pltpu.VMEM((n_blocks, n_sum, block_rows, cols), BF16),
                pltpu.VMEM((2, block_rows, k_rows), F32),
                pltpu.VMEM((2, n_gather, 2, batch, SB), F32),
                pltpu.VMEM((2, n_gather, 1, SB), F32),
                pltpu.VMEM((2, n_sum, 1, SB), F32),
                pltpu.VMEM((2, n_sum - 1, 2, batch, SB), F32),
                pltpu.VMEM((n_sum - 1, 2, batch, SB), F32),
                pltpu.VMEM((batch, k_rows), BF16),
                pltpu.VMEM((1, SB), F32),
                pltpu.VMEM((batch, SB), F32),
                pltpu.VMEM((2, batch, SB), F32),
                pltpu.VMEM((1, SB), F32),
                pltpu.VMEM((batch, SB), F32),
                pltpu.VMEM((1, SB), F32),
                pltpu.SemaphoreType.REGULAR,
                dma((n_sum, 2)), dma((n_sum,)), dma, dma, dma((2, n_sum)), dma, dma, dma((2,)),
                dma((2, 2)), dma, dma((2,)), dma, dma((2,)), dma, dma((2,)), dma, dma((2,)), dma((2,)),
            ],
            compiler_params=pltpu.CompilerParams(collective_id=0, has_side_effects=True,
                                                 vmem_limit_bytes=48 * 1024 * 1024),
            cost_estimate=pl.CostEstimate(flops=2 * batch * (n_steps - 1) * n_sum * k_rows * cols,
                                          bytes_accessed=n_sum * k_rows * cols * 2, transcendentals=0),
        )(a_blk, emis.reshape(n_steps * batch, SB), first_raw, lengths[None, :])
        return ll[0, :batch], alpha

    return jax.shard_map(local_forward, mesh=mesh, in_specs=(P('rows', None, 'states'), P(vec_axes, None), P(vec_axes), P('seqs', None), P('seqs')), out_specs=(P('seqs'), P('seqs', vec_axes)), check_vma=False)
```

```python
import functools

import jax
import jax.numpy as jnp
from jax import lax
from jax.experimental import pallas as pl
from jax.experimental.pallas import tpu as pltpu
from jax.sharding import PartitionSpec as P

CHIPS = (4, 4, 4)
SB = 128
LIFT = 2.0 ** 64
LAG = 1
P_AFTER = 1
NEAR = 0
BLOCK = 8
AHEAD = 6
F32 = jnp.float32
BF16 = jnp.bfloat16


def ring_distance(offset, n):
    return min(offset, n - offset)


def forward_kernel(dims, n_steps, block, a_ref, emit_ref, init_ref, tok_ref, len_ref, alpha_ref, ll_ref,
                   a_loc, e_both, e_loc, w_loc, r_in, c_in, p_in, u_in, u_out, a_bf, len_row, len_col, alpha_acc, ll_acc,
                   fin_alpha, fin_ll, by_word, picked, e_half, r0_own, tick, a_sem, a_send, e_pair, e_send, e_sem, r0_sem, r0_send, own_sem,
                   g_recv, g_send, c_recv, c_send, u_recv, u_send, p_recv, p_send, f_recv, f_send):
    nz, ny, nx = dims
    n_sum, n_gather = 2 * nz, 2 * nx
    batch = tok_ref.shape[0]
    half = n_gather * SB
    rows = block * batch
    n_blocks = n_steps // block
    per_step = n_sum // block
    core = lax.axis_index('rows')
    me = lax.axis_index('states')
    z = me // (ny * nx)
    y = (me // nx) % ny
    x = me % nx
    group = me // n_gather
    c_place = (((y + 1) // 2) % 2) * nx + x
    far = sorted(range(1, n_sum), key=lambda k: -(ring_distance(k // 2, nz) + k % 2))
    sources = sorted(((f, d) for f in range(2) for d in range(nx)), key=lambda o: o[0] + ring_distance(o[1], nx))
    slot_of = {o: i for i, o in enumerate(sources)}
    far_gather = sources[:0:-1]
    n_near = n_gather // 2
    n_far = n_gather - n_near

    def sum_peer(k, sign=1):
        flip = k % 2
        return ((z + sign * (k // 2) + nz) % nz) * ny * nx + (y + flip * (ny - 1 - 2 * y)) * nx + x

    def mirror(k):
        return ((nz - k // 2) % nz) * 2 + k % 2

    def gather_peer(flip, d):
        return (me // (ny * nx)) * ny * nx + (y + flip * (1 - 2 * (y % 2))) * nx + (x + d) % nx

    def remote(src, dst, send, recv, state, to=1):
        return pltpu.make_async_remote_copy(src_ref=src, dst_ref=dst, send_sem=send, recv_sem=recv,
                                            device_id={'rows': to, 'states': state},
                                            device_id_type=pl.DeviceIdType.MESH)

    def wait_bytes(ref, sem):
        pltpu.make_async_copy(ref, ref, sem).wait()

    def a_rows(state, h):
        for i, (f, d) in enumerate(sources):
            there = ((state // nx + f) % 2) * nx + (x + d) % nx
            yield (a_ref.at[pl.ds((state // n_gather) * half + there * SB, SB)], pl.ds((2 * i + h) * SB, SB))

    def start_a(h, k):
        peer = sum_peer(k, -1)
        for src, to in a_rows(peer, h):
            remote(src, a_loc.at[k, to], a_send.at[k], a_sem.at[k, h], peer).start()

    def e_copy(b, k):
        return remote(e_both.at[pl.ds(b * rows + batch, rows)], e_loc.at[b, k], e_send, e_sem.at[b % 2, k], sum_peer(k, -1))

    def pick_tokens():
        n_words = emit_ref.shape[1]

        def turn(first, count):
            tile = emit_ref[:, pl.ds(first, count)].astype(F32) * LIFT
            by_word[pl.ds(first, count), :] = tile.T

        def turn_tiles(i, carry):
            turn(pl.multiple_of(i * SB, SB), SB)
            return carry

        lax.fori_loop(0, n_words // SB, turn_tiles, 0, unroll=2)
        if n_words % SB:
            turn(n_words // SB * SB, n_words % SB)

        def pick(t, carry):
            for b in range(batch):
                picked[t, b:b + 1, :] = by_word[pl.ds(tok_ref[b, t], 1), :]
            e_half[pl.ds(pl.multiple_of(t * batch, batch), batch), :] = picked[t].astype(BF16)
            return carry

        lax.fori_loop(0, n_steps, pick, 0)
        r0_own[...] = picked[0] * init_ref[...]

    barrier = pltpu.get_barrier_semaphore()

    def announce(state, to):
        pl.semaphore_signal(barrier, inc=1, device_id={'rows': to, 'states': state}, device_id_type=pl.DeviceIdType.MESH)

    @pl.when(core == 0)
    def helper():
        announce(me, 1)
        pl.semaphore_wait(barrier, n_sum)
        for k in range(n_sum):
            start_a(0, k)
        e_both[pl.ds(n_steps * batch, batch), :] = jnp.zeros((batch, 2 * SB), BF16)
        pick_tokens()
        first = remote(r0_own, r_in.at[0, 0, 0], r0_send, r0_sem, me)
        first.start()
        every = pl.ds(0, n_steps * batch)
        mine = pltpu.make_async_copy(e_half, e_both.at[every, pl.ds(0, SB)], own_sem.at[0])
        mine.start()
        mine.wait()
        wait_bytes(e_both.at[every, pl.ds(SB, SB)], e_pair)
        for k in range(n_sum):
            e_copy(0, k).start()
        wait_bytes(e_loc.at[0], e_send)

        def send_part(i, carry):
            @pl.when(i >= AHEAD)
            def paced():
                pl.semaphore_wait(tick, 1)

            for n in range(per_step):
                e_copy(1 + i // block, (i % block) * per_step + n).start()
            wait_bytes(e_loc.at[0, pl.ds(0, per_step)], e_send)
            return carry

        lax.fori_loop(0, n_steps - block, send_part, 0)
        first.wait_send()
        for k in range(n_sum):
            wait_bytes(a_loc.at[k, pl.ds(0, half)], a_send.at[k])
        wait_bytes(fin_alpha, f_recv.at[0])
        wait_bytes(fin_ll, f_recv.at[1])
        alpha_ref[...] = fin_alpha[...]
        ll_ref[...] = fin_ll[:, :batch]

    @pl.when(core == 1)
    def owner():
        eye = (lax.broadcasted_iota(jnp.int32, (batch, SB), 0)
               == lax.broadcasted_iota(jnp.int32, (batch, SB), 1))

        def as_row(tile):
            col = jnp.sum(tile, axis=1, keepdims=True)
            return jnp.sum(jnp.where(eye, col, 0.0), axis=0, keepdims=True)

        def as_col(row):
            return jnp.sum(jnp.where(eye, row, 0.0), axis=1, keepdims=True)

        def start_gather(slot):
            for f, d in far_gather:
                there = slot_of[f, (nx - d) % nx]
                remote(r_in.at[slot, 0], r_in.at[slot, there], g_send, g_recv.at[slot, there // n_near],
                       gather_peer(f, d)).start()

        def start_parts(slot):
            for k in far:
                remote(p_in.at[slot, group], p_in.at[slot, group], p_send, p_recv.at[slot], sum_peer(k)).start()

        others = pl.ds(0, n_gather - 1)
        peers = pl.ds(0, n_sum - 1)

        def finish_norm(slot):
            wait_bytes(p_in.at[slot, peers], p_recv.at[slot])
            c_in[slot, c_place] = jnp.sum(p_in[slot], axis=0)
            for o in far_gather:
                remote(c_in.at[slot, c_place], c_in.at[slot, c_place], c_send, c_recv.at[slot], gather_peer(*o)).start()

        def wait_near(slot):
            if n_near > 1:
                wait_bytes(r_in.at[slot, pl.ds(0, n_near - 1)], g_recv.at[slot, 0])

        def wait_far(slot):
            wait_bytes(r_in.at[slot, pl.ds(0, n_far)], g_recv.at[slot, 1])

        def norm(slot):
            wait_bytes(c_in.at[slot, others], c_recv.at[slot])
            c_row = jnp.sum(c_in[slot], axis=0)
            c_col = as_col(c_row)
            inv = 1.0 / c_col
            return c_row, inv * (2.0 - c_col * inv)

        def keep(t, slot, c_row, inv):
            now = lax.convert_element_type(t, F32)
            active = now < len_col[...]
            for h in range(2):
                alpha_acc[h] = jnp.where(active, r_in[slot, 0, h] * inv, alpha_acc[h])
            ll_acc[...] = ll_acc[...] + jnp.where(now < len_row[...], jnp.log(c_row * (1.0 / LIFT)), 0.0)

        def add_w(b, k, fresh):
            part = lax.dot_general(e_loc[b, k], a_loc[k], (((1,), (1,)), ((), ())), preferred_element_type=F32)
            slot = b % 2
            w_loc[slot] = jnp.where(fresh, 0.0, w_loc[slot]) + part

        for k in far:
            announce(sum_peer(k), 1)
        for o in far_gather:
            announce(gather_peer(*o), 1)
        for k in range(n_sum):
            announce(sum_peer(k), 0)
        pl.semaphore_wait(barrier, n_sum + n_gather - 1)
        for k in range(1, n_sum):
            start_a(1, k)
        for src, to in a_rows(me, 1):
            pltpu.make_async_copy(src, a_loc.at[0, to], own_sem.at[1]).start()
        pick_tokens()
        alpha_acc[...] = jnp.zeros_like(alpha_acc)
        ll_acc[...] = jnp.zeros_like(ll_acc)
        w_loc[...] = jnp.zeros_like(w_loc)
        len_row[...] = jnp.zeros_like(len_row)
        len_row[:, :batch] = len_ref[...].astype(F32)
        len_col[...] = jnp.broadcast_to(as_col(len_row[...]), (batch, SB))
        pair = remote(e_half, e_both.at[pl.ds(0, n_steps * batch), pl.ds(SB, SB)], own_sem.at[0], e_pair, me, to=0)
        pair.start()
        r_in[0, 0, 1] = r0_own[...]
        wait_bytes(r0_own, r0_sem)
        p_in[0, group] = as_row(r_in[0, 0, 0] + r_in[0, 0, 1])
        start_parts(0)
        start_gather(0)
        finish_norm(0)
        wait_bytes(p_in.at[0, peers], p_send)
        wait_bytes(a_loc.at[0, pl.ds(0, half)], own_sem.at[1])

        def first_w(k, carry):
            wait_bytes(a_loc.at[k, pl.ds(0, half)], a_sem.at[k, 0])

            @pl.when(k > 0)
            def from_owner():
                wait_bytes(a_loc.at[k, pl.ds(0, half)], a_sem.at[k, 1])

            wait_bytes(e_loc.at[0, k], e_sem.at[0, k])
            add_w(0, k, False)
            return carry

        lax.fori_loop(0, n_sum, first_w, 0)
        pair.wait_send()
        for k in range(1, n_sum):
            wait_bytes(a_loc.at[k, pl.ds(0, half)], a_send.at[k])

        def one_step(t, carry):
            cur = t % 2
            nxt = (t + 1) % 2
            b = t // block
            row = pl.ds((t % block) * batch, batch)
            c_row, inv = norm(cur)
            total = jnp.zeros((batch, SB), F32)

            def take(first, last, total):
                for i in range(first, last):
                    for h in range(2):
                        cols = pl.ds((2 * i + h) * SB, SB)
                        tile = (r_in[cur, i, h] * inv).astype(BF16)
                        a_bf[:, cols] = tile
                        total = total + tile.astype(F32) * w_loc[b % 2, row, cols]
                return total

            def times(k, first, last):
                return jnp.dot(a_bf[:, first:last], a_loc[k, first:last], preferred_element_type=F32)

            order = far + [0]
            near_rows, all_rows = 2 * n_near * SB, 2 * half
            wait_near(cur)
            total = take(0, n_near, total)
            near = [times(k, 0, near_rows) for k in order[:NEAR]]
            wait_far(cur)
            total = take(n_near, n_gather, total)
            unit = jnp.where(t >= 0, jnp.float32(1.0), jnp.float32(0.0))
            ready = []

            def send_sum():
                k, part = ready.pop(0)
                for h in range(2):
                    u_out[k - 1, h] = part[:, h * SB:(h + 1) * SB]
                remote(u_out.at[k - 1], u_in.at[nxt, mirror(k) - 1], u_send, u_recv.at[nxt], sum_peer(k)).start()

            for i, k in enumerate(order):
                begin = near_rows if i < NEAR else 0
                middle = (begin + all_rows) // 2
                part = times(k, begin, middle) * unit + times(k, middle, all_rows)
                ready.append((k, part + near[i] if i < NEAR else part))
                if i == P_AFTER:
                    p_in[nxt, group] = as_row(total)
                    start_parts(nxt)
                if len(ready) > LAG:
                    send_sum()
            while len(ready) > 1:
                send_sum()
            own_part = ready[0][1]
            wait_bytes(r_in.at[cur, others], g_send)
            wait_bytes(c_in.at[cur, others], c_send)
            keep(t, cur, c_row, inv)
            finish_norm(nxt)
            wait_bytes(u_in.at[nxt], u_recv.at[nxt])
            for h in range(2):
                parts = [own_part[:, h * SB:(h + 1) * SB]] + [u_in[nxt, k, h] for k in range(n_sum - 1)]
                while len(parts) > 1:
                    parts = [parts[i] + parts[i + 1] for i in range(0, len(parts), 2)]
                r_in[nxt, 0, h] = parts[0] * e_loc[b, 0, row, pl.ds(h * SB, SB)].astype(F32)
            start_gather(nxt)

            @pl.when(t < n_steps - block - AHEAD)
            def go_on():
                pl.semaphore_signal(tick, inc=1, device_id={'rows': 0, 'states': me},
                                    device_id_type=pl.DeviceIdType.MESH)

            @pl.when(b + 1 < n_blocks)
            def next_w():
                later = b + 1
                for n in range(per_step):
                    k = (t % block) * per_step + n
                    wait_bytes(e_loc.at[later, k], e_sem.at[later % 2, k])
                    add_w(later, k, k == 0)

            wait_bytes(u_out, u_send)
            wait_bytes(p_in.at[nxt, peers], p_send)
            return carry

        lax.fori_loop(0, n_steps - 1, one_step, 0)
        last = (n_steps - 1) % 2
        c_row, inv = norm(last)
        wait_near(last)
        wait_far(last)
        keep(n_steps - 1, last, c_row, inv)
        wait_bytes(r_in.at[last, others], g_send)
        wait_bytes(c_in.at[last, others], c_send)
        result = [remote(alpha_acc.at[0], fin_alpha, f_send.at[0], f_recv.at[0], me, to=0),
                  remote(ll_acc, fin_ll, f_send.at[1], f_recv.at[1], me, to=0)]
        for copy in result:
            copy.start()
        alpha_ref[...] = alpha_acc[1]
        ll_ref[...] = ll_acc[:, :batch]
        for copy in result:
            copy.wait_send()


def solution(mesh):
    vec_axes = ('rows', 'states')
    nz, ny, nx = CHIPS
    n_sum, n_gather = 2 * nz, 2 * nx

    def local_forward(trans_blk, emit_blk, init_blk, tokens, lengths):
        batch, n_steps = tokens.shape
        cols = 2 * SB
        a_blk = trans_blk.reshape(trans_blk.shape[0], cols)
        vmem = pl.BlockSpec(memory_space=pltpu.VMEM)
        hbm = pl.BlockSpec(memory_space=pl.ANY)
        dma = pltpu.SemaphoreType.DMA
        k_rows = 2 * n_gather * SB
        block = min(BLOCK, n_sum)
        block_rows = block * batch
        n_blocks = n_steps // block
        alpha, ll = pl.pallas_call(
            functools.partial(forward_kernel, CHIPS, n_steps, block),
            out_shape=(jax.ShapeDtypeStruct((batch, SB), F32), jax.ShapeDtypeStruct((1, batch), F32)),
            in_specs=[hbm, vmem, vmem, pl.BlockSpec(memory_space=pltpu.SMEM), vmem],
            out_specs=(vmem, vmem),
            scratch_shapes=[
                pltpu.VMEM((n_sum, k_rows, cols), BF16),
                pltpu.VMEM(((n_steps + 1) * batch, cols), BF16),
                pltpu.VMEM((n_blocks, n_sum, block_rows, cols), BF16),
                pltpu.VMEM((2, block_rows, k_rows), F32),
                pltpu.VMEM((2, n_gather, 2, batch, SB), F32),
                pltpu.VMEM((2, n_gather, 1, SB), F32),
                pltpu.VMEM((2, n_sum, 1, SB), F32),
                pltpu.VMEM((2, n_sum - 1, 2, batch, SB), F32),
                pltpu.VMEM((n_sum - 1, 2, batch, SB), F32),
                pltpu.VMEM((batch, k_rows), BF16),
                pltpu.VMEM((1, SB), F32),
                pltpu.VMEM((batch, SB), F32),
                pltpu.VMEM((2, batch, SB), F32),
                pltpu.VMEM((1, SB), F32),
                pltpu.VMEM((batch, SB), F32),
                pltpu.VMEM((1, SB), F32),
                pltpu.VMEM((emit_blk.shape[1], SB), F32),
                pltpu.VMEM((n_steps, batch, SB), F32),
                pltpu.VMEM((n_steps * batch, SB), BF16),
                pltpu.VMEM((batch, SB), F32),
                pltpu.SemaphoreType.REGULAR,
                dma((n_sum, 2)), dma((n_sum,)), dma, dma, dma((2, n_sum)), dma, dma, dma((2,)),
                dma((2, 2)), dma, dma((2,)), dma, dma((2,)), dma, dma((2,)), dma, dma((2,)), dma((2,)),
            ],
            compiler_params=pltpu.CompilerParams(collective_id=0, has_side_effects=True,
                                                 vmem_limit_bytes=48 * 1024 * 1024),
            cost_estimate=pl.CostEstimate(flops=2 * batch * (n_steps - 1) * n_sum * k_rows * cols,
                                          bytes_accessed=n_sum * k_rows * cols * 2, transcendentals=0),
        )(a_blk, emit_blk, init_blk[None, :], tokens, lengths[None, :])
        return ll[0], alpha

    return jax.shard_map(local_forward, mesh=mesh, in_specs=(P('rows', None, 'states'), P(vec_axes, None), P(vec_axes), P('seqs', None), P('seqs')), out_specs=(P('seqs'), P('seqs', vec_axes)), check_vma=False)
```

```python
import functools

import jax
import jax.numpy as jnp
from jax import lax
from jax.experimental import pallas as pl
from jax.experimental.pallas import tpu as pltpu
from jax.sharding import PartitionSpec as P

CHIPS = (4, 4, 4)
SB = 128
LIFT = 2.0 ** 64
LAG = 1
P_AFTER = 1
NEAR = 0
BLOCK = 8
AHEAD = 6
F32 = jnp.float32
BF16 = jnp.bfloat16


def ring_distance(offset, n):
    return min(offset, n - offset)


def forward_kernel(dims, n_steps, block, a_ref, emit_ref, init_ref, tok_ref, len_ref, alpha_ref, ll_ref,
                   a_loc, e_both, e_loc, w_loc, r_in, c_in, p_in, u_in, u_out, a_bf, len_row, len_col, alpha_acc, ll_acc,
                   fin_alpha, fin_ll, by_word, picked, e_half, r0_own, tick, a_sem, a_send, e_pair, e_send, e_sem, r0_sem, r0_send, own_sem,
                   g_recv, g_send, c_recv, c_send, u_recv, u_send, p_recv, p_send, f_recv, f_send):
    nz, ny, nx = dims
    n_sum, n_gather = 2 * nz, 2 * nx
    batch = tok_ref.shape[0]
    half = n_gather * SB
    rows = block * batch
    n_blocks = n_steps // block
    per_step = n_sum // block
    core = lax.axis_index('rows')
    me = lax.axis_index('states')
    z = me // (ny * nx)
    y = (me // nx) % ny
    x = me % nx
    group = me // n_gather
    c_place = (((y + 1) // 2) % 2) * nx + x
    far = sorted(range(1, n_sum), key=lambda k: -(ring_distance(k // 2, nz) + k % 2))
    sources = sorted(((f, d) for f in range(2) for d in range(nx)), key=lambda o: o[0] + ring_distance(o[1], nx))
    slot_of = {o: i for i, o in enumerate(sources)}
    far_gather = sources[:0:-1]
    n_near = n_gather // 2
    n_far = n_gather - n_near

    def sum_peer(k, sign=1):
        flip = k % 2
        return ((z + sign * (k // 2) + nz) % nz) * ny * nx + (y + flip * (ny - 1 - 2 * y)) * nx + x

    def mirror(k):
        return ((nz - k // 2) % nz) * 2 + k % 2

    def gather_peer(flip, d):
        return (me // (ny * nx)) * ny * nx + (y + flip * (1 - 2 * (y % 2))) * nx + (x + d) % nx

    def remote(src, dst, send, recv, state, to=1):
        return pltpu.make_async_remote_copy(src_ref=src, dst_ref=dst, send_sem=send, recv_sem=recv,
                                            device_id={'rows': to, 'states': state},
                                            device_id_type=pl.DeviceIdType.MESH)

    def wait_bytes(ref, sem):
        pltpu.make_async_copy(ref, ref, sem).wait()

    def a_rows(state, h):
        for i, (f, d) in enumerate(sources):
            there = ((state // nx + f) % 2) * nx + (x + d) % nx
            yield (a_ref.at[pl.ds((state // n_gather) * half + there * SB, SB)], pl.ds((2 * i + h) * SB, SB))

    def start_a(h, k):
        peer = sum_peer(k, -1)
        for src, to in a_rows(peer, h):
            remote(src, a_loc.at[k, to], a_send.at[k], a_sem.at[k, h], peer).start()

    def e_copy(b, k):
        return remote(e_both.at[pl.ds(b * rows + batch, rows)], e_loc.at[b, k], e_send, e_sem.at[b % 2, k], sum_peer(k, -1))

    def pick_tokens():
        def widen(i, carry):
            some = pl.ds(pl.multiple_of(i * batch, batch), batch)
            by_word[some, :] = emit_ref[some, :].astype(F32) * LIFT
            return carry

        lax.fori_loop(0, emit_ref.shape[0] // batch, widen, 0, unroll=5)

        def pick(t, carry):
            for b in range(batch):
                picked[t, b:b + 1, :] = by_word[pl.ds(tok_ref[b, t], 1), :]
            e_half[pl.ds(pl.multiple_of(t * batch, batch), batch), :] = picked[t].astype(BF16)
            return carry

        lax.fori_loop(0, n_steps, pick, 0)
        r0_own[...] = picked[0] * init_ref[...]

    barrier = pltpu.get_barrier_semaphore()

    def announce(state, to):
        pl.semaphore_signal(barrier, inc=1, device_id={'rows': to, 'states': state}, device_id_type=pl.DeviceIdType.MESH)

    @pl.when(core == 0)
    def helper():
        announce(me, 1)
        pl.semaphore_wait(barrier, n_sum)
        for k in range(n_sum):
            start_a(0, k)
        e_both[pl.ds(n_steps * batch, batch), :] = jnp.zeros((batch, 2 * SB), BF16)
        pick_tokens()
        first = remote(r0_own, r_in.at[0, 0, 0], r0_send, r0_sem, me)
        first.start()
        every = pl.ds(0, n_steps * batch)
        mine = pltpu.make_async_copy(e_half, e_both.at[every, pl.ds(0, SB)], own_sem.at[0])
        mine.start()
        mine.wait()
        wait_bytes(e_both.at[every, pl.ds(SB, SB)], e_pair)
        for k in range(n_sum):
            e_copy(0, k).start()
        wait_bytes(e_loc.at[0], e_send)

        def send_part(i, carry):
            @pl.when(i >= AHEAD)
            def paced():
                pl.semaphore_wait(tick, 1)

            for n in range(per_step):
                e_copy(1 + i // block, (i % block) * per_step + n).start()
            wait_bytes(e_loc.at[0, pl.ds(0, per_step)], e_send)
            return carry

        lax.fori_loop(0, n_steps - block, send_part, 0)
        first.wait_send()
        for k in range(n_sum):
            wait_bytes(a_loc.at[k, pl.ds(0, half)], a_send.at[k])
        wait_bytes(fin_alpha, f_recv.at[0])
        wait_bytes(fin_ll, f_recv.at[1])
        alpha_ref[...] = fin_alpha[...]
        ll_ref[...] = fin_ll[:, :batch]

    @pl.when(core == 1)
    def owner():
        eye = (lax.broadcasted_iota(jnp.int32, (batch, SB), 0)
               == lax.broadcasted_iota(jnp.int32, (batch, SB), 1))

        def as_row(tile):
            col = jnp.sum(tile, axis=1, keepdims=True)
            return jnp.sum(jnp.where(eye, col, 0.0), axis=0, keepdims=True)

        def as_col(row):
            return jnp.sum(jnp.where(eye, row, 0.0), axis=1, keepdims=True)

        def start_gather(slot):
            for f, d in far_gather:
                there = slot_of[f, (nx - d) % nx]
                remote(r_in.at[slot, 0], r_in.at[slot, there], g_send, g_recv.at[slot, there // n_near],
                       gather_peer(f, d)).start()

        def start_parts(slot):
            for k in far:
                remote(p_in.at[slot, group], p_in.at[slot, group], p_send, p_recv.at[slot], sum_peer(k)).start()

        others = pl.ds(0, n_gather - 1)
        peers = pl.ds(0, n_sum - 1)

        def finish_norm(slot):
            wait_bytes(p_in.at[slot, peers], p_recv.at[slot])
            c_in[slot, c_place] = jnp.sum(p_in[slot], axis=0)
            for o in far_gather:
                remote(c_in.at[slot, c_place], c_in.at[slot, c_place], c_send, c_recv.at[slot], gather_peer(*o)).start()

        def wait_near(slot):
            if n_near > 1:
                wait_bytes(r_in.at[slot, pl.ds(0, n_near - 1)], g_recv.at[slot, 0])

        def wait_far(slot):
            wait_bytes(r_in.at[slot, pl.ds(0, n_far)], g_recv.at[slot, 1])

        def norm(slot):
            wait_bytes(c_in.at[slot, others], c_recv.at[slot])
            c_row = jnp.sum(c_in[slot], axis=0)
            c_col = as_col(c_row)
            inv = 1.0 / c_col
            return c_row, inv * (2.0 - c_col * inv)

        def keep(t, slot, c_row, inv):
            now = lax.convert_element_type(t, F32)
            active = now < len_col[...]
            for h in range(2):
                alpha_acc[h] = jnp.where(active, r_in[slot, 0, h] * inv, alpha_acc[h])
            ll_acc[...] = ll_acc[...] + jnp.where(now < len_row[...], jnp.log(c_row * (1.0 / LIFT)), 0.0)

        def add_w(b, k, fresh):
            part = lax.dot_general(e_loc[b, k], a_loc[k], (((1,), (1,)), ((), ())), preferred_element_type=F32)
            slot = b % 2
            w_loc[slot] = jnp.where(fresh, 0.0, w_loc[slot]) + part

        for k in far:
            announce(sum_peer(k), 1)
        for o in far_gather:
            announce(gather_peer(*o), 1)
        for k in range(n_sum):
            announce(sum_peer(k), 0)
        pl.semaphore_wait(barrier, n_sum + n_gather - 1)
        for k in range(1, n_sum):
            start_a(1, k)
        for src, to in a_rows(me, 1):
            pltpu.make_async_copy(src, a_loc.at[0, to], own_sem.at[1]).start()
        pick_tokens()
        alpha_acc[...] = jnp.zeros_like(alpha_acc)
        ll_acc[...] = jnp.zeros_like(ll_acc)
        w_loc[...] = jnp.zeros_like(w_loc)
        len_row[...] = jnp.zeros_like(len_row)
        len_row[:, :batch] = len_ref[...].astype(F32)
        len_col[...] = jnp.broadcast_to(as_col(len_row[...]), (batch, SB))
        pair = remote(e_half, e_both.at[pl.ds(0, n_steps * batch), pl.ds(SB, SB)], own_sem.at[0], e_pair, me, to=0)
        pair.start()
        r_in[0, 0, 1] = r0_own[...]
        wait_bytes(r0_own, r0_sem)
        p_in[0, group] = as_row(r_in[0, 0, 0] + r_in[0, 0, 1])
        start_parts(0)
        start_gather(0)
        finish_norm(0)
        wait_bytes(p_in.at[0, peers], p_send)
        wait_bytes(a_loc.at[0, pl.ds(0, half)], own_sem.at[1])

        def first_w(k, carry):
            wait_bytes(a_loc.at[k, pl.ds(0, half)], a_sem.at[k, 0])

            @pl.when(k > 0)
            def from_owner():
                wait_bytes(a_loc.at[k, pl.ds(0, half)], a_sem.at[k, 1])

            wait_bytes(e_loc.at[0, k], e_sem.at[0, k])
            add_w(0, k, False)
            return carry

        lax.fori_loop(0, n_sum, first_w, 0)
        pair.wait_send()
        for k in range(1, n_sum):
            wait_bytes(a_loc.at[k, pl.ds(0, half)], a_send.at[k])

        def one_step(t, carry):
            cur = t % 2
            nxt = (t + 1) % 2
            b = t // block
            row = pl.ds((t % block) * batch, batch)
            c_row, inv = norm(cur)
            total = jnp.zeros((batch, SB), F32)

            def take(first, last, total):
                for i in range(first, last):
                    for h in range(2):
                        cols = pl.ds((2 * i + h) * SB, SB)
                        tile = (r_in[cur, i, h] * inv).astype(BF16)
                        a_bf[:, cols] = tile
                        total = total + tile.astype(F32) * w_loc[b % 2, row, cols]
                return total

            def times(k, first, last):
                return jnp.dot(a_bf[:, first:last], a_loc[k, first:last], preferred_element_type=F32)

            order = far + [0]
            near_rows, all_rows = 2 * n_near * SB, 2 * half
            wait_near(cur)
            total = take(0, n_near, total)
            near = [times(k, 0, near_rows) for k in order[:NEAR]]
            wait_far(cur)
            total = take(n_near, n_gather, total)
            unit = jnp.where(t >= 0, jnp.float32(1.0), jnp.float32(0.0))
            ready = []

            def send_sum():
                k, part = ready.pop(0)
                for h in range(2):
                    u_out[k - 1, h] = part[:, h * SB:(h + 1) * SB]
                remote(u_out.at[k - 1], u_in.at[nxt, mirror(k) - 1], u_send, u_recv.at[nxt], sum_peer(k)).start()

            for i, k in enumerate(order):
                begin = near_rows if i < NEAR else 0
                middle = (begin + all_rows) // 2
                part = times(k, begin, middle) * unit + times(k, middle, all_rows)
                ready.append((k, part + near[i] if i < NEAR else part))
                if i == P_AFTER:
                    p_in[nxt, group] = as_row(total)
                    start_parts(nxt)
                if len(ready) > LAG:
                    send_sum()
            while len(ready) > 1:
                send_sum()
            own_part = ready[0][1]
            wait_bytes(r_in.at[cur, others], g_send)
            wait_bytes(c_in.at[cur, others], c_send)
            keep(t, cur, c_row, inv)
            finish_norm(nxt)
            wait_bytes(u_in.at[nxt], u_recv.at[nxt])
            for h in range(2):
                parts = [own_part[:, h * SB:(h + 1) * SB]] + [u_in[nxt, k, h] for k in range(n_sum - 1)]
                while len(parts) > 1:
                    parts = [parts[i] + parts[i + 1] for i in range(0, len(parts), 2)]
                r_in[nxt, 0, h] = parts[0] * e_loc[b, 0, row, pl.ds(h * SB, SB)].astype(F32)
            start_gather(nxt)

            @pl.when(t < n_steps - block - AHEAD)
            def go_on():
                pl.semaphore_signal(tick, inc=1, device_id={'rows': 0, 'states': me},
                                    device_id_type=pl.DeviceIdType.MESH)

            @pl.when(b + 1 < n_blocks)
            def next_w():
                later = b + 1
                for n in range(per_step):
                    k = (t % block) * per_step + n
                    wait_bytes(e_loc.at[later, k], e_sem.at[later % 2, k])
                    add_w(later, k, k == 0)

            wait_bytes(u_out, u_send)
            wait_bytes(p_in.at[nxt, peers], p_send)
            return carry

        lax.fori_loop(0, n_steps - 1, one_step, 0)
        last = (n_steps - 1) % 2
        c_row, inv = norm(last)
        wait_near(last)
        wait_far(last)
        keep(n_steps - 1, last, c_row, inv)
        wait_bytes(r_in.at[last, others], g_send)
        wait_bytes(c_in.at[last, others], c_send)
        result = [remote(alpha_acc.at[0], fin_alpha, f_send.at[0], f_recv.at[0], me, to=0),
                  remote(ll_acc, fin_ll, f_send.at[1], f_recv.at[1], me, to=0)]
        for copy in result:
            copy.start()
        alpha_ref[...] = alpha_acc[1]
        ll_ref[...] = ll_acc[:, :batch]
        for copy in result:
            copy.wait_send()


def solution(mesh):
    vec_axes = ('rows', 'states')
    nz, ny, nx = CHIPS
    n_sum, n_gather = 2 * nz, 2 * nx

    def local_forward(trans_blk, emit_blk, init_blk, tokens, lengths):
        batch, n_steps = tokens.shape
        cols = 2 * SB
        a_blk = trans_blk.reshape(trans_blk.shape[0], cols)
        vmem = pl.BlockSpec(memory_space=pltpu.VMEM)
        hbm = pl.BlockSpec(memory_space=pl.ANY)
        dma = pltpu.SemaphoreType.DMA
        k_rows = 2 * n_gather * SB
        block = min(BLOCK, n_sum)
        block_rows = block * batch
        n_blocks = n_steps // block
        alpha, ll = pl.pallas_call(
            functools.partial(forward_kernel, CHIPS, n_steps, block),
            out_shape=(jax.ShapeDtypeStruct((batch, SB), F32), jax.ShapeDtypeStruct((1, batch), F32)),
            in_specs=[hbm, vmem, vmem, pl.BlockSpec(memory_space=pltpu.SMEM), vmem],
            out_specs=(vmem, vmem),
            scratch_shapes=[
                pltpu.VMEM((n_sum, k_rows, cols), BF16),
                pltpu.VMEM(((n_steps + 1) * batch, cols), BF16),
                pltpu.VMEM((n_blocks, n_sum, block_rows, cols), BF16),
                pltpu.VMEM((2, block_rows, k_rows), F32),
                pltpu.VMEM((2, n_gather, 2, batch, SB), F32),
                pltpu.VMEM((2, n_gather, 1, SB), F32),
                pltpu.VMEM((2, n_sum, 1, SB), F32),
                pltpu.VMEM((2, n_sum - 1, 2, batch, SB), F32),
                pltpu.VMEM((n_sum - 1, 2, batch, SB), F32),
                pltpu.VMEM((batch, k_rows), BF16),
                pltpu.VMEM((1, SB), F32),
                pltpu.VMEM((batch, SB), F32),
                pltpu.VMEM((2, batch, SB), F32),
                pltpu.VMEM((1, SB), F32),
                pltpu.VMEM((batch, SB), F32),
                pltpu.VMEM((1, SB), F32),
                pltpu.VMEM((emit_blk.shape[1], SB), F32),
                pltpu.VMEM((n_steps, batch, SB), F32),
                pltpu.VMEM((n_steps * batch, SB), BF16),
                pltpu.VMEM((batch, SB), F32),
                pltpu.SemaphoreType.REGULAR,
                dma((n_sum, 2)), dma((n_sum,)), dma, dma, dma((2, n_sum)), dma, dma, dma((2,)),
                dma((2, 2)), dma, dma((2,)), dma, dma((2,)), dma, dma((2,)), dma, dma((2,)), dma((2,)),
            ],
            compiler_params=pltpu.CompilerParams(collective_id=0, has_side_effects=True,
                                                 vmem_limit_bytes=36 * 1024 * 1024),
            cost_estimate=pl.CostEstimate(flops=2 * batch * (n_steps - 1) * n_sum * k_rows * cols,
                                          bytes_accessed=n_sum * k_rows * cols * 2, transcendentals=0),
        )(a_blk, emit_blk.T, init_blk[None, :], tokens, lengths[None, :])
        return ll[0], alpha

    return jax.shard_map(local_forward, mesh=mesh, in_specs=(P('rows', None, 'states'), P(vec_axes, None), P(vec_axes), P('seqs', None), P('seqs')), out_specs=(P('seqs'), P('seqs', vec_axes)), check_vma=False)
```

```python
import functools

import jax
import jax.numpy as jnp
from jax import lax
from jax.experimental import pallas as pl
from jax.experimental.pallas import tpu as pltpu
from jax.sharding import PartitionSpec as P

CHIPS = (4, 4, 4)
SB = 128
LIFT = 2.0 ** 64
LAG = 1
P_AFTER = 1
NEAR = 0
BLOCK = 8
AHEAD = 6
F32 = jnp.float32
BF16 = jnp.bfloat16


def ring_distance(offset, n):
    return min(offset, n - offset)


def forward_kernel(dims, n_steps, block, a_ref, emit_ref, init_ref, tok_ref, len_ref, alpha_ref, ll_ref,
                   a_loc, e_both, e_loc, w_loc, r_in, c_in, p_in, u_in, u_out, a_bf, len_row, len_col, alpha_acc, ll_acc,
                   fin_alpha, fin_ll, by_word, picked, e_half, r0_own, tick, a_sem, a_send, e_pair, e_send, e_sem, r0_sem, r0_send, own_sem,
                   g_recv, g_send, c_recv, c_send, u_recv, u_send, p_recv, p_send, f_recv, f_send):
    nz, ny, nx = dims
    n_sum, n_gather = 2 * nz, 2 * nx
    batch = tok_ref.shape[0]
    half = n_gather * SB
    rows = block * batch
    n_blocks = n_steps // block
    per_step = n_sum // block
    core = lax.axis_index('rows')
    me = lax.axis_index('states')
    z = me // (ny * nx)
    y = (me // nx) % ny
    x = me % nx
    group = me // n_gather
    c_place = (((y + 1) // 2) % 2) * nx + x
    far = sorted(range(1, n_sum), key=lambda k: -(ring_distance(k // 2, nz) + k % 2))
    sources = sorted(((f, d) for f in range(2) for d in range(nx)), key=lambda o: o[0] + ring_distance(o[1], nx))
    slot_of = {o: i for i, o in enumerate(sources)}
    far_gather = sources[:0:-1]
    n_near = n_gather // 2
    n_far = n_gather - n_near

    def sum_peer(k, sign=1):
        flip = k % 2
        return ((z + sign * (k // 2) + nz) % nz) * ny * nx + (y + flip * (ny - 1 - 2 * y)) * nx + x

    def mirror(k):
        return ((nz - k // 2) % nz) * 2 + k % 2

    def gather_peer(flip, d):
        return (me // (ny * nx)) * ny * nx + (y + flip * (1 - 2 * (y % 2))) * nx + (x + d) % nx

    def remote(src, dst, send, recv, state, to=1):
        return pltpu.make_async_remote_copy(src_ref=src, dst_ref=dst, send_sem=send, recv_sem=recv,
                                            device_id={'rows': to, 'states': state},
                                            device_id_type=pl.DeviceIdType.MESH)

    def wait_bytes(ref, sem):
        pltpu.make_async_copy(ref, ref, sem).wait()

    def a_rows(state, h):
        for i, (f, d) in enumerate(sources):
            there = ((state // nx + f) % 2) * nx + (x + d) % nx
            yield (a_ref.at[pl.ds((state // n_gather) * half + there * SB, SB)], pl.ds((2 * i + h) * SB, SB))

    def start_a(h, k):
        peer = sum_peer(k, -1)
        for src, to in a_rows(peer, h):
            remote(src, a_loc.at[k, to], a_send.at[k], a_sem.at[k, h], peer).start()

    def e_copy(b, k):
        return remote(e_both.at[pl.ds(b * rows + batch, rows)], e_loc.at[b, k], e_send, e_sem.at[b % 2, k], sum_peer(k, -1))

    def pick_tokens():
        def widen(i, carry):
            some = pl.ds(pl.multiple_of(i * batch, batch), batch)
            by_word[some, :] = emit_ref[some, :].astype(F32) * LIFT
            return carry

        lax.fori_loop(0, emit_ref.shape[0] // batch, widen, 0, unroll=5)

        def pick(t, carry):
            for b in range(batch):
                picked[t, b:b + 1, :] = by_word[pl.ds(tok_ref[b, t], 1), :]
            e_half[pl.ds(pl.multiple_of(t * batch, batch), batch), :] = picked[t].astype(BF16)
            return carry

        lax.fori_loop(0, n_steps, pick, 0)
        r0_own[...] = picked[0] * init_ref[...]

    barrier = pltpu.get_barrier_semaphore()

    def announce(state, to):
        pl.semaphore_signal(barrier, inc=1, device_id={'rows': to, 'states': state}, device_id_type=pl.DeviceIdType.MESH)

    @pl.when(core == 0)
    def helper():
        announce(me, 1)
        pl.semaphore_wait(barrier, n_sum)
        for k in range(n_sum // 2):
            start_a(0, k)
        e_both[pl.ds(n_steps * batch, batch), :] = jnp.zeros((batch, 2 * SB), BF16)
        pick_tokens()
        first = remote(r0_own, r_in.at[0, 0, 0], r0_send, r0_sem, me)
        first.start()
        every = pl.ds(0, n_steps * batch)
        mine = pltpu.make_async_copy(e_half, e_both.at[every, pl.ds(0, SB)], own_sem.at[0])
        mine.start()
        mine.wait()
        wait_bytes(e_both.at[every, pl.ds(SB, SB)], e_pair)
        for k in range(n_sum):
            e_copy(0, k).start()
        for k in range(n_sum // 2, n_sum):
            start_a(0, k)
        wait_bytes(e_loc.at[0], e_send)

        def send_part(i, carry):
            @pl.when(i >= AHEAD)
            def paced():
                pl.semaphore_wait(tick, 1)

            for n in range(per_step):
                e_copy(1 + i // block, (i % block) * per_step + n).start()
            wait_bytes(e_loc.at[0, pl.ds(0, per_step)], e_send)
            return carry

        lax.fori_loop(0, n_steps - block, send_part, 0)
        first.wait_send()
        for k in range(n_sum):
            wait_bytes(a_loc.at[k, pl.ds(0, half)], a_send.at[k])
        wait_bytes(fin_alpha, f_recv.at[0])
        wait_bytes(fin_ll, f_recv.at[1])
        alpha_ref[...] = fin_alpha[...]
        ll_ref[...] = fin_ll[:, :batch]

    @pl.when(core == 1)
    def owner():
        eye = (lax.broadcasted_iota(jnp.int32, (batch, SB), 0)
               == lax.broadcasted_iota(jnp.int32, (batch, SB), 1))

        def as_row(tile):
            col = jnp.sum(tile, axis=1, keepdims=True)
            return jnp.sum(jnp.where(eye, col, 0.0), axis=0, keepdims=True)

        def as_col(row):
            return jnp.sum(jnp.where(eye, row, 0.0), axis=1, keepdims=True)

        def start_gather(slot):
            for f, d in far_gather:
                there = slot_of[f, (nx - d) % nx]
                remote(r_in.at[slot, 0], r_in.at[slot, there], g_send, g_recv.at[slot, there // n_near],
                       gather_peer(f, d)).start()

        def start_parts(slot):
            for k in far:
                remote(p_in.at[slot, group], p_in.at[slot, group], p_send, p_recv.at[slot], sum_peer(k)).start()

        others = pl.ds(0, n_gather - 1)
        peers = pl.ds(0, n_sum - 1)

        def finish_norm(slot):
            wait_bytes(p_in.at[slot, peers], p_recv.at[slot])
            c_in[slot, c_place] = jnp.sum(p_in[slot], axis=0)
            for o in far_gather:
                remote(c_in.at[slot, c_place], c_in.at[slot, c_place], c_send, c_recv.at[slot], gather_peer(*o)).start()

        def wait_near(slot):
            if n_near > 1:
                wait_bytes(r_in.at[slot, pl.ds(0, n_near - 1)], g_recv.at[slot, 0])

        def wait_far(slot):
            wait_bytes(r_in.at[slot, pl.ds(0, n_far)], g_recv.at[slot, 1])

        def norm(slot):
            wait_bytes(c_in.at[slot, others], c_recv.at[slot])
            c_row = jnp.sum(c_in[slot], axis=0)
            c_col = as_col(c_row)
            inv = 1.0 / c_col
            return c_row, inv * (2.0 - c_col * inv)

        def keep(t, slot, c_row, inv):
            now = lax.convert_element_type(t, F32)
            active = now < len_col[...]
            for h in range(2):
                alpha_acc[h] = jnp.where(active, r_in[slot, 0, h] * inv, alpha_acc[h])
            ll_acc[...] = ll_acc[...] + jnp.where(now < len_row[...], jnp.log(c_row * (1.0 / LIFT)), 0.0)

        def add_w(b, k, fresh):
            part = lax.dot_general(e_loc[b, k], a_loc[k], (((1,), (1,)), ((), ())), preferred_element_type=F32)
            slot = b % 2
            w_loc[slot] = jnp.where(fresh, 0.0, w_loc[slot]) + part

        for k in far:
            announce(sum_peer(k), 1)
        for o in far_gather:
            announce(gather_peer(*o), 1)
        for k in range(n_sum):
            announce(sum_peer(k), 0)
        pl.semaphore_wait(barrier, n_sum + n_gather - 1)
        for k in range(1, n_sum):
            start_a(1, k)
        for src, to in a_rows(me, 1):
            pltpu.make_async_copy(src, a_loc.at[0, to], own_sem.at[1]).start()
        pick_tokens()
        alpha_acc[...] = jnp.zeros_like(alpha_acc)
        ll_acc[...] = jnp.zeros_like(ll_acc)
        w_loc[...] = jnp.zeros_like(w_loc)
        len_row[...] = jnp.zeros_like(len_row)
        len_row[:, :batch] = len_ref[...].astype(F32)
        len_col[...] = jnp.broadcast_to(as_col(len_row[...]), (batch, SB))
        pair = remote(e_half, e_both.at[pl.ds(0, n_steps * batch), pl.ds(SB, SB)], own_sem.at[0], e_pair, me, to=0)
        pair.start()
        r_in[0, 0, 1] = r0_own[...]
        wait_bytes(r0_own, r0_sem)
        p_in[0, group] = as_row(r_in[0, 0, 0] + r_in[0, 0, 1])
        start_parts(0)
        start_gather(0)
        finish_norm(0)
        wait_bytes(p_in.at[0, peers], p_send)
        wait_bytes(a_loc.at[0, pl.ds(0, half)], own_sem.at[1])

        def first_w(k, carry):
            wait_bytes(a_loc.at[k, pl.ds(0, half)], a_sem.at[k, 0])

            @pl.when(k > 0)
            def from_owner():
                wait_bytes(a_loc.at[k, pl.ds(0, half)], a_sem.at[k, 1])

            wait_bytes(e_loc.at[0, k], e_sem.at[0, k])
            add_w(0, k, False)
            return carry

        lax.fori_loop(0, n_sum, first_w, 0)
        pair.wait_send()
        for k in range(1, n_sum):
            wait_bytes(a_loc.at[k, pl.ds(0, half)], a_send.at[k])

        def one_step(t, carry):
            cur = t % 2
            nxt = (t + 1) % 2
            b = t // block
            row = pl.ds((t % block) * batch, batch)
            c_row, inv = norm(cur)
            total = jnp.zeros((batch, SB), F32)

            def take(first, last, total):
                for i in range(first, last):
                    for h in range(2):
                        cols = pl.ds((2 * i + h) * SB, SB)
                        tile = (r_in[cur, i, h] * inv).astype(BF16)
                        a_bf[:, cols] = tile
                        total = total + tile.astype(F32) * w_loc[b % 2, row, cols]
                return total

            def times(k, first, last):
                return jnp.dot(a_bf[:, first:last], a_loc[k, first:last], preferred_element_type=F32)

            order = far + [0]
            near_rows, all_rows = 2 * n_near * SB, 2 * half
            wait_near(cur)
            total = take(0, n_near, total)
            near = [times(k, 0, near_rows) for k in order[:NEAR]]
            wait_far(cur)
            total = take(n_near, n_gather, total)
            unit = jnp.where(t >= 0, jnp.float32(1.0), jnp.float32(0.0))
            ready = []

            def send_sum():
                k, part = ready.pop(0)
                for h in range(2):
                    u_out[k - 1, h] = part[:, h * SB:(h + 1) * SB]
                remote(u_out.at[k - 1], u_in.at[nxt, mirror(k) - 1], u_send, u_recv.at[nxt], sum_peer(k)).start()

            for i, k in enumerate(order):
                begin = near_rows if i < NEAR else 0
                middle = (begin + all_rows) // 2
                part = times(k, begin, middle) * unit + times(k, middle, all_rows)
                ready.append((k, part + near[i] if i < NEAR else part))
                if i == P_AFTER:
                    p_in[nxt, group] = as_row(total)
                    start_parts(nxt)
                if len(ready) > LAG:
                    send_sum()
            while len(ready) > 1:
                send_sum()
            own_part = ready[0][1]
            wait_bytes(r_in.at[cur, others], g_send)
            wait_bytes(c_in.at[cur, others], c_send)
            keep(t, cur, c_row, inv)
            finish_norm(nxt)
            wait_bytes(u_in.at[nxt], u_recv.at[nxt])
            for h in range(2):
                parts = [own_part[:, h * SB:(h + 1) * SB]] + [u_in[nxt, k, h] for k in range(n_sum - 1)]
                while len(parts) > 1:
                    parts = [parts[i] + parts[i + 1] for i in range(0, len(parts), 2)]
                r_in[nxt, 0, h] = parts[0] * e_loc[b, 0, row, pl.ds(h * SB, SB)].astype(F32)
            start_gather(nxt)

            @pl.when(t < n_steps - block - AHEAD)
            def go_on():
                pl.semaphore_signal(tick, inc=1, device_id={'rows': 0, 'states': me},
                                    device_id_type=pl.DeviceIdType.MESH)

            @pl.when(b + 1 < n_blocks)
            def next_w():
                later = b + 1
                for n in range(per_step):
                    k = (t % block) * per_step + n
                    wait_bytes(e_loc.at[later, k], e_sem.at[later % 2, k])
                    add_w(later, k, k == 0)

            wait_bytes(u_out, u_send)
            wait_bytes(p_in.at[nxt, peers], p_send)
            return carry

        lax.fori_loop(0, n_steps - 1, one_step, 0)
        last = (n_steps - 1) % 2
        c_row, inv = norm(last)
        wait_near(last)
        wait_far(last)
        keep(n_steps - 1, last, c_row, inv)
        wait_bytes(r_in.at[last, others], g_send)
        wait_bytes(c_in.at[last, others], c_send)
        result = [remote(alpha_acc.at[0], fin_alpha, f_send.at[0], f_recv.at[0], me, to=0),
                  remote(ll_acc, fin_ll, f_send.at[1], f_recv.at[1], me, to=0)]
        for copy in result:
            copy.start()
        alpha_ref[...] = alpha_acc[1]
        ll_ref[...] = ll_acc[:, :batch]
        for copy in result:
            copy.wait_send()


def solution(mesh):
    vec_axes = ('rows', 'states')
    nz, ny, nx = CHIPS
    n_sum, n_gather = 2 * nz, 2 * nx

    def local_forward(trans_blk, emit_blk, init_blk, tokens, lengths):
        batch, n_steps = tokens.shape
        cols = 2 * SB
        a_blk = trans_blk.reshape(trans_blk.shape[0], cols)
        vmem = pl.BlockSpec(memory_space=pltpu.VMEM)
        hbm = pl.BlockSpec(memory_space=pl.ANY)
        dma = pltpu.SemaphoreType.DMA
        k_rows = 2 * n_gather * SB
        block = min(BLOCK, n_sum)
        block_rows = block * batch
        n_blocks = n_steps // block
        alpha, ll = pl.pallas_call(
            functools.partial(forward_kernel, CHIPS, n_steps, block),
            out_shape=(jax.ShapeDtypeStruct((batch, SB), F32), jax.ShapeDtypeStruct((1, batch), F32)),
            in_specs=[hbm, vmem, vmem, pl.BlockSpec(memory_space=pltpu.SMEM), vmem],
            out_specs=(vmem, vmem),
            scratch_shapes=[
                pltpu.VMEM((n_sum, k_rows, cols), BF16),
                pltpu.VMEM(((n_steps + 1) * batch, cols), BF16),
                pltpu.VMEM((n_blocks, n_sum, block_rows, cols), BF16),
                pltpu.VMEM((2, block_rows, k_rows), F32),
                pltpu.VMEM((2, n_gather, 2, batch, SB), F32),
                pltpu.VMEM((2, n_gather, 1, SB), F32),
                pltpu.VMEM((2, n_sum, 1, SB), F32),
                pltpu.VMEM((2, n_sum - 1, 2, batch, SB), F32),
                pltpu.VMEM((n_sum - 1, 2, batch, SB), F32),
                pltpu.VMEM((batch, k_rows), BF16),
                pltpu.VMEM((1, SB), F32),
                pltpu.VMEM((batch, SB), F32),
                pltpu.VMEM((2, batch, SB), F32),
                pltpu.VMEM((1, SB), F32),
                pltpu.VMEM((batch, SB), F32),
                pltpu.VMEM((1, SB), F32),
                pltpu.VMEM((emit_blk.shape[1], SB), F32),
                pltpu.VMEM((n_steps, batch, SB), F32),
                pltpu.VMEM((n_steps * batch, SB), BF16),
                pltpu.VMEM((batch, SB), F32),
                pltpu.SemaphoreType.REGULAR,
                dma((n_sum, 2)), dma((n_sum,)), dma, dma, dma((2, n_sum)), dma, dma, dma((2,)),
                dma((2, 2)), dma, dma((2,)), dma, dma((2,)), dma, dma((2,)), dma, dma((2,)), dma((2,)),
            ],
            compiler_params=pltpu.CompilerParams(collective_id=0, has_side_effects=True,
                                                 vmem_limit_bytes=36 * 1024 * 1024),
            cost_estimate=pl.CostEstimate(flops=2 * batch * (n_steps - 1) * n_sum * k_rows * cols,
                                          bytes_accessed=n_sum * k_rows * cols * 2, transcendentals=0),
        )(a_blk, emit_blk.T, init_blk[None, :], tokens, lengths[None, :])
        return ll[0], alpha

    return jax.shard_map(local_forward, mesh=mesh, in_specs=(P('rows', None, 'states'), P(vec_axes, None), P(vec_axes), P('seqs', None), P('seqs')), out_specs=(P('seqs'), P('seqs', vec_axes)), check_vma=False)
```

```python
import functools

import jax
import jax.numpy as jnp
from jax import lax
from jax.experimental import pallas as pl
from jax.experimental.pallas import tpu as pltpu
from jax.sharding import PartitionSpec as P

CHIPS = (4, 4, 4)
SB = 128
LIFT = 2.0 ** 64
LAG = 1
P_AFTER = 1
NEAR = 0
BLOCK = 8
AHEAD = 6
F32 = jnp.float32
BF16 = jnp.bfloat16


def ring_distance(offset, n):
    return min(offset, n - offset)


def forward_kernel(dims, n_steps, block, a_ref, emit_ref, init_ref, tok_ref, len_ref, alpha_ref, ll_ref,
                   a_loc, e_both, e_loc, w_loc, r_in, c_in, p_in, u_in, u_out, a_bf, len_row, len_col, alpha_acc, ll_acc,
                   fin_alpha, fin_ll, by_word, picked, e_half, r0_own, tick, a_sem, a_send, e_pair, e_send, e_sem, r0_sem, r0_send, own_sem,
                   g_recv, g_send, c_recv, c_send, u_recv, u_send, p_recv, p_send, f_recv, f_send):
    nz, ny, nx = dims
    n_sum, n_gather = 2 * nz, 2 * nx
    batch = tok_ref.shape[0]
    half = n_gather * SB
    rows = block * batch
    n_blocks = n_steps // block
    per_step = n_sum // block
    core = lax.axis_index('rows')
    me = lax.axis_index('states')
    z = me // (ny * nx)
    y = (me // nx) % ny
    x = me % nx
    group = me // n_gather
    c_place = (((y + 1) // 2) % 2) * nx + x
    far = sorted(range(1, n_sum), key=lambda k: -(ring_distance(k // 2, nz) + k % 2))
    sources = sorted(((f, d) for f in range(2) for d in range(nx)), key=lambda o: o[0] + ring_distance(o[1], nx))
    slot_of = {o: i for i, o in enumerate(sources)}
    far_gather = sources[:0:-1]
    n_near = n_gather // 2
    n_far = n_gather - n_near

    def sum_peer(k, sign=1):
        flip = k % 2
        return ((z + sign * (k // 2) + nz) % nz) * ny * nx + (y + flip * (ny - 1 - 2 * y)) * nx + x

    def mirror(k):
        return ((nz - k // 2) % nz) * 2 + k % 2

    def gather_peer(flip, d):
        return (me // (ny * nx)) * ny * nx + (y + flip * (1 - 2 * (y % 2))) * nx + (x + d) % nx

    def remote(src, dst, send, recv, state, to=1):
        return pltpu.make_async_remote_copy(src_ref=src, dst_ref=dst, send_sem=send, recv_sem=recv,
                                            device_id={'rows': to, 'states': state},
                                            device_id_type=pl.DeviceIdType.MESH)

    def wait_bytes(ref, sem):
        pltpu.make_async_copy(ref, ref, sem).wait()

    def a_rows(state, h):
        for i, (f, d) in enumerate(sources):
            there = ((state // nx + f) % 2) * nx + (x + d) % nx
            yield (a_ref.at[pl.ds((state // n_gather) * half + there * SB, SB)], pl.ds((2 * i + h) * SB, SB))

    def start_a(h, k):
        peer = sum_peer(k, -1)
        for src, to in a_rows(peer, h):
            remote(src, a_loc.at[k, to], a_send.at[k], a_sem.at[k, h], peer).start()

    def e_copy(b, k):
        return remote(e_both.at[pl.ds(b * rows + batch, rows)], e_loc.at[b, k], e_send, e_sem.at[b % 2, k], sum_peer(k, -1))

    def pick_tokens():
        def widen(i, carry):
            some = pl.ds(pl.multiple_of(i * batch, batch), batch)
            by_word[some, :] = emit_ref[some, :].astype(F32) * LIFT
            return carry

        lax.fori_loop(0, emit_ref.shape[0] // batch, widen, 0, unroll=5)

        def pick(t, carry):
            for b in range(batch):
                picked[t, b:b + 1, :] = by_word[pl.ds(tok_ref[b, t], 1), :]
            e_half[pl.ds(pl.multiple_of(t * batch, batch), batch), :] = picked[t].astype(BF16)
            return carry

        lax.fori_loop(0, n_steps, pick, 0)
        r0_own[...] = picked[0] * init_ref[...]

    barrier = pltpu.get_barrier_semaphore()

    def announce(state, to):
        pl.semaphore_signal(barrier, inc=1, device_id={'rows': to, 'states': state}, device_id_type=pl.DeviceIdType.MESH)

    @pl.when(core == 0)
    def helper():
        announce(me, 1)
        pl.semaphore_wait(barrier, n_sum)
        for k in range(1, n_sum, 2):
            start_a(0, k)
        e_both[pl.ds(n_steps * batch, batch), :] = jnp.zeros((batch, 2 * SB), BF16)
        pick_tokens()
        first = remote(r0_own, r_in.at[0, 0, 0], r0_send, r0_sem, me)
        first.start()
        every = pl.ds(0, n_steps * batch)
        mine = pltpu.make_async_copy(e_half, e_both.at[every, pl.ds(0, SB)], own_sem.at[0])
        mine.start()
        mine.wait()
        wait_bytes(e_both.at[every, pl.ds(SB, SB)], e_pair)
        for k in range(n_sum):
            e_copy(0, k).start()
        for k in range(0, n_sum, 2):
            start_a(0, k)
        wait_bytes(e_loc.at[0], e_send)

        def send_part(i, carry):
            @pl.when(i >= AHEAD)
            def paced():
                pl.semaphore_wait(tick, 1)

            for n in range(per_step):
                e_copy(1 + i // block, (i % block) * per_step + n).start()
            wait_bytes(e_loc.at[0, pl.ds(0, per_step)], e_send)
            return carry

        lax.fori_loop(0, n_steps - block, send_part, 0)
        first.wait_send()
        for k in range(n_sum):
            wait_bytes(a_loc.at[k, pl.ds(0, half)], a_send.at[k])
        wait_bytes(fin_alpha, f_recv.at[0])
        wait_bytes(fin_ll, f_recv.at[1])
        alpha_ref[...] = fin_alpha[...]
        ll_ref[...] = fin_ll[:, :batch]

    @pl.when(core == 1)
    def owner():
        eye = (lax.broadcasted_iota(jnp.int32, (batch, SB), 0)
               == lax.broadcasted_iota(jnp.int32, (batch, SB), 1))

        def as_row(tile):
            col = jnp.sum(tile, axis=1, keepdims=True)
            return jnp.sum(jnp.where(eye, col, 0.0), axis=0, keepdims=True)

        def as_col(row):
            return jnp.sum(jnp.where(eye, row, 0.0), axis=1, keepdims=True)

        def start_gather(slot):
            for f, d in far_gather:
                there = slot_of[f, (nx - d) % nx]
                remote(r_in.at[slot, 0], r_in.at[slot, there], g_send, g_recv.at[slot, there // n_near],
                       gather_peer(f, d)).start()

        def start_parts(slot):
            for k in far:
                remote(p_in.at[slot, group], p_in.at[slot, group], p_send, p_recv.at[slot], sum_peer(k)).start()

        others = pl.ds(0, n_gather - 1)
        peers = pl.ds(0, n_sum - 1)

        def finish_norm(slot):
            wait_bytes(p_in.at[slot, peers], p_recv.at[slot])
            c_in[slot, c_place] = jnp.sum(p_in[slot], axis=0)
            for o in far_gather:
                remote(c_in.at[slot, c_place], c_in.at[slot, c_place], c_send, c_recv.at[slot], gather_peer(*o)).start()

        def wait_near(slot):
            if n_near > 1:
                wait_bytes(r_in.at[slot, pl.ds(0, n_near - 1)], g_recv.at[slot, 0])

        def wait_far(slot):
            wait_bytes(r_in.at[slot, pl.ds(0, n_far)], g_recv.at[slot, 1])

        def norm(slot):
            wait_bytes(c_in.at[slot, others], c_recv.at[slot])
            c_row = jnp.sum(c_in[slot], axis=0)
            c_col = as_col(c_row)
            inv = 1.0 / c_col
            return c_row, inv * (2.0 - c_col * inv)

        def keep(t, slot, c_row, inv):
            now = lax.convert_element_type(t, F32)
            active = now < len_col[...]
            for h in range(2):
                alpha_acc[h] = jnp.where(active, r_in[slot, 0, h] * inv, alpha_acc[h])
            ll_acc[...] = ll_acc[...] + jnp.where(now < len_row[...], jnp.log(c_row * (1.0 / LIFT)), 0.0)

        def add_w(b, k, fresh):
            part = lax.dot_general(e_loc[b, k], a_loc[k], (((1,), (1,)), ((), ())), preferred_element_type=F32)
            slot = b % 2
            w_loc[slot] = jnp.where(fresh, 0.0, w_loc[slot]) + part

        for k in far:
            announce(sum_peer(k), 1)
        for o in far_gather:
            announce(gather_peer(*o), 1)
        for k in range(n_sum):
            announce(sum_peer(k), 0)
        pl.semaphore_wait(barrier, n_sum + n_gather - 1)
        for k in [*range(1, n_sum, 2), *range(2, n_sum, 2)]:
            start_a(1, k)
        for src, to in a_rows(me, 1):
            pltpu.make_async_copy(src, a_loc.at[0, to], own_sem.at[1]).start()
        pick_tokens()
        alpha_acc[...] = jnp.zeros_like(alpha_acc)
        ll_acc[...] = jnp.zeros_like(ll_acc)
        w_loc[...] = jnp.zeros_like(w_loc)
        len_row[...] = jnp.zeros_like(len_row)
        len_row[:, :batch] = len_ref[...].astype(F32)
        len_col[...] = jnp.broadcast_to(as_col(len_row[...]), (batch, SB))
        pair = remote(e_half, e_both.at[pl.ds(0, n_steps * batch), pl.ds(SB, SB)], own_sem.at[0], e_pair, me, to=0)
        pair.start()
        r_in[0, 0, 1] = r0_own[...]
        wait_bytes(r0_own, r0_sem)
        p_in[0, group] = as_row(r_in[0, 0, 0] + r_in[0, 0, 1])
        start_parts(0)
        start_gather(0)
        finish_norm(0)
        wait_bytes(p_in.at[0, peers], p_send)
        wait_bytes(a_loc.at[0, pl.ds(0, half)], own_sem.at[1])

        def first_w(i, carry):
            k = 2 * i + 1 - (n_sum + 1) * (i // (n_sum // 2))
            wait_bytes(a_loc.at[k, pl.ds(0, half)], a_sem.at[k, 0])

            @pl.when(k > 0)
            def from_owner():
                wait_bytes(a_loc.at[k, pl.ds(0, half)], a_sem.at[k, 1])

            wait_bytes(e_loc.at[0, k], e_sem.at[0, k])
            add_w(0, k, False)
            return carry

        lax.fori_loop(0, n_sum, first_w, 0)
        pair.wait_send()
        for k in range(1, n_sum):
            wait_bytes(a_loc.at[k, pl.ds(0, half)], a_send.at[k])

        def one_step(t, carry):
            cur = t % 2
            nxt = (t + 1) % 2
            b = t // block
            row = pl.ds((t % block) * batch, batch)
            c_row, inv = norm(cur)
            total = jnp.zeros((batch, SB), F32)

            def take(first, last, total):
                for i in range(first, last):
                    for h in range(2):
                        cols = pl.ds((2 * i + h) * SB, SB)
                        tile = (r_in[cur, i, h] * inv).astype(BF16)
                        a_bf[:, cols] = tile
                        total = total + tile.astype(F32) * w_loc[b % 2, row, cols]
                return total

            def times(k, first, last):
                return jnp.dot(a_bf[:, first:last], a_loc[k, first:last], preferred_element_type=F32)

            order = far + [0]
            near_rows, all_rows = 2 * n_near * SB, 2 * half
            wait_near(cur)
            total = take(0, n_near, total)
            near = [times(k, 0, near_rows) for k in order[:NEAR]]
            wait_far(cur)
            total = take(n_near, n_gather, total)
            unit = jnp.where(t >= 0, jnp.float32(1.0), jnp.float32(0.0))
            ready = []

            def send_sum():
                k, part = ready.pop(0)
                for h in range(2):
                    u_out[k - 1, h] = part[:, h * SB:(h + 1) * SB]
                remote(u_out.at[k - 1], u_in.at[nxt, mirror(k) - 1], u_send, u_recv.at[nxt], sum_peer(k)).start()

            for i, k in enumerate(order):
                begin = near_rows if i < NEAR else 0
                middle = (begin + all_rows) // 2
                part = times(k, begin, middle) * unit + times(k, middle, all_rows)
                ready.append((k, part + near[i] if i < NEAR else part))
                if i == P_AFTER:
                    p_in[nxt, group] = as_row(total)
                    start_parts(nxt)
                if len(ready) > LAG:
                    send_sum()
            while len(ready) > 1:
                send_sum()
            own_part = ready[0][1]
            wait_bytes(r_in.at[cur, others], g_send)
            wait_bytes(c_in.at[cur, others], c_send)
            keep(t, cur, c_row, inv)
            finish_norm(nxt)
            wait_bytes(u_in.at[nxt], u_recv.at[nxt])
            for h in range(2):
                parts = [own_part[:, h * SB:(h + 1) * SB]] + [u_in[nxt, k, h] for k in range(n_sum - 1)]
                while len(parts) > 1:
                    parts = [parts[i] + parts[i + 1] for i in range(0, len(parts), 2)]
                r_in[nxt, 0, h] = parts[0] * e_loc[b, 0, row, pl.ds(h * SB, SB)].astype(F32)
            start_gather(nxt)

            @pl.when(t < n_steps - block - AHEAD)
            def go_on():
                pl.semaphore_signal(tick, inc=1, device_id={'rows': 0, 'states': me},
                                    device_id_type=pl.DeviceIdType.MESH)

            @pl.when(b + 1 < n_blocks)
            def next_w():
                later = b + 1
                for n in range(per_step):
                    k = (t % block) * per_step + n
                    wait_bytes(e_loc.at[later, k], e_sem.at[later % 2, k])
                    add_w(later, k, k == 0)

            wait_bytes(u_out, u_send)
            wait_bytes(p_in.at[nxt, peers], p_send)
            return carry

        lax.fori_loop(0, n_steps - 1, one_step, 0)
        last = (n_steps - 1) % 2
        c_row, inv = norm(last)
        keep(n_steps - 1, last, c_row, inv)
        result = [remote(alpha_acc.at[0], fin_alpha, f_send.at[0], f_recv.at[0], me, to=0),
                  remote(ll_acc, fin_ll, f_send.at[1], f_recv.at[1], me, to=0)]
        for copy in result:
            copy.start()
        wait_near(last)
        wait_far(last)
        wait_bytes(r_in.at[last, others], g_send)
        wait_bytes(c_in.at[last, others], c_send)
        alpha_ref[...] = alpha_acc[1]
        ll_ref[...] = ll_acc[:, :batch]
        for copy in result:
            copy.wait_send()


def solution(mesh):
    vec_axes = ('rows', 'states')
    nz, ny, nx = CHIPS
    n_sum, n_gather = 2 * nz, 2 * nx

    def local_forward(trans_blk, emit_blk, init_blk, tokens, lengths):
        batch, n_steps = tokens.shape
        cols = 2 * SB
        a_blk = trans_blk.reshape(trans_blk.shape[0], cols)
        vmem = pl.BlockSpec(memory_space=pltpu.VMEM)
        hbm = pl.BlockSpec(memory_space=pl.ANY)
        dma = pltpu.SemaphoreType.DMA
        k_rows = 2 * n_gather * SB
        block = min(BLOCK, n_sum)
        block_rows = block * batch
        n_blocks = n_steps // block
        alpha, ll = pl.pallas_call(
            functools.partial(forward_kernel, CHIPS, n_steps, block),
            out_shape=(jax.ShapeDtypeStruct((batch, SB), F32), jax.ShapeDtypeStruct((1, batch), F32)),
            in_specs=[hbm, vmem, vmem, pl.BlockSpec(memory_space=pltpu.SMEM), vmem],
            out_specs=(vmem, vmem),
            scratch_shapes=[
                pltpu.VMEM((n_sum, k_rows, cols), BF16),
                pltpu.VMEM(((n_steps + 1) * batch, cols), BF16),
                pltpu.VMEM((n_blocks, n_sum, block_rows, cols), BF16),
                pltpu.VMEM((2, block_rows, k_rows), F32),
                pltpu.VMEM((2, n_gather, 2, batch, SB), F32),
                pltpu.VMEM((2, n_gather, 1, SB), F32),
                pltpu.VMEM((2, n_sum, 1, SB), F32),
                pltpu.VMEM((2, n_sum - 1, 2, batch, SB), F32),
                pltpu.VMEM((n_sum - 1, 2, batch, SB), F32),
                pltpu.VMEM((batch, k_rows), BF16),
                pltpu.VMEM((1, SB), F32),
                pltpu.VMEM((batch, SB), F32),
                pltpu.VMEM((2, batch, SB), F32),
                pltpu.VMEM((1, SB), F32),
                pltpu.VMEM((batch, SB), F32),
                pltpu.VMEM((1, SB), F32),
                pltpu.VMEM((emit_blk.shape[1], SB), F32),
                pltpu.VMEM((n_steps, batch, SB), F32),
                pltpu.VMEM((n_steps * batch, SB), BF16),
                pltpu.VMEM((batch, SB), F32),
                pltpu.SemaphoreType.REGULAR,
                dma((n_sum, 2)), dma((n_sum,)), dma, dma, dma((2, n_sum)), dma, dma, dma((2,)),
                dma((2, 2)), dma, dma((2,)), dma, dma((2,)), dma, dma((2,)), dma, dma((2,)), dma((2,)),
            ],
            compiler_params=pltpu.CompilerParams(collective_id=0, has_side_effects=True,
                                                 vmem_limit_bytes=36 * 1024 * 1024),
            cost_estimate=pl.CostEstimate(flops=2 * batch * (n_steps - 1) * n_sum * k_rows * cols,
                                          bytes_accessed=n_sum * k_rows * cols * 2, transcendentals=0),
        )(a_blk, emit_blk.T, init_blk[None, :], tokens, lengths[None, :])
        return ll[0], alpha

    return jax.shard_map(local_forward, mesh=mesh, in_specs=(P('rows', None, 'states'), P(vec_axes, None), P(vec_axes), P('seqs', None), P('seqs')), out_specs=(P('seqs'), P('seqs', vec_axes)), check_vma=False)
```

```python
import functools

import jax
import jax.numpy as jnp
from jax import lax
from jax.experimental import pallas as pl
from jax.experimental.pallas import tpu as pltpu
from jax.sharding import PartitionSpec as P

CHIPS = (4, 4, 4)
SB = 128
LIFT = 2.0 ** 64
LAG = 1
P_AFTER = 1
NEAR = 0
BLOCK = 8
AHEAD = 6
F32 = jnp.float32
BF16 = jnp.bfloat16


def ring_distance(offset, n):
    return min(offset, n - offset)


def forward_kernel(dims, n_steps, block, a_ref, emit_ref, init_ref, tok_ref, len_ref, alpha_ref, ll_ref,
                   a_loc, e_both, e_loc, w_loc, r_in, c_in, p_in, u_in, u_out, a_bf, len_row, len_col, alpha_acc, ll_acc,
                   fin_alpha, fin_ll, by_word, picked, e_half, r0_own, tick, a_sem, a_send, e_pair, e_send, e_sem, r0_sem, r0_send, own_sem,
                   g_recv, g_send, c_recv, c_send, u_recv, u_send, p_recv, p_send, f_recv, f_send):
    nz, ny, nx = dims
    n_sum, n_gather = 2 * nz, 2 * nx
    batch = tok_ref.shape[0]
    half = n_gather * SB
    rows = block * batch
    n_blocks = n_steps // block
    per_step = n_sum // block
    core = lax.axis_index('rows')
    me = lax.axis_index('states')
    z = me // (ny * nx)
    y = (me // nx) % ny
    x = me % nx
    group = me // n_gather
    c_place = (((y + 1) // 2) % 2) * nx + x
    far = sorted(range(1, n_sum), key=lambda k: -(ring_distance(k // 2, nz) + k % 2))
    sources = sorted(((f, d) for f in range(2) for d in range(nx)), key=lambda o: o[0] + ring_distance(o[1], nx))
    slot_of = {o: i for i, o in enumerate(sources)}
    far_gather = sources[:0:-1]
    n_near = n_gather // 2
    n_far = n_gather - n_near

    def sum_peer(k, sign=1):
        flip = k % 2
        return ((z + sign * (k // 2) + nz) % nz) * ny * nx + (y + flip * (ny - 1 - 2 * y)) * nx + x

    def mirror(k):
        return ((nz - k // 2) % nz) * 2 + k % 2

    def gather_peer(flip, d):
        return (me // (ny * nx)) * ny * nx + (y + flip * (1 - 2 * (y % 2))) * nx + (x + d) % nx

    def remote(src, dst, send, recv, state, to=1):
        return pltpu.make_async_remote_copy(src_ref=src, dst_ref=dst, send_sem=send, recv_sem=recv,
                                            device_id={'rows': to, 'states': state},
                                            device_id_type=pl.DeviceIdType.MESH)

    def wait_bytes(ref, sem):
        pltpu.make_async_copy(ref, ref, sem).wait()

    def a_rows(state, h):
        for i, (f, d) in enumerate(sources):
            there = ((state // nx + f) % 2) * nx + (x + d) % nx
            yield (a_ref.at[pl.ds((state // n_gather) * half + there * SB, SB)], pl.ds((2 * i + h) * SB, SB))

    def start_a(h, k):
        peer = sum_peer(k, -1)
        for src, to in a_rows(peer, h):
            remote(src, a_loc.at[k, to], a_send.at[k], a_sem.at[k, h], peer).start()

    def e_copy(b, k):
        return remote(e_both.at[pl.ds(b * rows + batch, rows)], e_loc.at[b, k], e_send, e_sem.at[b % 2, k], sum_peer(k, -1))

    def pick_tokens():
        def widen(i, carry):
            some = pl.ds(pl.multiple_of(i * batch, batch), batch)
            by_word[some, :] = emit_ref[some, :].astype(F32) * LIFT
            return carry

        lax.fori_loop(0, emit_ref.shape[0] // batch, widen, 0, unroll=5)

        def pick(t, carry):
            for b in range(batch):
                picked[t, b:b + 1, :] = by_word[pl.ds(tok_ref[b, t], 1), :]
            e_half[pl.ds(pl.multiple_of(t * batch, batch), batch), :] = picked[t].astype(BF16)
            return carry

        lax.fori_loop(0, n_steps, pick, 0)
        r0_own[...] = picked[0] * init_ref[...]

    barrier = pltpu.get_barrier_semaphore()

    def announce(state, to):
        pl.semaphore_signal(barrier, inc=1, device_id={'rows': to, 'states': state}, device_id_type=pl.DeviceIdType.MESH)

    @pl.when(core == 0)
    def helper():
        announce(me, 1)
        pl.semaphore_wait(barrier, n_sum)
        for k in range(1, n_sum, 2):
            start_a(0, k)
        e_both[pl.ds(n_steps * batch, batch), :] = jnp.zeros((batch, 2 * SB), BF16)
        pick_tokens()
        first = remote(r0_own, r_in.at[0, 0, 0], r0_send, r0_sem, me)
        first.start()
        every = pl.ds(0, n_steps * batch)
        mine = pltpu.make_async_copy(e_half, e_both.at[every, pl.ds(0, SB)], own_sem.at[0])
        mine.start()
        mine.wait()
        wait_bytes(e_both.at[every, pl.ds(SB, SB)], e_pair)
        for k in range(n_sum):
            e_copy(0, k).start()
        for k in range(0, n_sum, 2):
            start_a(0, k)
        wait_bytes(e_loc.at[0], e_send)

        def send_part(i, carry):
            @pl.when(i >= AHEAD)
            def paced():
                pl.semaphore_wait(tick, 1)

            for n in range(per_step):
                e_copy(1 + i // block, (i % block) * per_step + n).start()
            wait_bytes(e_loc.at[0, pl.ds(0, per_step)], e_send)
            return carry

        lax.fori_loop(0, n_steps - block, send_part, 0)
        first.wait_send()
        for k in range(n_sum):
            wait_bytes(a_loc.at[k, pl.ds(0, half)], a_send.at[k])
        wait_bytes(fin_alpha, f_recv.at[0])
        wait_bytes(fin_ll, f_recv.at[1])
        alpha_ref[...] = fin_alpha[...]
        ll_ref[...] = fin_ll[:, :batch]

    @pl.when(core == 1)
    def owner():
        eye = (lax.broadcasted_iota(jnp.int32, (batch, SB), 0)
               == lax.broadcasted_iota(jnp.int32, (batch, SB), 1))

        def as_row(tile):
            col = jnp.sum(tile, axis=1, keepdims=True)
            return jnp.sum(jnp.where(eye, col, 0.0), axis=0, keepdims=True)

        def as_col(row):
            return jnp.sum(jnp.where(eye, row, 0.0), axis=1, keepdims=True)

        def start_gather(slot):
            for f, d in far_gather:
                there = slot_of[f, (nx - d) % nx]
                remote(r_in.at[slot, 0], r_in.at[slot, there], g_send, g_recv.at[slot, there // n_near],
                       gather_peer(f, d)).start()

        def start_parts(slot):
            for k in far:
                remote(p_in.at[slot, group], p_in.at[slot, group], p_send, p_recv.at[slot], sum_peer(k)).start()

        others = pl.ds(0, n_gather - 1)
        peers = pl.ds(0, n_sum - 1)

        def finish_norm(slot):
            wait_bytes(p_in.at[slot, peers], p_recv.at[slot])
            c_in[slot, c_place] = jnp.sum(p_in[slot], axis=0)
            for o in far_gather:
                remote(c_in.at[slot, c_place], c_in.at[slot, c_place], c_send, c_recv.at[slot], gather_peer(*o)).start()

        def wait_near(slot):
            if n_near > 1:
                wait_bytes(r_in.at[slot, pl.ds(0, n_near - 1)], g_recv.at[slot, 0])

        def wait_far(slot):
            wait_bytes(r_in.at[slot, pl.ds(0, n_far)], g_recv.at[slot, 1])

        def norm(slot):
            wait_bytes(c_in.at[slot, others], c_recv.at[slot])
            c_row = jnp.sum(c_in[slot], axis=0)
            c_col = as_col(c_row)
            inv = 1.0 / c_col
            return c_row, inv * (2.0 - c_col * inv)

        def keep(t, slot, c_row, inv):
            now = lax.convert_element_type(t, F32)
            active = now < len_col[...]
            for h in range(2):
                alpha_acc[h] = jnp.where(active, r_in[slot, 0, h] * inv, alpha_acc[h])
            ll_acc[...] = ll_acc[...] + jnp.where(now < len_row[...], jnp.log(c_row * (1.0 / LIFT)), 0.0)

        def add_w(b, k, fresh):
            part = lax.dot_general(e_loc[b, k], a_loc[k], (((1,), (1,)), ((), ())), preferred_element_type=F32)
            slot = b % 2
            w_loc[slot] = jnp.where(fresh, 0.0, w_loc[slot]) + part

        for k in far:
            announce(sum_peer(k), 1)
        for o in far_gather:
            announce(gather_peer(*o), 1)
        for k in range(n_sum):
            announce(sum_peer(k), 0)
        pl.semaphore_wait(barrier, n_sum + n_gather - 1)
        for k in range(1, n_sum, 2):
            start_a(1, k)
        for src, to in a_rows(me, 1):
            pltpu.make_async_copy(src, a_loc.at[0, to], own_sem.at[1]).start()
        pick_tokens()
        alpha_acc[...] = jnp.zeros_like(alpha_acc)
        ll_acc[...] = jnp.zeros_like(ll_acc)
        w_loc[...] = jnp.zeros_like(w_loc)
        len_row[...] = jnp.zeros_like(len_row)
        len_row[:, :batch] = len_ref[...].astype(F32)
        len_col[...] = jnp.broadcast_to(as_col(len_row[...]), (batch, SB))
        pair = remote(e_half, e_both.at[pl.ds(0, n_steps * batch), pl.ds(SB, SB)], own_sem.at[0], e_pair, me, to=0)
        pair.start()
        r_in[0, 0, 1] = r0_own[...]
        wait_bytes(r0_own, r0_sem)
        p_in[0, group] = as_row(r_in[0, 0, 0] + r_in[0, 0, 1])
        start_parts(0)
        start_gather(0)
        for k in range(2, n_sum, 2):
            start_a(1, k)
        finish_norm(0)
        wait_bytes(p_in.at[0, peers], p_send)
        wait_bytes(a_loc.at[0, pl.ds(0, half)], own_sem.at[1])

        def first_w(i, carry):
            k = 2 * i + 1 - (n_sum + 1) * (i // (n_sum // 2))
            wait_bytes(a_loc.at[k, pl.ds(0, half)], a_sem.at[k, 0])

            @pl.when(k > 0)
            def from_owner():
                wait_bytes(a_loc.at[k, pl.ds(0, half)], a_sem.at[k, 1])

            wait_bytes(e_loc.at[0, k], e_sem.at[0, k])
            add_w(0, k, False)
            return carry

        lax.fori_loop(0, n_sum, first_w, 0)
        pair.wait_send()
        for k in range(1, n_sum):
            wait_bytes(a_loc.at[k, pl.ds(0, half)], a_send.at[k])

        def one_step(t, carry):
            cur = t % 2
            nxt = (t + 1) % 2
            b = t // block
            row = pl.ds((t % block) * batch, batch)
            c_row, inv = norm(cur)
            total = jnp.zeros((batch, SB), F32)

            def take(first, last, total):
                for i in range(first, last):
                    for h in range(2):
                        cols = pl.ds((2 * i + h) * SB, SB)
                        tile = (r_in[cur, i, h] * inv).astype(BF16)
                        a_bf[:, cols] = tile
                        total = total + tile.astype(F32) * w_loc[b % 2, row, cols]
                return total

            def times(k, first, last):
                return jnp.dot(a_bf[:, first:last], a_loc[k, first:last], preferred_element_type=F32)

            order = far + [0]
            near_rows, all_rows = 2 * n_near * SB, 2 * half
            wait_near(cur)
            total = take(0, n_near, total)
            near = [times(k, 0, near_rows) for k in order[:NEAR]]
            wait_far(cur)
            total = take(n_near, n_gather, total)
            unit = jnp.where(t >= 0, jnp.float32(1.0), jnp.float32(0.0))
            ready = []

            def send_sum():
                k, part = ready.pop(0)
                for h in range(2):
                    u_out[k - 1, h] = part[:, h * SB:(h + 1) * SB]
                remote(u_out.at[k - 1], u_in.at[nxt, mirror(k) - 1], u_send, u_recv.at[nxt], sum_peer(k)).start()

            for i, k in enumerate(order):
                begin = near_rows if i < NEAR else 0
                middle = (begin + all_rows) // 2
                part = times(k, begin, middle) * unit + times(k, middle, all_rows)
                ready.append((k, part + near[i] if i < NEAR else part))
                if i == P_AFTER:
                    p_in[nxt, group] = as_row(total)
                    start_parts(nxt)
                if len(ready) > LAG:
                    send_sum()
            while len(ready) > 1:
                send_sum()
            own_part = ready[0][1]
            wait_bytes(r_in.at[cur, others], g_send)
            wait_bytes(c_in.at[cur, others], c_send)
            keep(t, cur, c_row, inv)
            finish_norm(nxt)
            wait_bytes(u_in.at[nxt], u_recv.at[nxt])
            for h in range(2):
                parts = [own_part[:, h * SB:(h + 1) * SB]] + [u_in[nxt, k, h] for k in range(n_sum - 1)]
                while len(parts) > 1:
                    parts = [parts[i] + parts[i + 1] for i in range(0, len(parts), 2)]
                r_in[nxt, 0, h] = parts[0] * e_loc[b, 0, row, pl.ds(h * SB, SB)].astype(F32)
            start_gather(nxt)

            @pl.when(t < n_steps - block - AHEAD)
            def go_on():
                pl.semaphore_signal(tick, inc=1, device_id={'rows': 0, 'states': me},
                                    device_id_type=pl.DeviceIdType.MESH)

            @pl.when(b + 1 < n_blocks)
            def next_w():
                later = b + 1
                for n in range(per_step):
                    k = (t % block) * per_step + n
                    wait_bytes(e_loc.at[later, k], e_sem.at[later % 2, k])
                    add_w(later, k, k == 0)

            wait_bytes(u_out, u_send)
            wait_bytes(p_in.at[nxt, peers], p_send)
            return carry

        lax.fori_loop(0, n_steps - 1, one_step, 0)
        last = (n_steps - 1) % 2
        c_row, inv = norm(last)
        keep(n_steps - 1, last, c_row, inv)
        result = [remote(alpha_acc.at[0], fin_alpha, f_send.at[0], f_recv.at[0], me, to=0),
                  remote(ll_acc, fin_ll, f_send.at[1], f_recv.at[1], me, to=0)]
        for copy in result:
            copy.start()
        wait_near(last)
        wait_far(last)
        wait_bytes(r_in.at[last, others], g_send)
        wait_bytes(c_in.at[last, others], c_send)
        alpha_ref[...] = alpha_acc[1]
        ll_ref[...] = ll_acc[:, :batch]
        for copy in result:
            copy.wait_send()


def solution(mesh):
    vec_axes = ('rows', 'states')
    nz, ny, nx = CHIPS
    n_sum, n_gather = 2 * nz, 2 * nx

    def local_forward(trans_blk, emit_blk, init_blk, tokens, lengths):
        batch, n_steps = tokens.shape
        cols = 2 * SB
        a_blk = trans_blk.reshape(trans_blk.shape[0], cols)
        vmem = pl.BlockSpec(memory_space=pltpu.VMEM)
        hbm = pl.BlockSpec(memory_space=pl.ANY)
        dma = pltpu.SemaphoreType.DMA
        k_rows = 2 * n_gather * SB
        block = min(BLOCK, n_sum)
        block_rows = block * batch
        n_blocks = n_steps // block
        alpha, ll = pl.pallas_call(
            functools.partial(forward_kernel, CHIPS, n_steps, block),
            out_shape=(jax.ShapeDtypeStruct((batch, SB), F32), jax.ShapeDtypeStruct((1, batch), F32)),
            in_specs=[hbm, vmem, vmem, pl.BlockSpec(memory_space=pltpu.SMEM), vmem],
            out_specs=(vmem, vmem),
            scratch_shapes=[
                pltpu.VMEM((n_sum, k_rows, cols), BF16),
                pltpu.VMEM(((n_steps + 1) * batch, cols), BF16),
                pltpu.VMEM((n_blocks, n_sum, block_rows, cols), BF16),
                pltpu.VMEM((2, block_rows, k_rows), F32),
                pltpu.VMEM((2, n_gather, 2, batch, SB), F32),
                pltpu.VMEM((2, n_gather, 1, SB), F32),
                pltpu.VMEM((2, n_sum, 1, SB), F32),
                pltpu.VMEM((2, n_sum - 1, 2, batch, SB), F32),
                pltpu.VMEM((n_sum - 1, 2, batch, SB), F32),
                pltpu.VMEM((batch, k_rows), BF16),
                pltpu.VMEM((1, SB), F32),
                pltpu.VMEM((batch, SB), F32),
                pltpu.VMEM((2, batch, SB), F32),
                pltpu.VMEM((1, SB), F32),
                pltpu.VMEM((batch, SB), F32),
                pltpu.VMEM((1, SB), F32),
                pltpu.VMEM((emit_blk.shape[1], SB), F32),
                pltpu.VMEM((n_steps, batch, SB), F32),
                pltpu.VMEM((n_steps * batch, SB), BF16),
                pltpu.VMEM((batch, SB), F32),
                pltpu.SemaphoreType.REGULAR,
                dma((n_sum, 2)), dma((n_sum,)), dma, dma, dma((2, n_sum)), dma, dma, dma((2,)),
                dma((2, 2)), dma, dma((2,)), dma, dma((2,)), dma, dma((2,)), dma, dma((2,)), dma((2,)),
            ],
            compiler_params=pltpu.CompilerParams(collective_id=0, has_side_effects=True,
                                                 vmem_limit_bytes=36 * 1024 * 1024),
            cost_estimate=pl.CostEstimate(flops=2 * batch * (n_steps - 1) * n_sum * k_rows * cols,
                                          bytes_accessed=n_sum * k_rows * cols * 2, transcendentals=0),
        )(a_blk, emit_blk.T, init_blk[None, :], tokens, lengths[None, :])
        return ll[0], alpha

    return jax.shard_map(local_forward, mesh=mesh, in_specs=(P('rows', None, 'states'), P(vec_axes, None), P(vec_axes), P('seqs', None), P('seqs')), out_specs=(P('seqs'), P('seqs', vec_axes)), check_vma=False)
```

```python
import functools

import jax
import jax.numpy as jnp
from jax import lax
from jax.experimental import pallas as pl
from jax.experimental.pallas import tpu as pltpu
from jax.sharding import PartitionSpec as P

CHIPS = (4, 4, 4)
SB = 128
LIFT = 2.0 ** 64
LAG = 1
P_AFTER = 1
NEAR = 0
BLOCK = 8
AHEAD = 6
F32 = jnp.float32
BF16 = jnp.bfloat16


def ring_distance(offset, n):
    return min(offset, n - offset)


def forward_kernel(dims, n_steps, block, a_ref, emit_ref, init_ref, tok_ref, len_ref, alpha_ref, ll_ref,
                   a_loc, e_both, e_loc, w_loc, r_in, c_in, p_in, u_in, u_out, a_bf, len_row, len_col, alpha_acc, ll_acc,
                   fin_alpha, fin_ll, by_word, picked, e_half, r0_own, tick, a_sem, a_send, e_pair, e_send, e_sem, r0_sem, r0_send, own_sem,
                   g_recv, g_send, c_recv, c_send, u_recv, u_send, p_recv, p_send, f_recv, f_send):
    nz, ny, nx = dims
    n_sum, n_gather = 2 * nz, 2 * nx
    batch = tok_ref.shape[0]
    half = n_gather * SB
    rows = block * batch
    n_blocks = n_steps // block
    per_step = n_sum // block
    core = lax.axis_index('rows')
    me = lax.axis_index('states')
    z = me // (ny * nx)
    y = (me // nx) % ny
    x = me % nx
    group = me // n_gather
    c_place = (((y + 1) // 2) % 2) * nx + x
    far = sorted(range(1, n_sum), key=lambda k: -(ring_distance(k // 2, nz) + k % 2))
    sources = sorted(((f, d) for f in range(2) for d in range(nx)), key=lambda o: o[0] + ring_distance(o[1], nx))
    slot_of = {o: i for i, o in enumerate(sources)}
    far_gather = sources[:0:-1]
    n_near = n_gather // 2
    n_far = n_gather - n_near

    def sum_peer(k, sign=1):
        flip = k % 2
        return ((z + sign * (k // 2) + nz) % nz) * ny * nx + (y + flip * (ny - 1 - 2 * y)) * nx + x

    def mirror(k):
        return ((nz - k // 2) % nz) * 2 + k % 2

    def gather_peer(flip, d):
        return (me // (ny * nx)) * ny * nx + (y + flip * (1 - 2 * (y % 2))) * nx + (x + d) % nx

    def remote(src, dst, send, recv, state, to=1):
        return pltpu.make_async_remote_copy(src_ref=src, dst_ref=dst, send_sem=send, recv_sem=recv,
                                            device_id={'rows': to, 'states': state},
                                            device_id_type=pl.DeviceIdType.MESH)

    def wait_bytes(ref, sem):
        pltpu.make_async_copy(ref, ref, sem).wait()

    def a_rows(state, h):
        for i, (f, d) in enumerate(sources):
            there = ((state // nx + f) % 2) * nx + (x + d) % nx
            yield (a_ref.at[pl.ds((state // n_gather) * half + there * SB, SB)], pl.ds((2 * i + h) * SB, SB))

    def start_a(h, k):
        peer = sum_peer(k, -1)
        for src, to in a_rows(peer, h):
            remote(src, a_loc.at[k, to], a_send.at[k], a_sem.at[k, h], peer).start()

    def e_copy(b, k):
        return remote(e_both.at[pl.ds(b * rows + batch, rows)], e_loc.at[b, k], e_send, e_sem.at[b % 2, k], sum_peer(k, -1))

    def pick_tokens():
        def widen(i, carry):
            some = pl.ds(pl.multiple_of(i * batch, batch), batch)
            by_word[some, :] = emit_ref[some, :].astype(F32) * LIFT
            return carry

        lax.fori_loop(0, emit_ref.shape[0] // batch, widen, 0, unroll=5)

        def pick(t, carry):
            for b in range(batch):
                picked[t, b:b + 1, :] = by_word[pl.ds(tok_ref[b, t], 1), :]
            e_half[pl.ds(pl.multiple_of(t * batch, batch), batch), :] = picked[t].astype(BF16)
            return carry

        lax.fori_loop(0, n_steps, pick, 0)
        r0_own[...] = picked[0] * init_ref[...]

    barrier = pltpu.get_barrier_semaphore()

    def announce(state, to):
        pl.semaphore_signal(barrier, inc=1, device_id={'rows': to, 'states': state}, device_id_type=pl.DeviceIdType.MESH)

    @pl.when(core == 0)
    def helper():
        announce(me, 1)
        pl.semaphore_wait(barrier, n_sum)
        for k in range(1, n_sum, 2):
            start_a(0, k)
        e_both[pl.ds(n_steps * batch, batch), :] = jnp.zeros((batch, 2 * SB), BF16)
        pick_tokens()
        first = remote(r0_own, r_in.at[0, 0, 0], r0_send, r0_sem, me)
        first.start()
        every = pl.ds(0, n_steps * batch)
        mine = pltpu.make_async_copy(e_half, e_both.at[every, pl.ds(0, SB)], own_sem.at[0])
        mine.start()
        mine.wait()
        wait_bytes(e_both.at[every, pl.ds(SB, SB)], e_pair)
        for k in range(n_sum):
            e_copy(0, k).start()
        for k in range(0, n_sum, 2):
            start_a(0, k)
        wait_bytes(e_loc.at[0], e_send)

        def send_part(i, carry):
            @pl.when(i >= AHEAD)
            def paced():
                pl.semaphore_wait(tick, 1)

            for n in range(per_step):
                e_copy(1 + i // block, (i % block) * per_step + n).start()
            wait_bytes(e_loc.at[0, pl.ds(0, per_step)], e_send)
            return carry

        lax.fori_loop(0, n_steps - block, send_part, 0)
        first.wait_send()
        for k in range(n_sum):
            wait_bytes(a_loc.at[k, pl.ds(0, half)], a_send.at[k])
        wait_bytes(fin_alpha, f_recv.at[0])
        wait_bytes(fin_ll, f_recv.at[1])
        alpha_ref[...] = fin_alpha[...]
        ll_ref[...] = fin_ll[:, :batch]

    @pl.when(core == 1)
    def owner():
        eye = (lax.broadcasted_iota(jnp.int32, (batch, SB), 0)
               == lax.broadcasted_iota(jnp.int32, (batch, SB), 1))

        def as_row(tile):
            col = jnp.sum(tile, axis=1, keepdims=True)
            return jnp.sum(jnp.where(eye, col, 0.0), axis=0, keepdims=True)

        def as_col(row):
            return jnp.sum(jnp.where(eye, row, 0.0), axis=1, keepdims=True)

        def start_gather(slot):
            for f, d in far_gather:
                there = slot_of[f, (nx - d) % nx]
                remote(r_in.at[slot, 0], r_in.at[slot, there], g_send, g_recv.at[slot, there // n_near],
                       gather_peer(f, d)).start()

        def start_parts(slot):
            for k in far:
                remote(p_in.at[slot, group], p_in.at[slot, group], p_send, p_recv.at[slot], sum_peer(k)).start()

        others = pl.ds(0, n_gather - 1)
        peers = pl.ds(0, n_sum - 1)

        def finish_norm(slot):
            wait_bytes(p_in.at[slot, peers], p_recv.at[slot])
            c_in[slot, c_place] = jnp.sum(p_in[slot], axis=0)
            for o in far_gather:
                remote(c_in.at[slot, c_place], c_in.at[slot, c_place], c_send, c_recv.at[slot], gather_peer(*o)).start()

        def wait_near(slot):
            if n_near > 1:
                wait_bytes(r_in.at[slot, pl.ds(0, n_near - 1)], g_recv.at[slot, 0])

        def wait_far(slot):
            wait_bytes(r_in.at[slot, pl.ds(0, n_far)], g_recv.at[slot, 1])

        def norm(slot):
            wait_bytes(c_in.at[slot, others], c_recv.at[slot])
            c_row = jnp.sum(c_in[slot], axis=0)
            c_col = as_col(c_row)
            inv = 1.0 / c_col
            return c_row, inv * (2.0 - c_col * inv)

        def keep(t, slot, c_row, inv):
            now = lax.convert_element_type(t, F32)
            active = now < len_col[...]
            for h in range(2):
                alpha_acc[h] = jnp.where(active, r_in[slot, 0, h] * inv, alpha_acc[h])
            ll_acc[...] = ll_acc[...] + jnp.where(now < len_row[...], jnp.log(c_row * (1.0 / LIFT)), 0.0)

        def add_w(b, k, fresh):
            part = lax.dot_general(e_loc[b, k], a_loc[k], (((1,), (1,)), ((), ())), preferred_element_type=F32)
            slot = b % 2
            w_loc[slot] = jnp.where(fresh, 0.0, w_loc[slot]) + part

        for k in far:
            announce(sum_peer(k), 1)
        for o in far_gather:
            announce(gather_peer(*o), 1)
        for k in range(n_sum):
            announce(sum_peer(k), 0)
        pl.semaphore_wait(barrier, n_sum + n_gather - 1)
        for k in [*range(1, n_sum, 2), *range(2, n_sum - 2, 2)]:
            start_a(1, k)
        for src, to in a_rows(me, 1):
            pltpu.make_async_copy(src, a_loc.at[0, to], own_sem.at[1]).start()
        pick_tokens()
        alpha_acc[...] = jnp.zeros_like(alpha_acc)
        ll_acc[...] = jnp.zeros_like(ll_acc)
        w_loc[...] = jnp.zeros_like(w_loc)
        len_row[...] = jnp.zeros_like(len_row)
        len_row[:, :batch] = len_ref[...].astype(F32)
        len_col[...] = jnp.broadcast_to(as_col(len_row[...]), (batch, SB))
        pair = remote(e_half, e_both.at[pl.ds(0, n_steps * batch), pl.ds(SB, SB)], own_sem.at[0], e_pair, me, to=0)
        pair.start()
        r_in[0, 0, 1] = r0_own[...]
        wait_bytes(r0_own, r0_sem)
        p_in[0, group] = as_row(r_in[0, 0, 0] + r_in[0, 0, 1])
        start_parts(0)
        start_gather(0)
        start_a(1, n_sum - 2)
        finish_norm(0)
        wait_bytes(p_in.at[0, peers], p_send)
        wait_bytes(a_loc.at[0, pl.ds(0, half)], own_sem.at[1])

        def first_w(i, carry):
            k = 2 * i + 1 - (n_sum + 1) * (i // (n_sum // 2))
            wait_bytes(a_loc.at[k, pl.ds(0, half)], a_sem.at[k, 0])

            @pl.when(k > 0)
            def from_owner():
                wait_bytes(a_loc.at[k, pl.ds(0, half)], a_sem.at[k, 1])

            wait_bytes(e_loc.at[0, k], e_sem.at[0, k])
            add_w(0, k, False)
            return carry

        lax.fori_loop(0, n_sum, first_w, 0)
        pair.wait_send()
        for k in range(1, n_sum):
            wait_bytes(a_loc.at[k, pl.ds(0, half)], a_send.at[k])

        def one_step(t, carry):
            cur = t % 2
            nxt = (t + 1) % 2
            b = t // block
            row = pl.ds((t % block) * batch, batch)
            c_row, inv = norm(cur)
            total = jnp.zeros((batch, SB), F32)

            def take(first, last, total):
                for i in range(first, last):
                    for h in range(2):
                        cols = pl.ds((2 * i + h) * SB, SB)
                        tile = (r_in[cur, i, h] * inv).astype(BF16)
                        a_bf[:, cols] = tile
                        total = total + tile.astype(F32) * w_loc[b % 2, row, cols]
                return total

            def times(k, first, last):
                return jnp.dot(a_bf[:, first:last], a_loc[k, first:last], preferred_element_type=F32)

            order = far + [0]
            near_rows, all_rows = 2 * n_near * SB, 2 * half
            wait_near(cur)
            total = take(0, n_near, total)
            near = [times(k, 0, near_rows) for k in order[:NEAR]]
            wait_far(cur)
            total = take(n_near, n_gather, total)
            unit = jnp.where(t >= 0, jnp.float32(1.0), jnp.float32(0.0))
            ready = []

            def send_sum():
                k, part = ready.pop(0)
                for h in range(2):
                    u_out[k - 1, h] = part[:, h * SB:(h + 1) * SB]
                remote(u_out.at[k - 1], u_in.at[nxt, mirror(k) - 1], u_send, u_recv.at[nxt], sum_peer(k)).start()

            for i, k in enumerate(order):
                begin = near_rows if i < NEAR else 0
                middle = (begin + all_rows) // 2
                part = times(k, begin, middle) * unit + times(k, middle, all_rows)
                ready.append((k, part + near[i] if i < NEAR else part))
                if i == P_AFTER:
                    p_in[nxt, group] = as_row(total)
                    start_parts(nxt)
                if len(ready) > LAG:
                    send_sum()
            while len(ready) > 1:
                send_sum()
            own_part = ready[0][1]
            wait_bytes(r_in.at[cur, others], g_send)
            wait_bytes(c_in.at[cur, others], c_send)
            keep(t, cur, c_row, inv)
            finish_norm(nxt)
            wait_bytes(u_in.at[nxt], u_recv.at[nxt])
            for h in range(2):
                parts = [own_part[:, h * SB:(h + 1) * SB]] + [u_in[nxt, k, h] for k in range(n_sum - 1)]
                while len(parts) > 1:
                    parts = [parts[i] + parts[i + 1] for i in range(0, len(parts), 2)]
                r_in[nxt, 0, h] = parts[0] * e_loc[b, 0, row, pl.ds(h * SB, SB)].astype(F32)
            start_gather(nxt)

            @pl.when(t < n_steps - block - AHEAD)
            def go_on():
                pl.semaphore_signal(tick, inc=1, device_id={'rows': 0, 'states': me},
                                    device_id_type=pl.DeviceIdType.MESH)

            @pl.when(b + 1 < n_blocks)
            def next_w():
                later = b + 1
                for n in range(per_step):
                    k = (t % block) * per_step + n
                    wait_bytes(e_loc.at[later, k], e_sem.at[later % 2, k])
                    add_w(later, k, k == 0)

            wait_bytes(u_out, u_send)
            wait_bytes(p_in.at[nxt, peers], p_send)
            return carry

        lax.fori_loop(0, n_steps - 1, one_step, 0)
        last = (n_steps - 1) % 2
        c_row, inv = norm(last)
        keep(n_steps - 1, last, c_row, inv)
        result = [remote(alpha_acc.at[0], fin_alpha, f_send.at[0], f_recv.at[0], me, to=0),
                  remote(ll_acc, fin_ll, f_send.at[1], f_recv.at[1], me, to=0)]
        for copy in result:
            copy.start()
        wait_near(last)
        wait_far(last)
        wait_bytes(r_in.at[last, others], g_send)
        wait_bytes(c_in.at[last, others], c_send)
        alpha_ref[...] = alpha_acc[1]
        ll_ref[...] = ll_acc[:, :batch]
        for copy in result:
            copy.wait_send()


def solution(mesh):
    vec_axes = ('rows', 'states')
    nz, ny, nx = CHIPS
    n_sum, n_gather = 2 * nz, 2 * nx

    def local_forward(trans_blk, emit_blk, init_blk, tokens, lengths):
        batch, n_steps = tokens.shape
        cols = 2 * SB
        a_blk = trans_blk.reshape(trans_blk.shape[0], cols)
        vmem = pl.BlockSpec(memory_space=pltpu.VMEM)
        hbm = pl.BlockSpec(memory_space=pl.ANY)
        dma = pltpu.SemaphoreType.DMA
        k_rows = 2 * n_gather * SB
        block = min(BLOCK, n_sum)
        block_rows = block * batch
        n_blocks = n_steps // block
        alpha, ll = pl.pallas_call(
            functools.partial(forward_kernel, CHIPS, n_steps, block),
            out_shape=(jax.ShapeDtypeStruct((batch, SB), F32), jax.ShapeDtypeStruct((1, batch), F32)),
            in_specs=[hbm, vmem, vmem, pl.BlockSpec(memory_space=pltpu.SMEM), vmem],
            out_specs=(vmem, vmem),
            scratch_shapes=[
                pltpu.VMEM((n_sum, k_rows, cols), BF16),
                pltpu.VMEM(((n_steps + 1) * batch, cols), BF16),
                pltpu.VMEM((n_blocks, n_sum, block_rows, cols), BF16),
                pltpu.VMEM((2, block_rows, k_rows), F32),
                pltpu.VMEM((2, n_gather, 2, batch, SB), F32),
                pltpu.VMEM((2, n_gather, 1, SB), F32),
                pltpu.VMEM((2, n_sum, 1, SB), F32),
                pltpu.VMEM((2, n_sum - 1, 2, batch, SB), F32),
                pltpu.VMEM((n_sum - 1, 2, batch, SB), F32),
                pltpu.VMEM((batch, k_rows), BF16),
                pltpu.VMEM((1, SB), F32),
                pltpu.VMEM((batch, SB), F32),
                pltpu.VMEM((2, batch, SB), F32),
                pltpu.VMEM((1, SB), F32),
                pltpu.VMEM((batch, SB), F32),
                pltpu.VMEM((1, SB), F32),
                pltpu.VMEM((emit_blk.shape[1], SB), F32),
                pltpu.VMEM((n_steps, batch, SB), F32),
                pltpu.VMEM((n_steps * batch, SB), BF16),
                pltpu.VMEM((batch, SB), F32),
                pltpu.SemaphoreType.REGULAR,
                dma((n_sum, 2)), dma((n_sum,)), dma, dma, dma((2, n_sum)), dma, dma, dma((2,)),
                dma((2, 2)), dma, dma((2,)), dma, dma((2,)), dma, dma((2,)), dma, dma((2,)), dma((2,)),
            ],
            compiler_params=pltpu.CompilerParams(collective_id=0, has_side_effects=True,
                                                 vmem_limit_bytes=36 * 1024 * 1024),
            cost_estimate=pl.CostEstimate(flops=2 * batch * (n_steps - 1) * n_sum * k_rows * cols,
                                          bytes_accessed=n_sum * k_rows * cols * 2, transcendentals=0),
        )(a_blk, emit_blk.T, init_blk[None, :], tokens, lengths[None, :])
        return ll[0], alpha

    return jax.shard_map(local_forward, mesh=mesh, in_specs=(P('rows', None, 'states'), P(vec_axes, None), P(vec_axes), P('seqs', None), P('seqs')), out_specs=(P('seqs'), P('seqs', vec_axes)), check_vma=False)
```

```python
import functools

import jax
import jax.numpy as jnp
from jax import lax
from jax.experimental import pallas as pl
from jax.experimental.pallas import tpu as pltpu
from jax.sharding import PartitionSpec as P

CHIPS = (4, 4, 4)
SB = 128
LIFT = 2.0 ** 64
LAG = 1
P_AFTER = 1
NEAR = 0
BLOCK = 8
AHEAD = 6
F32 = jnp.float32
BF16 = jnp.bfloat16


def ring_distance(offset, n):
    return min(offset, n - offset)


def forward_kernel(dims, n_steps, block, a_ref, emit_ref, init_ref, tok_ref, len_ref, alpha_ref, ll_ref,
                   a_loc, e_both, e_loc, w_loc, r_in, c_in, p_in, u_in, u_out, a_bf, len_row, len_col, alpha_acc, ll_acc,
                   fin_alpha, fin_ll, by_word, picked, e_half, r0_own, tick, a_sem, a_send, e_pair, e_send, e_sem, r0_sem, r0_send, own_sem,
                   g_recv, g_send, c_recv, c_send, u_recv, u_send, p_recv, p_send, f_recv, f_send):
    nz, ny, nx = dims
    n_sum, n_gather = 2 * nz, 2 * nx
    batch = tok_ref.shape[0]
    half = n_gather * SB
    rows = block * batch
    n_blocks = n_steps // block
    per_step = n_sum // block
    core = lax.axis_index('rows')
    me = lax.axis_index('states')
    z = me // (ny * nx)
    y = (me // nx) % ny
    x = me % nx
    group = me // n_gather
    c_place = (((y + 1) // 2) % 2) * nx + x
    far = sorted(range(1, n_sum), key=lambda k: -(ring_distance(k // 2, nz) + k % 2))
    sources = sorted(((f, d) for f in range(2) for d in range(nx)), key=lambda o: o[0] + ring_distance(o[1], nx))
    slot_of = {o: i for i, o in enumerate(sources)}
    far_gather = sources[:0:-1]
    n_near = n_gather // 2
    n_far = n_gather - n_near

    def sum_peer(k, sign=1):
        flip = k % 2
        return ((z + sign * (k // 2) + nz) % nz) * ny * nx + (y + flip * (ny - 1 - 2 * y)) * nx + x

    def mirror(k):
        return ((nz - k // 2) % nz) * 2 + k % 2

    def gather_peer(flip, d):
        return (me // (ny * nx)) * ny * nx + (y + flip * (1 - 2 * (y % 2))) * nx + (x + d) % nx

    def remote(src, dst, send, recv, state, to=1):
        return pltpu.make_async_remote_copy(src_ref=src, dst_ref=dst, send_sem=send, recv_sem=recv,
                                            device_id={'rows': to, 'states': state},
                                            device_id_type=pl.DeviceIdType.MESH)

    def wait_bytes(ref, sem):
        pltpu.make_async_copy(ref, ref, sem).wait()

    def a_rows(state, h):
        for i, (f, d) in enumerate(sources):
            there = ((state // nx + f) % 2) * nx + (x + d) % nx
            yield (a_ref.at[pl.ds((state // n_gather) * half + there * SB, SB)], pl.ds((2 * i + h) * SB, SB))

    def start_a(h, k):
        peer = sum_peer(k, -1)
        for src, to in a_rows(peer, h):
            remote(src, a_loc.at[k, to], a_send.at[k], a_sem.at[k, h], peer).start()

    def e_copy(b, k):
        return remote(e_both.at[pl.ds(b * rows + batch, rows)], e_loc.at[b, k], e_send, e_sem.at[b % 2, k], sum_peer(k, -1))

    def pick_tokens():
        def widen(i, carry):
            some = pl.ds(pl.multiple_of(i * batch, batch), batch)
            by_word[some, :] = emit_ref[some, :].astype(F32) * LIFT
            return carry

        lax.fori_loop(0, emit_ref.shape[0] // batch, widen, 0, unroll=25)

        def pick(t, carry):
            for b in range(batch):
                picked[t, b:b + 1, :] = by_word[pl.ds(tok_ref[b, t], 1), :]
            e_half[pl.ds(pl.multiple_of(t * batch, batch), batch), :] = picked[t].astype(BF16)
            return carry

        lax.fori_loop(0, n_steps, pick, 0, unroll=4)
        r0_own[...] = picked[0] * init_ref[...]

    barrier = pltpu.get_barrier_semaphore()

    def announce(state, to):
        pl.semaphore_signal(barrier, inc=1, device_id={'rows': to, 'states': state}, device_id_type=pl.DeviceIdType.MESH)

    @pl.when(core == 0)
    def helper():
        announce(me, 1)
        pl.semaphore_wait(barrier, n_sum)
        for k in range(n_sum // 2):
            start_a(0, k)
        e_both[pl.ds(n_steps * batch, batch), :] = jnp.zeros((batch, 2 * SB), BF16)
        pick_tokens()
        first = remote(r0_own, r_in.at[0, 0, 0], r0_send, r0_sem, me)
        first.start()
        every = pl.ds(0, n_steps * batch)
        mine = pltpu.make_async_copy(e_half, e_both.at[every, pl.ds(0, SB)], own_sem.at[0])
        mine.start()
        mine.wait()
        wait_bytes(e_both.at[every, pl.ds(SB, SB)], e_pair)
        for k in range(n_sum):
            e_copy(0, k).start()
        for k in range(n_sum // 2, n_sum):
            start_a(0, k)
        wait_bytes(e_loc.at[0], e_send)

        def send_part(i, carry):
            @pl.when(i >= AHEAD)
            def paced():
                pl.semaphore_wait(tick, 1)

            for n in range(per_step):
                e_copy(1 + i // block, (i % block) * per_step + n).start()
            wait_bytes(e_loc.at[0, pl.ds(0, per_step)], e_send)
            return carry

        lax.fori_loop(0, n_steps - block, send_part, 0)
        first.wait_send()
        for k in range(n_sum):
            wait_bytes(a_loc.at[k, pl.ds(0, half)], a_send.at[k])
        wait_bytes(fin_alpha, f_recv.at[0])
        wait_bytes(fin_ll, f_recv.at[1])
        alpha_ref[...] = fin_alpha[...]
        ll_ref[...] = fin_ll[:, :batch]

    @pl.when(core == 1)
    def owner():
        eye = (lax.broadcasted_iota(jnp.int32, (batch, SB), 0)
               == lax.broadcasted_iota(jnp.int32, (batch, SB), 1))

        def as_row(tile):
            col = jnp.sum(tile, axis=1, keepdims=True)
            return jnp.sum(jnp.where(eye, col, 0.0), axis=0, keepdims=True)

        def as_col(row):
            return jnp.sum(jnp.where(eye, row, 0.0), axis=1, keepdims=True)

        def start_gather(slot):
            for f, d in far_gather:
                there = slot_of[f, (nx - d) % nx]
                remote(r_in.at[slot, 0], r_in.at[slot, there], g_send, g_recv.at[slot, there // n_near],
                       gather_peer(f, d)).start()

        def start_parts(slot):
            for k in far:
                remote(p_in.at[slot, group], p_in.at[slot, group], p_send, p_recv.at[slot], sum_peer(k)).start()

        others = pl.ds(0, n_gather - 1)
        peers = pl.ds(0, n_sum - 1)

        def finish_norm(slot):
            wait_bytes(p_in.at[slot, peers], p_recv.at[slot])
            c_in[slot, c_place] = jnp.sum(p_in[slot], axis=0)
            for o in far_gather:
                remote(c_in.at[slot, c_place], c_in.at[slot, c_place], c_send, c_recv.at[slot], gather_peer(*o)).start()

        def wait_near(slot):
            if n_near > 1:
                wait_bytes(r_in.at[slot, pl.ds(0, n_near - 1)], g_recv.at[slot, 0])

        def wait_far(slot):
            wait_bytes(r_in.at[slot, pl.ds(0, n_far)], g_recv.at[slot, 1])

        def norm(slot):
            wait_bytes(c_in.at[slot, others], c_recv.at[slot])
            c_row = jnp.sum(c_in[slot], axis=0)
            c_col = as_col(c_row)
            inv = 1.0 / c_col
            return c_row, inv * (2.0 - c_col * inv)

        def keep(t, slot, c_row, inv):
            now = lax.convert_element_type(t, F32)
            active = now < len_col[...]
            for h in range(2):
                alpha_acc[h] = jnp.where(active, r_in[slot, 0, h] * inv, alpha_acc[h])
            ll_acc[...] = ll_acc[...] + jnp.where(now < len_row[...], jnp.log(c_row * (1.0 / LIFT)), 0.0)

        def add_w(b, k, fresh):
            part = lax.dot_general(e_loc[b, k], a_loc[k], (((1,), (1,)), ((), ())), preferred_element_type=F32)
            slot = b % 2
            w_loc[slot] = jnp.where(fresh, 0.0, w_loc[slot]) + part

        for k in far:
            announce(sum_peer(k), 1)
        for o in far_gather:
            announce(gather_peer(*o), 1)
        for k in range(n_sum):
            announce(sum_peer(k), 0)
        pl.semaphore_wait(barrier, n_sum + n_gather - 1)
        for k in range(1, n_sum):
            start_a(1, k)
        for src, to in a_rows(me, 1):
            pltpu.make_async_copy(src, a_loc.at[0, to], own_sem.at[1]).start()
        pick_tokens()
        alpha_acc[...] = jnp.zeros_like(alpha_acc)
        ll_acc[...] = jnp.zeros_like(ll_acc)
        w_loc[...] = jnp.zeros_like(w_loc)
        len_row[...] = jnp.zeros_like(len_row)
        len_row[:, :batch] = len_ref[...].astype(F32)
        len_col[...] = jnp.broadcast_to(as_col(len_row[...]), (batch, SB))
        pair = remote(e_half, e_both.at[pl.ds(0, n_steps * batch), pl.ds(SB, SB)], own_sem.at[0], e_pair, me, to=0)
        pair.start()
        r_in[0, 0, 1] = r0_own[...]
        wait_bytes(r0_own, r0_sem)
        p_in[0, group] = as_row(r_in[0, 0, 0] + r_in[0, 0, 1])
        start_parts(0)
        start_gather(0)
        finish_norm(0)
        wait_bytes(p_in.at[0, peers], p_send)
        wait_bytes(a_loc.at[0, pl.ds(0, half)], own_sem.at[1])

        def first_w(k, carry):
            wait_bytes(a_loc.at[k, pl.ds(0, half)], a_sem.at[k, 0])

            @pl.when(k > 0)
            def from_owner():
                wait_bytes(a_loc.at[k, pl.ds(0, half)], a_sem.at[k, 1])

            wait_bytes(e_loc.at[0, k], e_sem.at[0, k])
            add_w(0, k, False)
            return carry

        lax.fori_loop(0, n_sum, first_w, 0)
        pair.wait_send()
        for k in range(1, n_sum):
            wait_bytes(a_loc.at[k, pl.ds(0, half)], a_send.at[k])

        def one_step(t, carry):
            cur = t % 2
            nxt = (t + 1) % 2
            b = t // block
            row = pl.ds((t % block) * batch, batch)
            c_row, inv = norm(cur)
            total = jnp.zeros((batch, SB), F32)

            def take(first, last, total):
                for i in range(first, last):
                    for h in range(2):
                        cols = pl.ds((2 * i + h) * SB, SB)
                        tile = (r_in[cur, i, h] * inv).astype(BF16)
                        a_bf[:, cols] = tile
                        total = total + tile.astype(F32) * w_loc[b % 2, row, cols]
                return total

            def times(k, first, last):
                return jnp.dot(a_bf[:, first:last], a_loc[k, first:last], preferred_element_type=F32)

            order = far + [0]
            near_rows, all_rows = 2 * n_near * SB, 2 * half
            wait_near(cur)
            total = take(0, n_near, total)
            near = [times(k, 0, near_rows) for k in order[:NEAR]]
            wait_far(cur)
            total = take(n_near, n_gather, total)
            unit = jnp.where(t >= 0, jnp.float32(1.0), jnp.float32(0.0))
            ready = []

            def send_sum():
                k, part = ready.pop(0)
                for h in range(2):
                    u_out[k - 1, h] = part[:, h * SB:(h + 1) * SB]
                remote(u_out.at[k - 1], u_in.at[nxt, mirror(k) - 1], u_send, u_recv.at[nxt], sum_peer(k)).start()

            for i, k in enumerate(order):
                begin = near_rows if i < NEAR else 0
                middle = (begin + all_rows) // 2
                part = times(k, begin, middle) * unit + times(k, middle, all_rows)
                ready.append((k, part + near[i] if i < NEAR else part))
                if i == P_AFTER:
                    p_in[nxt, group] = as_row(total)
                    start_parts(nxt)
                if len(ready) > LAG:
                    send_sum()
            while len(ready) > 1:
                send_sum()
            own_part = ready[0][1]
            wait_bytes(r_in.at[cur, others], g_send)
            wait_bytes(c_in.at[cur, others], c_send)
            keep(t, cur, c_row, inv)
            finish_norm(nxt)
            wait_bytes(u_in.at[nxt], u_recv.at[nxt])
            for h in range(2):
                parts = [own_part[:, h * SB:(h + 1) * SB]] + [u_in[nxt, k, h] for k in range(n_sum - 1)]
                while len(parts) > 1:
                    parts = [parts[i] + parts[i + 1] for i in range(0, len(parts), 2)]
                r_in[nxt, 0, h] = parts[0] * e_loc[b, 0, row, pl.ds(h * SB, SB)].astype(F32)
            start_gather(nxt)

            @pl.when(t < n_steps - block - AHEAD)
            def go_on():
                pl.semaphore_signal(tick, inc=1, device_id={'rows': 0, 'states': me},
                                    device_id_type=pl.DeviceIdType.MESH)

            @pl.when(b + 1 < n_blocks)
            def next_w():
                later = b + 1
                for n in range(per_step):
                    k = (t % block) * per_step + n
                    wait_bytes(e_loc.at[later, k], e_sem.at[later % 2, k])
                    add_w(later, k, k == 0)

            wait_bytes(u_out, u_send)
            wait_bytes(p_in.at[nxt, peers], p_send)
            return carry

        lax.fori_loop(0, n_steps - 1, one_step, 0)
        last = (n_steps - 1) % 2
        c_row, inv = norm(last)
        wait_near(last)
        wait_far(last)
        keep(n_steps - 1, last, c_row, inv)
        wait_bytes(r_in.at[last, others], g_send)
        wait_bytes(c_in.at[last, others], c_send)
        result = [remote(alpha_acc.at[0], fin_alpha, f_send.at[0], f_recv.at[0], me, to=0),
                  remote(ll_acc, fin_ll, f_send.at[1], f_recv.at[1], me, to=0)]
        for copy in result:
            copy.start()
        alpha_ref[...] = alpha_acc[1]
        ll_ref[...] = ll_acc[:, :batch]
        for copy in result:
            copy.wait_send()


def solution(mesh):
    vec_axes = ('rows', 'states')
    nz, ny, nx = CHIPS
    n_sum, n_gather = 2 * nz, 2 * nx

    def local_forward(trans_blk, emit_blk, init_blk, tokens, lengths):
        batch, n_steps = tokens.shape
        cols = 2 * SB
        a_blk = trans_blk.reshape(trans_blk.shape[0], cols)
        vmem = pl.BlockSpec(memory_space=pltpu.VMEM)
        hbm = pl.BlockSpec(memory_space=pl.ANY)
        dma = pltpu.SemaphoreType.DMA
        k_rows = 2 * n_gather * SB
        block = min(BLOCK, n_sum)
        block_rows = block * batch
        n_blocks = n_steps // block
        alpha, ll = pl.pallas_call(
            functools.partial(forward_kernel, CHIPS, n_steps, block),
            out_shape=(jax.ShapeDtypeStruct((batch, SB), F32), jax.ShapeDtypeStruct((1, batch), F32)),
            in_specs=[hbm, vmem, vmem, pl.BlockSpec(memory_space=pltpu.SMEM), vmem],
            out_specs=(vmem, vmem),
            scratch_shapes=[
                pltpu.VMEM((n_sum, k_rows, cols), BF16),
                pltpu.VMEM(((n_steps + 1) * batch, cols), BF16),
                pltpu.VMEM((n_blocks, n_sum, block_rows, cols), BF16),
                pltpu.VMEM((2, block_rows, k_rows), F32),
                pltpu.VMEM((2, n_gather, 2, batch, SB), F32),
                pltpu.VMEM((2, n_gather, 1, SB), F32),
                pltpu.VMEM((2, n_sum, 1, SB), F32),
                pltpu.VMEM((2, n_sum - 1, 2, batch, SB), F32),
                pltpu.VMEM((n_sum - 1, 2, batch, SB), F32),
                pltpu.VMEM((batch, k_rows), BF16),
                pltpu.VMEM((1, SB), F32),
                pltpu.VMEM((batch, SB), F32),
                pltpu.VMEM((2, batch, SB), F32),
                pltpu.VMEM((1, SB), F32),
                pltpu.VMEM((batch, SB), F32),
                pltpu.VMEM((1, SB), F32),
                pltpu.VMEM((emit_blk.shape[1], SB), F32),
                pltpu.VMEM((n_steps, batch, SB), F32),
                pltpu.VMEM((n_steps * batch, SB), BF16),
                pltpu.VMEM((batch, SB), F32),
                pltpu.SemaphoreType.REGULAR,
                dma((n_sum, 2)), dma((n_sum,)), dma, dma, dma((2, n_sum)), dma, dma, dma((2,)),
                dma((2, 2)), dma, dma((2,)), dma, dma((2,)), dma, dma((2,)), dma, dma((2,)), dma((2,)),
            ],
            compiler_params=pltpu.CompilerParams(collective_id=0, has_side_effects=True,
                                                 vmem_limit_bytes=36 * 1024 * 1024),
            cost_estimate=pl.CostEstimate(flops=2 * batch * (n_steps - 1) * n_sum * k_rows * cols,
                                          bytes_accessed=n_sum * k_rows * cols * 2, transcendentals=0),
        )(a_blk, emit_blk.T, init_blk[None, :], tokens, lengths[None, :])
        return ll[0], alpha

    return jax.shard_map(local_forward, mesh=mesh, in_specs=(P('rows', None, 'states'), P(vec_axes, None), P(vec_axes), P('seqs', None), P('seqs')), out_specs=(P('seqs'), P('seqs', vec_axes)), check_vma=False)
```
